32 devices in a mesh: dp: 16 (over z, y, core), mlp: 2 (over x).
Axes of the slice: x: 2, y: 2, z: 4, core: 2. Of those that a mesh axis runs over, the one named last changes fastest.
Arguments:
- block_input: bfloat16 [16, 2, 160, 1024], P('dp', 'mlp'), may hold values from -6 to 6
- span_offset: int32 [16, 2], replicated, may hold values from 0 to 15, as said below
- ln_gain: float32 [1024], replicated, may hold values from 0.5 to 1.5
- ln_bias: float32 [1024], replicated, may hold values from -3 to 3
- w_qkv: bfloat16 [1024, 3072], replicated, may hold values from -0.25 to 0.25
- b_qkv: float32 [3072], replicated, may hold values from -3 to 3
- w_out: bfloat16 [1024, 1024], replicated, may hold values from -1 to 1
- b_out: float32 [1024], replicated, may hold values from -3 to 3
- w_up: bfloat16 [1024, 4096], P(None, 'mlp'), may hold values from -0.1875 to 0.1875
- b_up: float32 [4096], P('mlp'), may hold values from -3 to 3
- w_down: bfloat16 [4096, 1024], P('mlp'), may hold values from -0.09375 to 0.09375
- b_down: float32 [1024], replicated, may hold values from -3 to 3
- cotangent: bfloat16 [16, 2, 160, 1024], P('dp', 'mlp'), may hold values from -6 to 6
Outputs:
- output: bfloat16 [16, 2, 160, 1024], P('dp', 'mlp')
- grad_input: float32 [16, 2, 160, 1024], P('dp', 'mlp')
- grad_ln_gain: float32 [1024], P('mlp')
- grad_ln_bias: float32 [1024], P('mlp')
- grad_w_qkv: float32 [1024, 3072], P(None, 'mlp')
- grad_b_qkv: float32 [3072], P('mlp')
- grad_w_out: float32 [1024, 1024], P(None, 'mlp')
- grad_b_out: float32 [1024], P('mlp')
- grad_w_up: float32 [1024, 4096], P(None, 'mlp')
- grad_b_up: float32 [4096], P('mlp')
- grad_w_down: float32 [4096, 1024], P('mlp')
- grad_b_down: float32 [1024], P('mlp')
The draws below stay inside these ranges and needn't reach their ends.
Inputs may be any that keep to these rules, and one draw needn't show every extreme that they name: For every sequence s, span_offset[:, s] is a permutation of 0 to 15.
All inputs are finite; a program needn't handle non-finite values.
Results may differ from the reference program's by a relative error of at most 0.02.
Values may be sent and summed in bfloat16 or wider, within the bound.
A program may use at most 256 MiB of HBM per device.

```python
import math
import jax
import jax.numpy as jnp
from jax import lax

D = 1024
HEADS = 16
HEAD_DIM = 64
FF = 4096
ROT = 16
TOK_DEV = 160
SPANS = 16
SEQS = 2


def draw_span_offset(key, part):
    seq_keys = jax.random.split(key, SEQS)
    orders = jax.vmap(lambda one_key: jax.random.permutation(one_key, SPANS))(seq_keys)
    return jnp.transpose(orders).astype(jnp.int32)


def block_scale(stream_key, shape, shards, low, high):
    level = 1.0
    for dim, blocks in shards:
        steps = jax.random.uniform(jax.random.fold_in(jax.random.fold_in(stream_key, 6), dim), (blocks,), jnp.float32, low / len(shards), high / len(shards))
        level = level * jnp.repeat(jnp.exp(steps), shape[dim] // blocks).reshape((-1,) + (1,) * (len(shape) - 1 - dim))
    return level


def bell_draw(rng, shape, deviation, limit, cuts=(), kind=jnp.bfloat16):
    level = block_scale(rng, shape, cuts, -0.22, 0.18) if cuts else 1.0
    values = jax.random.normal(rng, shape, jnp.float32) * deviation * level
    return jnp.minimum(jnp.maximum(values, -limit), limit).astype(kind)


def setup_inputs(seed: int = 0) -> dict:
    key_list = jax.random.split(jax.random.key(seed), 14)
    block_input = bell_draw(key_list[0], (SPANS, SEQS, TOK_DEV, D), 1.0, 6.0, ((0, 16), (1, 2)))
    span_offset = draw_span_offset(jax.random.fold_in(key_list[13], 71), 0)
    ln_gain = jnp.clip(1.0 + 0.1 * jax.random.normal(key_list[2], (D,), jnp.float32), 0.5, 1.5)
    ln_bias = bell_draw(key_list[3], (D,), 0.5, 3.0, (), jnp.float32)
    w_qkv = bell_draw(key_list[4], (D, 3 * D), (D // 2) ** -0.5, 0.25)
    b_qkv = bell_draw(key_list[5], (3 * D,), 0.5, 3.0, (), jnp.float32)
    w_out = bell_draw(key_list[6], (D, D), (D // 32) ** -0.5, 1.0)
    b_out = bell_draw(key_list[7], (D,), 0.5, 3.0, (), jnp.float32)
    w_up = bell_draw(key_list[8], (D, FF), D ** -0.5, 0.1875, ((1, 2),))
    b_up = bell_draw(key_list[9], (FF,), 0.5, 3.0, ((0, 2),), jnp.float32)
    w_down = bell_draw(key_list[10], (FF, D), FF ** -0.5, 0.09375, ((0, 2),))
    b_down = bell_draw(key_list[11], (D,), 0.5, 3.0, (), jnp.float32)
    cotangent = bell_draw(key_list[12], (SPANS, SEQS, TOK_DEV, D), 1.0, 6.0, ((0, 16), (1, 2)))
    return {"block_input": block_input, "span_offset": span_offset, "ln_gain": ln_gain, "ln_bias": ln_bias, "w_qkv": w_qkv, "b_qkv": b_qkv, "w_out": w_out, "b_out": b_out, "w_up": w_up, "b_up": b_up, "w_down": w_down, "b_down": b_down, "cotangent": cotangent}


HIGHEST = lax.Precision.HIGHEST
EPSILON = 1e-05
ROPE_BASE = 10000.0
SQRT_HALF = 1.0 / math.sqrt(2.0)

@jax.custom_vjp
def low(v):
    return lax.optimization_barrier(v.astype(jnp.bfloat16)).astype(jnp.float32)

@jax.custom_vjp
def low_back(v):
    return v

def low_keep(v):
    return (low(v), None)

def low_pass(kept, grad):
    return (grad,)

def back_keep(v):
    return (v, None)

def back_low(kept, grad):
    return (low(grad),)
low.defvjp(low_keep, low_pass)
low_back.defvjp(back_keep, back_low)

def rotate(values, positions, sign_factor):
    half_rot = ROT // 2
    frequency = ROPE_BASE ** (-(jnp.arange(half_rot, dtype=jnp.float32) * 2.0 / ROT))
    angles = positions.astype(jnp.float32)[:, None] * frequency[None, :]
    cosine = jnp.cos(angles)[:, None, :]
    sine_part = sign_factor * jnp.sin(angles)[:, None, :]
    first_half = values[..., :half_rot]
    second_half = values[..., half_rot:ROT]
    return jnp.concatenate([first_half * cosine - second_half * sine_part, second_half * cosine + first_half * sine_part, values[..., ROT:]], axis=-1)

def layer_norm(row_data, gain_vec, shift_vec):
    centre = lax.optimization_barrier(jnp.mean(row_data, axis=-1, keepdims=True))
    centred = row_data - centre
    spread = lax.optimization_barrier(jnp.mean(centred * centred, axis=-1, keepdims=True))
    scaled = centred * lax.rsqrt(spread + EPSILON)
    return scaled * gain_vec + shift_vec

def gelu_exact(values):
    return 0.5 * values * (1.0 + lax.erf(values * SQRT_HALF))

def reference(block_input, span_offset, ln_gain, ln_bias, w_qkv, b_qkv, w_out, b_out, w_up, b_up, w_down, b_down, cotangent):
    scale_dot = 1.0 / math.sqrt(HEAD_DIM)
    params = (ln_gain, ln_bias, w_qkv.astype(jnp.float32), b_qkv, w_out.astype(jnp.float32), b_out, w_up.astype(jnp.float32), b_up, w_down.astype(jnp.float32), b_down)

    def forward(inputs_all, weights):
        gain_vec, shift_vec, qkv_mat, qkv_bias, out_mat, out_bias, up_mat, up_bias, down_mat, down_bias = weights

        def one_sequence(packed):
            rows_in, offsets = packed
            span_count = rows_in.shape[0]
            tok_count = rows_in.shape[1]
            length_all = span_count * tok_count
            row_data = rows_in.reshape(length_all, D)
            positions = (offsets[:, None] * tok_count + jnp.arange(tok_count, dtype=jnp.int32)[None, :]).reshape(length_all)
            normed = low(layer_norm(row_data, gain_vec, shift_vec))
            project = low_back(jnp.dot(normed, qkv_mat, precision=HIGHEST) + qkv_bias)
            queries = low(rotate(project[:, :D].reshape(length_all, HEADS, HEAD_DIM), positions, 1.0))
            keys_all = low(rotate(project[:, D:2 * D].reshape(length_all, HEADS, HEAD_DIM), positions, 1.0))
            values_all = low(project[:, 2 * D:].reshape(length_all, HEADS, HEAD_DIM))
            group_size = max(1, 512 // tok_count)
            while span_count % group_size:
                group_size -= 1
            block_rows = group_size * tok_count
            block_count = length_all // block_rows

            def attend_block(packed_block):
                query_block, query_pos = packed_block
                raw_dot = jnp.einsum('qhd,khd->hqk', query_block, keys_all, precision=HIGHEST)
                scores = low_back(raw_dot * scale_dot)
                allowed = positions[None, :] <= query_pos[:, None]
                weights_exp = jnp.where(allowed[None], jnp.exp(scores), 0.0)
                totals = low_back(lax.optimization_barrier(jnp.sum(weights_exp, axis=-1)))
                mixed_sum = low_back(jnp.einsum('hqk,khd->qhd', low(weights_exp), values_all, precision=HIGHEST))
                return (mixed_sum / totals.T[:, :, None]).reshape(block_rows, D)
            attended = lax.map(jax.checkpoint(attend_block), (queries.reshape(block_count, block_rows, HEADS, HEAD_DIM), positions.reshape(block_count, block_rows))).reshape(length_all, D)
            attn_branch = jnp.dot(low(attended), out_mat, precision=HIGHEST) + out_bias
            up_proj = low_back(jnp.dot(normed, up_mat, precision=HIGHEST) + up_bias)
            mlp_branch = jnp.dot(low(gelu_exact(up_proj)), down_mat, precision=HIGHEST) + down_bias
            return (row_data + attn_branch + mlp_branch).reshape(span_count, tok_count, D)
        outputs = lax.map(jax.checkpoint(one_sequence), (jnp.swapaxes(inputs_all, 0, 1), jnp.swapaxes(span_offset, 0, 1)))
        return jnp.swapaxes(outputs, 0, 1)
    result, pullback = jax.vjp(forward, block_input.astype(jnp.float32), params)
    grad_in, gradients = pullback(cotangent.astype(jnp.float32))
    return (result.astype(jnp.bfloat16), grad_in, gradients[0], gradients[1], gradients[2], gradients[3], gradients[4], gradients[5], gradients[6], gradients[7], gradients[8], gradients[9])
```

```python
import functools
import math

import jax
import jax.numpy as jnp
from jax import lax
from jax.experimental import pallas as pl
from jax.experimental.pallas import tpu as pltpu
from jax.sharding import PartitionSpec as P

HEADS = 16
HEAD_DIM = 64
ROT = 16

EPSILON = 1e-05
ROPE_BASE = 10000.0
SQRT_HALF = 1.0 / math.sqrt(2.0)
INV_ROOT_TWO_PI = 1.0 / math.sqrt(2.0 * math.pi)

MESH = pl.DeviceIdType.MESH
F32 = jnp.float32
BF16 = jnp.bfloat16
LANES = 128
VMEM_BIG = 60 * 1024 * 1024


def dot_nn(a, b):
    return lax.dot_general(a, b, (((1,), (0,)), ((), ())), preferred_element_type=F32)


def dot_nt(a, b):
    return lax.dot_general(a, b, (((1,), (1,)), ((), ())), preferred_element_type=F32)


def dot_tn(a, b):
    return lax.dot_general(a, b, (((0,), (0,)), ((), ())), preferred_element_type=F32)


def rotary_tables(positions):
    lane = jnp.arange(LANES, dtype=jnp.int32) % HEAD_DIM
    half = ROT // 2
    frequency = ROPE_BASE ** (-((lane % half).astype(F32) * 2.0 / ROT))
    angles = positions.astype(F32)[:, None] * frequency[None, :]
    cosine = jnp.where(lane < ROT, jnp.cos(angles), 1.0)
    sine = jnp.sin(angles)
    up = jnp.where(lane < half, -sine, 0.0)
    down = jnp.where((lane >= half) & (lane < ROT), sine, 0.0)
    return jnp.stack([cosine, up, down])


def rotate_tile(x, tables, sign):
    half = ROT // 2
    return (
        x * tables[0]
        + pltpu.roll(x, LANES - half, 1) * (tables[1] * sign)
        + pltpu.roll(x, half, 1) * (tables[2] * sign)
    )


def split_pair(first, second, low):
    swap_first = pltpu.roll(first, HEAD_DIM, 1)
    swap_second = pltpu.roll(second, HEAD_DIM, 1)
    return jnp.where(low, first, swap_second), jnp.where(low, swap_first, second)


def project_kernel(
    x_ref, cot_ref, gain_ref, shift_ref, wq_ref, wk_ref, wv_ref, bq_ref, bk_ref, bv_ref, wo_ref, tab_ref,
    normed_ref, send_ref,
):
    @pl.when(pl.program_id(0) == 0)
    def _():
        rows = x_ref[...].astype(F32)
        centre = jnp.mean(rows, axis=-1, keepdims=True)
        centred = rows - centre
        spread = jnp.mean(centred * centred, axis=-1, keepdims=True)
        unit = centred * lax.rsqrt(spread + EPSILON)
        normed_ref[...] = (unit * gain_ref[...] + shift_ref[...]).astype(BF16)

    normed = normed_ref[...]
    q = dot_nn(normed, wq_ref[...]) + bq_ref[...]
    k = dot_nn(normed, wk_ref[...]) + bk_ref[...]
    v = dot_nn(normed, wv_ref[...]) + bv_ref[...]
    grad_att = dot_nt(cot_ref[...], wo_ref[...])
    tables = [tab_ref[i] for i in range(3)]
    low = lax.broadcasted_iota(jnp.int32, (x_ref.shape[0], LANES), 1) < HEAD_DIM
    for tile in range(q.shape[1] // LANES):
        cols = slice(tile * LANES, (tile + 1) * LANES)
        q_tile = rotate_tile(q[:, cols], tables, 1.0)
        k_tile = rotate_tile(k[:, cols], tables, 1.0)
        qk = split_pair(q_tile, k_tile, low)
        vg = split_pair(v[:, cols], grad_att[:, cols], low)
        for side in range(2):
            send_ref[2 * tile + side, :, :LANES] = qk[side].astype(BF16)
            send_ref[2 * tile + side, :, LANES:] = vg[side].astype(BF16)


def project(x, cot, gain, shift, w_qkv, b_qkv, w_out, tables):
    tok, width = x.shape
    group = 256
    steps = width // group
    heads_step = group // HEAD_DIM
    const = lambda shape: pl.BlockSpec(shape, lambda g: (0,) * len(shape))
    w_spec = lambda part: pl.BlockSpec((width, group), lambda g: (0, part * steps + g))
    b_spec = lambda part: pl.BlockSpec((1, group), lambda g: (0, part * steps + g))
    return pl.pallas_call(
        project_kernel,
        grid=(steps,),
        out_shape=(
            jax.ShapeDtypeStruct((tok, width), BF16),
            jax.ShapeDtypeStruct((HEADS, tok, 4 * HEAD_DIM), BF16),
        ),
        in_specs=[
            const((tok, width)), const((tok, width)), const((1, width)), const((1, width)),
            w_spec(0), w_spec(1), w_spec(2), b_spec(0), b_spec(1), b_spec(2),
            pl.BlockSpec((group, width), lambda g: (g, 0)),
            const((3, tok, LANES)),
        ],
        out_specs=(
            const((tok, width)),
            pl.BlockSpec((heads_step, tok, 4 * HEAD_DIM), lambda g: (g, 0, 0)),
        ),
        name="project",
    )(x, cot, gain, shift, w_qkv, w_qkv, w_qkv, b_qkv, b_qkv, b_qkv, w_out, tables)


def exchange_kernel(count, peers, blocks, *refs):
    heads_in, rest = refs[0], refs[1:]
    pairs_in, rest = rest[:count], rest[count:]
    heads_out, rest = rest[0], rest[1:]
    pairs_out, rest = rest[:count], rest[count:]
    head_send, head_recv, pair_send, pair_recv, local_sem = rest
    me = lax.axis_index("dp")
    other = 1 - lax.axis_index("mlp")
    barrier = pltpu.get_barrier_semaphore()
    for step in range(1, peers):
        pl.semaphore_signal(barrier, inc=1, device_id={"dp": lax.rem(me + step, peers)}, device_id_type=MESH)
    if count:
        pl.semaphore_signal(barrier, inc=1, device_id={"mlp": other}, device_id_type=MESH)
    pl.semaphore_wait(barrier, peers - 1 + (1 if count else 0))
    copies = []
    for i in range(count):
        copies.append(
            pltpu.make_async_remote_copy(
                src_ref=pairs_in[i], dst_ref=pairs_out[i], send_sem=pair_send.at[i], recv_sem=pair_recv.at[i],
                device_id={"mlp": other}, device_id_type=MESH,
            )
        )
    for step in range(1, peers):
        target = lax.rem(me + step, peers)
        copies.append(
            pltpu.make_async_remote_copy(
                src_ref=heads_in.at[target], dst_ref=heads_out.at[me],
                send_sem=head_send.at[step], recv_sem=head_recv.at[step],
                device_id={"dp": target}, device_id_type=MESH,
            )
        )
    for copy in copies:
        copy.start()
    own = pltpu.make_async_copy(heads_in.at[me], heads_out.at[me], local_sem)
    own.start()
    own.wait()
    for copy in copies:
        copy.wait()


def exchange(heads, pairs, collective):
    count = len(pairs)
    peers = heads.shape[0]
    any_spec = pl.BlockSpec(memory_space=pl.ANY)
    out = pl.pallas_call(
        functools.partial(exchange_kernel, count, peers, None),
        out_shape=(jax.ShapeDtypeStruct(heads.shape, heads.dtype),)
        + tuple(jax.ShapeDtypeStruct(p.shape, p.dtype) for p in pairs),
        in_specs=[any_spec] * (1 + count),
        out_specs=(any_spec,) * (1 + count),
        scratch_shapes=[
            pltpu.SemaphoreType.DMA((peers,)),
            pltpu.SemaphoreType.DMA((peers,)),
            pltpu.SemaphoreType.DMA((max(count, 1),)),
            pltpu.SemaphoreType.DMA((max(count, 1),)),
            pltpu.SemaphoreType.DMA,
        ],
        compiler_params=pltpu.CompilerParams(collective_id=collective, has_side_effects=True),
        name="exchange" + str(collective),
    )(heads, *pairs)
    return out[0], out[1:]


def swap_kernel(count, *refs):
    ins, outs = refs[:count], refs[count : 2 * count]
    send, recv = refs[2 * count :]
    other = 1 - lax.axis_index("mlp")
    barrier = pltpu.get_barrier_semaphore()
    pl.semaphore_signal(barrier, inc=1, device_id={"mlp": other}, device_id_type=MESH)
    pl.semaphore_wait(barrier, 1)
    copies = [
        pltpu.make_async_remote_copy(
            src_ref=ins[i], dst_ref=outs[i], send_sem=send.at[i], recv_sem=recv.at[i],
            device_id={"mlp": other}, device_id_type=MESH,
        )
        for i in range(count)
    ]
    for copy in copies:
        copy.start()
    for copy in copies:
        copy.wait()


def swap(arrays, collective):
    count = len(arrays)
    any_spec = pl.BlockSpec(memory_space=pl.ANY)
    return pl.pallas_call(
        functools.partial(swap_kernel, count),
        out_shape=tuple(jax.ShapeDtypeStruct(a.shape, a.dtype) for a in arrays),
        in_specs=[any_spec] * count,
        out_specs=(any_spec,) * count,
        scratch_shapes=[pltpu.SemaphoreType.DMA((count,)), pltpu.SemaphoreType.DMA((count,))],
        compiler_params=pltpu.CompilerParams(collective_id=collective, has_side_effects=True),
        name="swap" + str(collective),
    )(*arrays)


def attention_kernel(
    tile, order_ref, in_ref, out_ref,
    q_nat, k_nat, v_nat, k_tr, v_tr, g_tr, probs, kv_grad, aq_out,
):
    spans, tok, _ = in_ref.shape
    length = spans * tok
    blocks = length // tile
    scale = 1.0 / math.sqrt(HEAD_DIM)
    zeros = jnp.zeros((tok, HEAD_DIM), BF16)

    def gather(place, carry):
        span = order_ref[place]
        rows = pl.ds(pl.multiple_of(place * tok, tok), tok)
        data = in_ref[span]
        q_nat[rows, :] = jnp.concatenate([data[:, :HEAD_DIM] * jnp.asarray(scale, BF16), zeros], axis=1)
        k_nat[rows, :] = data[:, HEAD_DIM : 2 * HEAD_DIM]
        v_nat[rows, :] = data[:, 2 * HEAD_DIM : 3 * HEAD_DIM]
        return carry

    lax.fori_loop(0, spans, gather, 0)

    def gather_grad(place, carry):
        span = order_ref[place]
        rows = pl.ds(pl.multiple_of(place * tok, tok), tok)
        g_nat_rows = in_ref[span][:, 3 * HEAD_DIM :]
        aq_out[rows, :HEAD_DIM] = g_nat_rows
        return carry

    lax.fori_loop(0, spans, gather_grad, 0)

    def flip(block, carry):
        rows = pl.ds(pl.multiple_of(block * tile, tile), tile)
        k_tr[:, rows] = k_nat[rows, :].T
        v_tr[:, rows] = v_nat[rows, :].T
        g_tr[:, rows] = aq_out[rows, :HEAD_DIM].T
        kv_grad[rows, :] = jnp.zeros((tile, 2 * HEAD_DIM), F32)
        return carry

    lax.fori_loop(0, blocks, flip, 0)

    key_row = lax.broadcasted_iota(jnp.int32, (tile, tile), 0)
    query_col = lax.broadcasted_iota(jnp.int32, (tile, tile), 1)
    causal = key_row <= query_col
    pad = jnp.zeros((tile, HEAD_DIM), BF16)

    def query_block(block, carry):
        q_rows = pl.ds(pl.multiple_of(block * tile, tile), tile)
        queries_pad = q_nat[q_rows, :]
        queries = queries_pad[:, :HEAD_DIM]

        def forward(j, state, masked):
            mixed, totals = state
            rows = pl.ds(pl.multiple_of(j * tile, tile), tile)
            prob = jnp.exp(dot_nt(k_nat[rows, :], queries))
            if masked:
                prob = jnp.where(causal, prob, 0.0)
            probs[rows, :] = prob
            mixed = mixed + dot_nn(v_tr[:, rows], prob.astype(BF16))
            totals = totals + jnp.sum(prob.reshape(tile // 8, 8, tile), axis=0)
            return mixed, totals

        state = (jnp.zeros((HEAD_DIM, tile), F32), jnp.zeros((8, tile), F32))
        state = lax.fori_loop(0, block, lambda j, s: forward(j, s, False), state)
        mixed, totals = forward(block, state, True)
        totals = jnp.sum(totals, axis=0, keepdims=True)
        attended = mixed / totals
        grad_att = g_tr[:, q_rows].astype(F32)
        grad_mixed = (grad_att / totals).astype(BF16)
        grad_totals = (-jnp.sum(grad_att * attended, axis=0, keepdims=True) / totals).astype(BF16).astype(F32)
        grad_pad = jnp.concatenate([pad, grad_mixed.T], axis=1)

        def backward(j, grad_q):
            rows = pl.ds(pl.multiple_of(j * tile, tile), tile)
            prob = probs[rows, :]
            grad_scores = (prob * (dot_nn(v_nat[rows, :], grad_mixed) + grad_totals)).astype(BF16)
            kv_grad[rows, :] += dot_nn(grad_scores, queries_pad) + dot_nn(prob.astype(BF16), grad_pad)
            return grad_q + dot_nn(k_tr[:, rows], grad_scores)

        grad_q = lax.fori_loop(0, block + 1, backward, jnp.zeros((HEAD_DIM, tile), F32))
        aq_out[q_rows, :] = jnp.concatenate([attended, grad_q * scale], axis=0).T.astype(BF16)
        return carry

    lax.fori_loop(0, blocks, query_block, 0)

    def scatter(place, carry):
        span = order_ref[place]
        rows = pl.ds(pl.multiple_of(place * tok, tok), tok)
        out_ref[span, :, : 2 * HEAD_DIM] = aq_out[rows, :]
        out_ref[span, :, 2 * HEAD_DIM :] = kv_grad[rows, :].astype(BF16)
        return carry

    lax.fori_loop(0, spans, scatter, 0)


def attention(heads, order):
    spans, tok, width = heads.shape
    length = spans * tok
    tile = 256
    vmem = pl.BlockSpec(memory_space=pltpu.VMEM)
    return pl.pallas_call(
        functools.partial(attention_kernel, tile),
        out_shape=jax.ShapeDtypeStruct(heads.shape, BF16),
        in_specs=[pl.BlockSpec(memory_space=pltpu.SMEM), vmem],
        out_specs=vmem,
        scratch_shapes=[
            pltpu.VMEM((length, 2 * HEAD_DIM), BF16),
            pltpu.VMEM((length, HEAD_DIM), BF16),
            pltpu.VMEM((length, HEAD_DIM), BF16),
            pltpu.VMEM((HEAD_DIM, length), BF16),
            pltpu.VMEM((HEAD_DIM, length), BF16),
            pltpu.VMEM((HEAD_DIM, length), BF16),
            pltpu.VMEM((length, tile), F32),
            pltpu.VMEM((length, 2 * HEAD_DIM), F32),
            pltpu.VMEM((length, 2 * HEAD_DIM), BF16),
        ],
        compiler_params=pltpu.CompilerParams(vmem_limit_bytes=VMEM_BIG),
        name="attention",
    )(order, heads)


def finish_kernel(
    heads_ref, x_ref, cot_ref, gain_ref, wqkv_ref, wout_ref, bias_ref, mlp_a, mlp_b, gn_a, gn_b, tab_ref,
    out_ref, grad_in_ref, att_ref, gproj_ref, small_ref, bqkv_ref,
):
    tok, width = x_ref.shape
    tables = [tab_ref[i] for i in range(3)]
    low = lax.broadcasted_iota(jnp.int32, (tok, LANES), 1) < HEAD_DIM
    for pair in range(HEADS // 2):
        cols = slice(pair * LANES, (pair + 1) * LANES)
        even, odd = heads_ref[2 * pair].astype(F32), heads_ref[2 * pair + 1].astype(F32)
        att, gq = split_pair(even[:, :LANES], odd[:, :LANES], low)
        gk, gv = split_pair(even[:, LANES:], odd[:, LANES:], low)
        att_ref[:, cols] = att.astype(BF16)
        gproj_ref[:, pair * LANES : (pair + 1) * LANES] = rotate_tile(gq, tables, -1.0).astype(BF16)
        gproj_ref[:, width + pair * LANES : width + (pair + 1) * LANES] = rotate_tile(gk, tables, -1.0).astype(BF16)
        gproj_ref[:, 2 * width + pair * LANES : 2 * width + (pair + 1) * LANES] = gv.astype(BF16)
    rows = x_ref[...].astype(F32)
    cot = cot_ref[...].astype(F32)
    attn = dot_nn(att_ref[...], wout_ref[...])
    branch = mlp_a[...].astype(F32) + mlp_b[...].astype(F32)
    out_ref[...] = (rows + attn + branch + bias_ref[...]).astype(BF16)
    grad_normed = dot_nt(gproj_ref[...], wqkv_ref[...]) + gn_a[...].astype(F32) + gn_b[...].astype(F32)
    centre = jnp.mean(rows, axis=-1, keepdims=True)
    centred = rows - centre
    inv = lax.rsqrt(jnp.mean(centred * centred, axis=-1, keepdims=True) + EPSILON)
    unit = centred * inv
    small_ref[0:1, :] = jnp.sum(grad_normed * unit, axis=0, keepdims=True)
    small_ref[1:2, :] = jnp.sum(grad_normed, axis=0, keepdims=True)
    small_ref[2:3, :] = jnp.sum(cot, axis=0, keepdims=True)
    bqkv_ref[...] = jnp.sum(gproj_ref[...].astype(F32), axis=0, keepdims=True)
    grad_unit = grad_normed * gain_ref[...]
    grad_in_ref[...] = cot + inv * (
        grad_unit
        - jnp.mean(grad_unit, axis=-1, keepdims=True)
        - unit * jnp.mean(grad_unit * unit, axis=-1, keepdims=True)
    )


def finish(heads, x, cot, gain, w_qkv, w_out, bias, mlp_parts, gn_parts, tables):
    tok, width = x.shape
    vmem = pl.BlockSpec(memory_space=pltpu.VMEM)
    return pl.pallas_call(
        finish_kernel,
        out_shape=(
            jax.ShapeDtypeStruct((tok, width), BF16),
            jax.ShapeDtypeStruct((tok, width), F32),
            jax.ShapeDtypeStruct((tok, width), BF16),
            jax.ShapeDtypeStruct((tok, 3 * width), BF16),
            jax.ShapeDtypeStruct((8, width), F32),
            jax.ShapeDtypeStruct((1, 3 * width), F32),
        ),
        in_specs=[vmem] * 12,
        out_specs=(vmem,) * 6,
        compiler_params=pltpu.CompilerParams(vmem_limit_bytes=VMEM_BIG),
        name="finish",
    )(heads, x, cot, gain, w_qkv, w_out, bias, *mlp_parts, *gn_parts, tables)


def by_heads(
    block_input, span_offset, ln_gain, ln_bias, w_qkv, b_qkv, w_out, b_out, w_up, b_up, w_down, b_down, cotangent
):
    tok, width = block_input.shape[2:]
    spans = span_offset.shape[0]
    span_here = lax.axis_index("dp")
    seq_here = lax.axis_index("mlp")
    offsets = lax.dynamic_index_in_dim(span_offset, seq_here, axis=1, keepdims=False)
    places = jnp.arange(spans, dtype=jnp.int32)
    order = jnp.sum(jnp.where(offsets[None, :] == places[:, None], places[None, :], 0), axis=1)
    offset_here = lax.dynamic_index_in_dim(offsets, span_here, axis=0, keepdims=False)
    tables = rotary_tables(offset_here * tok + jnp.arange(tok, dtype=jnp.int32))
    x, cot = block_input[0, 0], cotangent[0, 0]
    gain, shift = ln_gain[None], ln_bias[None]

    normed, send = project(x, cot, gain, shift, w_qkv, b_qkv[None], w_out, tables)
    heads, (normed_peer, cot_peer) = exchange(send, (normed, cot), 0)

    normed_all = jnp.concatenate([normed, normed_peer])
    cot_all = jnp.concatenate([cot, cot_peer])
    up = dot_nn(normed_all, w_up) + b_up
    erf_part = 0.5 * (1.0 + lax.erf(up * SQRT_HALF))
    activated = (up * erf_part).astype(BF16)
    slope = erf_part + up * jnp.exp(-0.5 * up * up) * INV_ROOT_TWO_PI
    grad_up = (dot_nt(cot_all, w_down) * slope).astype(BF16)
    mlp_part = dot_nn(activated, w_down).astype(BF16)
    gn_part = dot_nt(grad_up, w_up).astype(BF16)
    grad_w_down = dot_tn(activated, cot_all).astype(BF16)
    grad_w_up = dot_tn(normed_all, grad_up).astype(BF16)
    grad_b_up = jnp.sum(grad_up.astype(F32), axis=0).astype(BF16)

    done = attention(heads, order)
    back, (mlp_other, gn_other) = exchange(done, (mlp_part[tok:], gn_part[tok:]), 1)
    output, grad_input, attended, grad_project, small, grad_b_qkv = finish(
        back, x, cot, gain, w_qkv, w_out, (b_out + b_down)[None],
        (mlp_part[:tok], mlp_other), (gn_part[:tok], gn_other), tables,
    )
    third = 3 * width // 2
    gp_here = lax.dynamic_slice_in_dim(grad_project, seq_here * third, third, axis=1)
    gp_give = lax.dynamic_slice_in_dim(grad_project, (1 - seq_here) * third, third, axis=1)
    att_peer, gp_peer = swap((attended, gp_give), 2)
    cot_cols = lax.dynamic_slice_in_dim(cot_all, seq_here * (width // 2), width // 2, axis=1)
    grad_w_qkv = dot_tn(normed_all, jnp.concatenate([gp_here, gp_peer])).astype(BF16)
    grad_w_out = dot_tn(jnp.concatenate([attended, att_peer]), cot_cols).astype(BF16)

    everyone = ("dp", "mlp")
    vec = jnp.concatenate([small[0], small[1], small[2], grad_b_qkv[0]])
    vec, b_up_sum, s_qkv, s_out, s_up, s_down = (
        lax.psum(vec, everyone),
        lax.psum(grad_b_up, "dp"),
        lax.psum(grad_w_qkv, "dp"),
        lax.psum(grad_w_out, "dp"),
        lax.psum(grad_w_up, "dp"),
        lax.psum(grad_w_down, "dp"),
    )
    half = width // 2
    piece = lambda start, size: lax.dynamic_slice_in_dim(vec, start + seq_here * size, size)
    bias_sum = piece(2 * width, half)
    return (
        output.reshape(1, 1, tok, width),
        grad_input.reshape(1, 1, tok, width),
        piece(0, half),
        piece(width, half),
        s_qkv.astype(F32),
        piece(3 * width, third),
        s_out.astype(F32),
        bias_sum,
        s_up.astype(F32),
        b_up_sum.astype(F32),
        s_down.astype(F32),
        bias_sum,
    )


def rotate(values, positions, sign_factor):
    half_rot = ROT // 2
    frequency = ROPE_BASE ** (-(jnp.arange(half_rot, dtype=jnp.float32) * 2.0 / ROT))
    angles = positions.astype(jnp.float32)[:, None] * frequency[None, :]
    cosine = jnp.cos(angles)[:, None, :]
    sine_part = sign_factor * jnp.sin(angles)[:, None, :]
    first_half = values[..., :half_rot]
    second_half = values[..., half_rot:ROT]
    return jnp.concatenate(
        [
            first_half * cosine - second_half * sine_part,
            second_half * cosine + first_half * sine_part,
            values[..., ROT:],
        ],
        axis=-1,
    )


def gelu_exact(values):
    return 0.5 * values * (1.0 + lax.erf(values * SQRT_HALF))


def gelu_slope(values):
    return (
        0.5 * (1.0 + lax.erf(values * SQRT_HALF))
        + values * jnp.exp(-0.5 * values * values) * INV_ROOT_TWO_PI
    )


def piece_count(total_rows):
    count_blocks = max(1, total_rows // 1024)
    while total_rows % count_blocks:
        count_blocks += 1
    return count_blocks


def row_positions(offsets, count_rows, tok_count):
    index_all = jnp.arange(count_rows, dtype=jnp.int32)
    span_of = index_all // tok_count
    within = index_all - span_of * tok_count
    matches = span_of[:, None] == jnp.arange(offsets.shape[0], dtype=jnp.int32)[None, :]
    offset_of = jnp.sum(jnp.where(matches, offsets[None, :], 0), axis=1)
    return offset_of * tok_count + within


def contract_rows(left_mat, right_mat):
    return lax.dot_general(
        left_mat, right_mat, (((0,), (0,)), ((), ())), preferred_element_type=jnp.float32
    )


def contract_cols(left_mat, right_mat):
    return lax.dot_general(
        left_mat, right_mat, (((1,), (1,)), ((), ())), preferred_element_type=jnp.float32
    )


def local(
    block_input,
    span_offset,
    ln_gain,
    ln_bias,
    w_qkv,
    b_qkv,
    w_out,
    b_out,
    w_up,
    b_up,
    w_down,
    b_down,
    cotangent,
):
    tok_count = block_input.shape[2]
    model_width = block_input.shape[3]
    scale_dot = 1.0 / math.sqrt(HEAD_DIM)
    span_here = lax.axis_index("dp")
    seq_here = lax.axis_index("mlp")
    offsets = lax.dynamic_index_in_dim(span_offset, seq_here, axis=1, keepdims=False)
    offset_here = lax.dynamic_index_in_dim(offsets, span_here, axis=0, keepdims=False)
    positions = offset_here * tok_count + jnp.arange(tok_count, dtype=jnp.int32)
    row_data = block_input[0, 0].astype(jnp.float32)
    centre = jnp.mean(row_data, axis=-1, keepdims=True)
    centred = row_data - centre
    spread = jnp.mean(centred * centred, axis=-1, keepdims=True)
    inv_scale = lax.rsqrt(spread + EPSILON)
    unit_rows = centred * inv_scale
    normed = (unit_rows * ln_gain + ln_bias).astype(jnp.bfloat16)
    project = jnp.dot(normed, w_qkv, preferred_element_type=jnp.float32) + b_qkv
    queries = rotate(
        project[:, :model_width].reshape(tok_count, HEADS, HEAD_DIM), positions, 1.0
    ).astype(jnp.bfloat16)
    keys_here = rotate(
        project[:, model_width : 2 * model_width].reshape(tok_count, HEADS, HEAD_DIM),
        positions,
        1.0,
    ).astype(jnp.bfloat16)
    values_here = (
        project[:, 2 * model_width :].reshape(tok_count, HEADS, HEAD_DIM).astype(jnp.bfloat16)
    )
    keys_flat = keys_here.reshape(tok_count, model_width)
    values_flat = values_here.reshape(tok_count, model_width)
    start_state = (
        jnp.zeros((tok_count, HEADS, HEAD_DIM), jnp.float32),
        jnp.zeros((HEADS, tok_count), jnp.float32),
    )
    keys_piece = lax.all_gather(keys_flat, "dp", axis=0, tiled=True)
    values_piece = lax.all_gather(values_flat, "dp", axis=0, tiled=True)
    piece_rows = keys_piece.shape[0]
    blocks = piece_count(piece_rows)
    sub_rows = piece_rows // blocks
    key_pos = row_positions(offsets, piece_rows, tok_count)

    def attend_one_block(state_now, packed):
        keys_blk, values_blk, pos_blk = packed
        key_heads = keys_blk.reshape(sub_rows, HEADS, HEAD_DIM)
        value_heads = values_blk.reshape(sub_rows, HEADS, HEAD_DIM)
        scores = (
            jnp.einsum("qhd,khd->hqk", queries, key_heads, preferred_element_type=jnp.float32)
            * scale_dot
        )
        allowed = pos_blk[None, :] <= positions[:, None]
        weights_exp = jnp.where(allowed[None], jnp.exp(scores), 0.0)
        mixed_sum, totals = state_now
        mixed_sum = mixed_sum + jnp.einsum(
            "hqk,khd->qhd",
            weights_exp.astype(jnp.bfloat16),
            value_heads,
            preferred_element_type=jnp.float32,
        )
        return ((mixed_sum, totals + jnp.sum(weights_exp, axis=-1)), None)

    state_now, _unused = lax.scan(
        attend_one_block,
        start_state,
        (
            keys_piece.reshape(blocks, sub_rows, model_width),
            values_piece.reshape(blocks, sub_rows, model_width),
            key_pos.reshape(blocks, sub_rows),
        ),
    )
    mixed_sum, totals = state_now
    attended = mixed_sum / totals.T[:, :, None]
    attended_low = attended.reshape(tok_count, model_width).astype(jnp.bfloat16)
    attn_branch = jnp.dot(attended_low, w_out, preferred_element_type=jnp.float32) + b_out
    normed_all = lax.all_gather(normed, "mlp", axis=0, tiled=True)
    up_proj = jnp.dot(normed_all, w_up, preferred_element_type=jnp.float32) + b_up
    activated = gelu_exact(up_proj).astype(jnp.bfloat16)
    mlp_branch = (
        lax.psum_scatter(
            jnp.dot(activated, w_down, preferred_element_type=jnp.float32).astype(jnp.bfloat16),
            "mlp",
            scatter_dimension=0,
            tiled=True,
        ).astype(jnp.float32)
        + b_down
    )
    output = (row_data + attn_branch + mlp_branch).astype(jnp.bfloat16)
    grad_out = cotangent[0, 0]
    grad_w_out = contract_rows(attended_low, grad_out)
    grad_bias_out = jnp.sum(grad_out.astype(jnp.float32), axis=0)
    grad_all = lax.all_gather(grad_out, "mlp", axis=0, tiled=True)
    grad_w_down = contract_rows(activated, grad_all)
    grad_act = contract_cols(grad_all, w_down)
    grad_up = (grad_act * gelu_slope(up_proj)).astype(jnp.bfloat16)
    grad_w_up = contract_rows(normed_all, grad_up)
    grad_b_up = jnp.sum(grad_up.astype(jnp.float32), axis=0)
    grad_norm_mlp = lax.psum_scatter(
        contract_cols(grad_up, w_up).astype(jnp.bfloat16), "mlp", scatter_dimension=0, tiled=True
    ).astype(jnp.float32)
    grad_att = contract_cols(grad_out, w_out).reshape(tok_count, HEADS, HEAD_DIM)
    grad_mixed = (grad_att / totals.T[:, :, None]).astype(jnp.bfloat16)
    grad_totals = ((-jnp.sum(grad_att * attended, axis=-1)).T / totals).astype(jnp.bfloat16)
    grad_totals_wide = grad_totals.astype(jnp.float32)[:, :, None]
    zero_heads = jnp.zeros((tok_count, HEADS, HEAD_DIM), jnp.float32)
    grad_query_sum = zero_heads
    keys_piece = lax.all_gather(keys_flat, "dp", axis=0, tiled=True)
    values_piece = lax.all_gather(values_flat, "dp", axis=0, tiled=True)
    piece_rows = keys_piece.shape[0]
    blocks = piece_count(piece_rows)
    back_sub_rows = piece_rows // blocks
    key_pos = row_positions(offsets, piece_rows, tok_count)

    def back_one_block(running_sum, packed):
        keys_blk, values_blk, pos_blk = packed
        key_heads = keys_blk.reshape(back_sub_rows, HEADS, HEAD_DIM)
        value_heads = values_blk.reshape(back_sub_rows, HEADS, HEAD_DIM)
        scores = (
            jnp.einsum("qhd,khd->hqk", queries, key_heads, preferred_element_type=jnp.float32)
            * scale_dot
        )
        allowed = pos_blk[None, :] <= positions[:, None]
        weights_exp = jnp.where(allowed[None], jnp.exp(scores), 0.0)
        grad_exp = jnp.einsum(
            "qhd,khd->hqk", grad_mixed, value_heads, preferred_element_type=jnp.float32
        )
        grad_scores = (weights_exp * (grad_exp + grad_totals_wide)).astype(jnp.bfloat16)
        running_sum = running_sum + scale_dot * jnp.einsum(
            "hqk,khd->qhd", grad_scores, key_heads, preferred_element_type=jnp.float32
        )
        grad_key_blk = scale_dot * jnp.einsum(
            "hqk,qhd->khd", grad_scores, queries, preferred_element_type=jnp.float32
        )
        grad_value_blk = jnp.einsum(
            "hqk,qhd->khd",
            weights_exp.astype(jnp.bfloat16),
            grad_mixed,
            preferred_element_type=jnp.float32,
        )
        joined = jnp.concatenate(
            [
                grad_key_blk.reshape(back_sub_rows, model_width),
                grad_value_blk.reshape(back_sub_rows, model_width),
            ],
            axis=1,
        )
        return (running_sum, joined)

    grad_query_sum, stacked = lax.scan(
        back_one_block,
        grad_query_sum,
        (
            keys_piece.reshape(blocks, back_sub_rows, model_width),
            values_piece.reshape(blocks, back_sub_rows, model_width),
            key_pos.reshape(blocks, back_sub_rows),
        ),
    )
    grad_kv_sum = stacked.reshape(piece_rows, 2 * model_width)
    grad_kv = lax.psum_scatter(
        grad_kv_sum.astype(jnp.bfloat16), "dp", scatter_dimension=0, tiled=True
    ).astype(jnp.float32)
    grad_keys = grad_kv[:, :model_width].reshape(tok_count, HEADS, HEAD_DIM)
    grad_values = grad_kv[:, model_width:].reshape(tok_count, HEADS, HEAD_DIM)
    grad_query_pre = rotate(grad_query_sum, positions, -1.0).reshape(tok_count, model_width)
    grad_key_pre = rotate(grad_keys, positions, -1.0).reshape(tok_count, model_width)
    grad_project = jnp.concatenate(
        [grad_query_pre, grad_key_pre, grad_values.reshape(tok_count, model_width)], axis=1
    ).astype(jnp.bfloat16)
    grad_w_qkv = contract_rows(normed, grad_project)
    grad_b_qkv = jnp.sum(grad_project.astype(jnp.float32), axis=0)
    grad_normed = contract_cols(grad_project, w_qkv) + grad_norm_mlp
    grad_ln_gain = jnp.sum(grad_normed * unit_rows, axis=0)
    grad_ln_bias = jnp.sum(grad_normed, axis=0)
    grad_unit = grad_normed * ln_gain
    grad_rows = inv_scale * (
        grad_unit
        - jnp.mean(grad_unit, axis=-1, keepdims=True)
        - unit_rows * jnp.mean(grad_unit * unit_rows, axis=-1, keepdims=True)
    )
    grad_input = (grad_out.astype(jnp.float32) + grad_rows).reshape(1, 1, tok_count, model_width)
    part_qkv, part_out, part_bqkv, part_bias, part_gain, part_shift = (
        lax.psum_scatter(
            grad_w_qkv.astype(jnp.bfloat16), "mlp", scatter_dimension=1, tiled=True
        ).astype(jnp.float32),
        lax.psum_scatter(
            grad_w_out.astype(jnp.bfloat16), "mlp", scatter_dimension=1, tiled=True
        ).astype(jnp.float32),
        lax.psum_scatter(
            grad_b_qkv.astype(jnp.bfloat16), "mlp", scatter_dimension=0, tiled=True
        ).astype(jnp.float32),
        lax.psum_scatter(
            grad_bias_out.astype(jnp.bfloat16), "mlp", scatter_dimension=0, tiled=True
        ).astype(jnp.float32),
        lax.psum_scatter(
            grad_ln_gain.astype(jnp.bfloat16), "mlp", scatter_dimension=0, tiled=True
        ).astype(jnp.float32),
        lax.psum_scatter(
            grad_ln_bias.astype(jnp.bfloat16), "mlp", scatter_dimension=0, tiled=True
        ).astype(jnp.float32),
    )
    summed = (
        lax.psum(part_qkv.astype(jnp.bfloat16), "dp").astype(jnp.float32),
        lax.psum(part_out.astype(jnp.bfloat16), "dp").astype(jnp.float32),
        lax.psum(part_bqkv.astype(jnp.bfloat16), "dp").astype(jnp.float32),
        lax.psum(part_bias.astype(jnp.bfloat16), "dp").astype(jnp.float32),
        lax.psum(part_gain.astype(jnp.bfloat16), "dp").astype(jnp.float32),
        lax.psum(part_shift.astype(jnp.bfloat16), "dp").astype(jnp.float32),
        lax.psum(grad_w_up.astype(jnp.bfloat16), "dp").astype(jnp.float32),
        lax.psum(grad_b_up.astype(jnp.bfloat16), "dp").astype(jnp.float32),
        lax.psum(grad_w_down.astype(jnp.bfloat16), "dp").astype(jnp.float32),
    )
    return (
        output.reshape(1, 1, tok_count, model_width),
        grad_input,
        summed[4],
        summed[5],
        summed[0],
        summed[2],
        summed[1],
        summed[3],
        summed[6],
        summed[7],
        summed[8],
        summed[3],
    )


def solution(mesh):
    fits = mesh.shape["dp"] == HEADS and mesh.shape["mlp"] == 2
    return jax.shard_map(
        by_heads if fits else local,
        mesh=mesh,
        in_specs=(
            P("dp", "mlp", None, None),
            P(),
            P(),
            P(),
            P(),
            P(),
            P(),
            P(),
            P(None, "mlp"),
            P("mlp"),
            P("mlp", None),
            P(),
            P("dp", "mlp", None, None),
        ),
        out_specs=(
            P("dp", "mlp", None, None),
            P("dp", "mlp", None, None),
            P("mlp"),
            P("mlp"),
            P(None, "mlp"),
            P("mlp"),
            P(None, "mlp"),
            P("mlp"),
            P(None, "mlp"),
            P("mlp"),
            P("mlp", None),
            P("mlp"),
        ),
        check_vma=False,
    )
```

```python
import functools
import math

import jax
import jax.numpy as jnp
from jax import lax
from jax.experimental import pallas as pl
from jax.experimental.pallas import tpu as pltpu
from jax.sharding import PartitionSpec as P

HEADS = 16
HEAD_DIM = 64
ROT = 16

EPSILON = 1e-05
ROPE_BASE = 10000.0
SQRT_HALF = 1.0 / math.sqrt(2.0)
INV_ROOT_TWO_PI = 1.0 / math.sqrt(2.0 * math.pi)

MESH = pl.DeviceIdType.MESH
F32 = jnp.float32
BF16 = jnp.bfloat16
LANES = 128
VMEM_BIG = 60 * 1024 * 1024


def dot_nn(a, b):
    return lax.dot_general(a, b, (((1,), (0,)), ((), ())), preferred_element_type=F32)


def dot_nt(a, b):
    return lax.dot_general(a, b, (((1,), (1,)), ((), ())), preferred_element_type=F32)


def dot_tn(a, b):
    return lax.dot_general(a, b, (((0,), (0,)), ((), ())), preferred_element_type=F32)


def rotary_tables(positions):
    lane = jnp.arange(LANES, dtype=jnp.int32) % HEAD_DIM
    half = ROT // 2
    frequency = ROPE_BASE ** (-((lane % half).astype(F32) * 2.0 / ROT))
    angles = positions.astype(F32)[:, None] * frequency[None, :]
    cosine = jnp.where(lane < ROT, jnp.cos(angles), 1.0)
    sine = jnp.sin(angles)
    up = jnp.where(lane < half, -sine, 0.0)
    down = jnp.where((lane >= half) & (lane < ROT), sine, 0.0)
    return jnp.stack([cosine, up, down])


def rotate_tile(x, tables, sign):
    half = ROT // 2
    return (
        x * tables[0]
        + pltpu.roll(x, LANES - half, 1) * (tables[1] * sign)
        + pltpu.roll(x, half, 1) * (tables[2] * sign)
    )


def split_pair(first, second, low):
    swap_first = pltpu.roll(first, HEAD_DIM, 1)
    swap_second = pltpu.roll(second, HEAD_DIM, 1)
    return jnp.where(low, first, swap_second), jnp.where(low, swap_first, second)


def project_kernel(
    x_ref, cot_ref, gain_ref, shift_ref, wq_ref, wk_ref, wv_ref, bq_ref, bk_ref, bv_ref, wo_ref, tab_ref,
    normed_ref, send_ref,
):
    @pl.when(pl.program_id(0) == 0)
    def _():
        rows = x_ref[...].astype(F32)
        centre = jnp.mean(rows, axis=-1, keepdims=True)
        centred = rows - centre
        spread = jnp.mean(centred * centred, axis=-1, keepdims=True)
        unit = centred * lax.rsqrt(spread + EPSILON)
        normed_ref[...] = (unit * gain_ref[...] + shift_ref[...]).astype(BF16)

    normed = normed_ref[...]
    q = dot_nn(normed, wq_ref[...]) + bq_ref[...]
    k = dot_nn(normed, wk_ref[...]) + bk_ref[...]
    v = dot_nn(normed, wv_ref[...]) + bv_ref[...]
    grad_att = dot_nt(cot_ref[...], wo_ref[...])
    tables = [tab_ref[i] for i in range(3)]
    low = lax.broadcasted_iota(jnp.int32, (x_ref.shape[0], LANES), 1) < HEAD_DIM
    for tile in range(q.shape[1] // LANES):
        cols = slice(tile * LANES, (tile + 1) * LANES)
        q_tile = rotate_tile(q[:, cols], tables, 1.0)
        k_tile = rotate_tile(k[:, cols], tables, 1.0)
        qk = split_pair(q_tile, k_tile, low)
        vg = split_pair(v[:, cols], grad_att[:, cols], low)
        for side in range(2):
            send_ref[2 * tile + side, :, :LANES] = qk[side].astype(BF16)
            send_ref[2 * tile + side, :, LANES:] = vg[side].astype(BF16)


def project(x, cot, gain, shift, w_qkv, b_qkv, w_out, tables):
    tok, width = x.shape
    group = 256
    steps = width // group
    heads_step = group // HEAD_DIM
    const = lambda shape: pl.BlockSpec(shape, lambda g: (0,) * len(shape))
    w_spec = lambda part: pl.BlockSpec((width, group), lambda g: (0, part * steps + g))
    b_spec = lambda part: pl.BlockSpec((1, group), lambda g: (0, part * steps + g))
    return pl.pallas_call(
        project_kernel,
        grid=(steps,),
        out_shape=(
            jax.ShapeDtypeStruct((tok, width), BF16),
            jax.ShapeDtypeStruct((HEADS, tok, 4 * HEAD_DIM), BF16),
        ),
        in_specs=[
            const((tok, width)), const((tok, width)), const((1, width)), const((1, width)),
            w_spec(0), w_spec(1), w_spec(2), b_spec(0), b_spec(1), b_spec(2),
            pl.BlockSpec((group, width), lambda g: (g, 0)),
            const((3, tok, LANES)),
        ],
        out_specs=(
            const((tok, width)),
            pl.BlockSpec((heads_step, tok, 4 * HEAD_DIM), lambda g: (g, 0, 0)),
        ),
        name="project",
    )(x, cot, gain, shift, w_qkv, w_qkv, w_qkv, b_qkv, b_qkv, b_qkv, w_out, tables)


def exchange_kernel(count, peers, blocks, *refs):
    heads_in, rest = refs[0], refs[1:]
    pairs_in, rest = rest[:count], rest[count:]
    heads_out, rest = rest[0], rest[1:]
    pairs_out, rest = rest[:count], rest[count:]
    head_send, head_recv, pair_send, pair_recv, local_sem = rest
    me = lax.axis_index("dp")
    other = 1 - lax.axis_index("mlp")
    barrier = pltpu.get_barrier_semaphore()
    for step in range(1, peers):
        pl.semaphore_signal(barrier, inc=1, device_id={"dp": lax.rem(me + step, peers)}, device_id_type=MESH)
    if count:
        pl.semaphore_signal(barrier, inc=1, device_id={"mlp": other}, device_id_type=MESH)
    pl.semaphore_wait(barrier, peers - 1 + (1 if count else 0))
    copies = []
    for i in range(count):
        copies.append(
            pltpu.make_async_remote_copy(
                src_ref=pairs_in[i], dst_ref=pairs_out[i], send_sem=pair_send.at[i], recv_sem=pair_recv.at[i],
                device_id={"mlp": other}, device_id_type=MESH,
            )
        )
    for step in range(1, peers):
        target = lax.rem(me + step, peers)
        copies.append(
            pltpu.make_async_remote_copy(
                src_ref=heads_in.at[target], dst_ref=heads_out.at[me],
                send_sem=head_send.at[step], recv_sem=head_recv.at[step],
                device_id={"dp": target}, device_id_type=MESH,
            )
        )
    for copy in copies:
        copy.start()
    own = pltpu.make_async_copy(heads_in.at[me], heads_out.at[me], local_sem)
    own.start()
    own.wait()
    for copy in copies:
        copy.wait()


def exchange(heads, pairs, collective):
    count = len(pairs)
    peers = heads.shape[0]
    any_spec = pl.BlockSpec(memory_space=pl.ANY)
    out = pl.pallas_call(
        functools.partial(exchange_kernel, count, peers, None),
        out_shape=(jax.ShapeDtypeStruct(heads.shape, heads.dtype),)
        + tuple(jax.ShapeDtypeStruct(p.shape, p.dtype) for p in pairs),
        in_specs=[any_spec] * (1 + count),
        out_specs=(any_spec,) * (1 + count),
        scratch_shapes=[
            pltpu.SemaphoreType.DMA((peers,)),
            pltpu.SemaphoreType.DMA((peers,)),
            pltpu.SemaphoreType.DMA((max(count, 1),)),
            pltpu.SemaphoreType.DMA((max(count, 1),)),
            pltpu.SemaphoreType.DMA,
        ],
        compiler_params=pltpu.CompilerParams(collective_id=collective, has_side_effects=True),
        name="exchange" + str(collective),
    )(heads, *pairs)
    return out[0], out[1:]


def swap_kernel(count, *refs):
    ins, outs = refs[:count], refs[count : 2 * count]
    send, recv = refs[2 * count :]
    other = 1 - lax.axis_index("mlp")
    barrier = pltpu.get_barrier_semaphore()
    pl.semaphore_signal(barrier, inc=1, device_id={"mlp": other}, device_id_type=MESH)
    pl.semaphore_wait(barrier, 1)
    copies = [
        pltpu.make_async_remote_copy(
            src_ref=ins[i], dst_ref=outs[i], send_sem=send.at[i], recv_sem=recv.at[i],
            device_id={"mlp": other}, device_id_type=MESH,
        )
        for i in range(count)
    ]
    for copy in copies:
        copy.start()
    for copy in copies:
        copy.wait()


def swap(arrays, collective):
    count = len(arrays)
    any_spec = pl.BlockSpec(memory_space=pl.ANY)
    return pl.pallas_call(
        functools.partial(swap_kernel, count),
        out_shape=tuple(jax.ShapeDtypeStruct(a.shape, a.dtype) for a in arrays),
        in_specs=[any_spec] * count,
        out_specs=(any_spec,) * count,
        scratch_shapes=[pltpu.SemaphoreType.DMA((count,)), pltpu.SemaphoreType.DMA((count,))],
        compiler_params=pltpu.CompilerParams(collective_id=collective, has_side_effects=True),
        name="swap" + str(collective),
    )(*arrays)


def attention_kernel(
    tile, order_ref, in_ref, out_ref,
    q_nat, k_nat, v_nat, k_tr, v_tr, g_tr, probs, kv_grad, aq_out,
):
    spans, tok, _ = in_ref.shape
    length = spans * tok
    blocks = length // tile
    scale = 1.0 / math.sqrt(HEAD_DIM)
    zeros = jnp.zeros((tok, HEAD_DIM), BF16)

    def gather(place, carry):
        span = order_ref[place]
        rows = pl.ds(pl.multiple_of(place * tok, tok), tok)
        data = in_ref[span]
        q_nat[rows, :] = jnp.concatenate([data[:, :HEAD_DIM] * jnp.asarray(scale, BF16), zeros], axis=1)
        k_nat[rows, :] = data[:, HEAD_DIM : 2 * HEAD_DIM]
        v_nat[rows, :] = data[:, 2 * HEAD_DIM : 3 * HEAD_DIM]
        return carry

    lax.fori_loop(0, spans, gather, 0)

    def gather_grad(place, carry):
        span = order_ref[place]
        rows = pl.ds(pl.multiple_of(place * tok, tok), tok)
        g_nat_rows = in_ref[span][:, 3 * HEAD_DIM :]
        aq_out[rows, :HEAD_DIM] = g_nat_rows
        return carry

    lax.fori_loop(0, spans, gather_grad, 0)

    def flip(block, carry):
        rows = pl.ds(pl.multiple_of(block * tile, tile), tile)
        k_tr[:, rows] = k_nat[rows, :].T
        v_tr[:, rows] = v_nat[rows, :].T
        g_tr[:, rows] = aq_out[rows, :HEAD_DIM].T
        kv_grad[rows, :] = jnp.zeros((tile, 2 * HEAD_DIM), F32)
        return carry

    lax.fori_loop(0, blocks, flip, 0)

    key_row = lax.broadcasted_iota(jnp.int32, (tile, tile), 0)
    query_col = lax.broadcasted_iota(jnp.int32, (tile, tile), 1)
    causal = key_row <= query_col
    pad = jnp.zeros((tile, HEAD_DIM), BF16)

    def query_block(block, carry):
        q_rows = pl.ds(pl.multiple_of(block * tile, tile), tile)
        queries_pad = q_nat[q_rows, :]
        queries = queries_pad[:, :HEAD_DIM]

        def forward(j, state, masked):
            mixed, totals = state
            rows = pl.ds(pl.multiple_of(j * tile, tile), tile)
            prob = jnp.exp(dot_nt(k_nat[rows, :], queries))
            if masked:
                prob = jnp.where(causal, prob, 0.0)
            probs[rows, :] = prob
            mixed = mixed + dot_nn(v_tr[:, rows], prob.astype(BF16))
            totals = totals + jnp.sum(prob.reshape(tile // 8, 8, tile), axis=0)
            return mixed, totals

        state = (jnp.zeros((HEAD_DIM, tile), F32), jnp.zeros((8, tile), F32))
        state = lax.fori_loop(0, block, lambda j, s: forward(j, s, False), state)
        mixed, totals = forward(block, state, True)
        totals = jnp.sum(totals, axis=0, keepdims=True)
        attended = mixed / totals
        grad_att = g_tr[:, q_rows].astype(F32)
        grad_mixed = (grad_att / totals).astype(BF16)
        grad_totals = (-jnp.sum(grad_att * attended, axis=0, keepdims=True) / totals).astype(BF16).astype(F32)
        grad_pad = jnp.concatenate([pad, grad_mixed.T], axis=1)

        def backward(j, grad_q):
            rows = pl.ds(pl.multiple_of(j * tile, tile), tile)
            prob = probs[rows, :]
            grad_scores = (prob * (dot_nn(v_nat[rows, :], grad_mixed) + grad_totals)).astype(BF16)
            kv_grad[rows, :] += dot_nn(grad_scores, queries_pad) + dot_nn(prob.astype(BF16), grad_pad)
            return grad_q + dot_nn(k_tr[:, rows], grad_scores)

        grad_q = lax.fori_loop(0, block + 1, backward, jnp.zeros((HEAD_DIM, tile), F32))
        aq_out[q_rows, :] = jnp.concatenate([attended, grad_q * scale], axis=0).T.astype(BF16)
        return carry

    lax.fori_loop(0, blocks, query_block, 0)

    def scatter(place, carry):
        span = order_ref[place]
        rows = pl.ds(pl.multiple_of(place * tok, tok), tok)
        out_ref[span, :, : 2 * HEAD_DIM] = aq_out[rows, :]
        out_ref[span, :, 2 * HEAD_DIM :] = kv_grad[rows, :].astype(BF16)
        return carry

    lax.fori_loop(0, spans, scatter, 0)


def attention(heads, order):
    spans, tok, width = heads.shape
    length = spans * tok
    tile = 256
    vmem = pl.BlockSpec(memory_space=pltpu.VMEM)
    return pl.pallas_call(
        functools.partial(attention_kernel, tile),
        out_shape=jax.ShapeDtypeStruct(heads.shape, BF16),
        in_specs=[pl.BlockSpec(memory_space=pltpu.SMEM), vmem],
        out_specs=vmem,
        scratch_shapes=[
            pltpu.VMEM((length, 2 * HEAD_DIM), BF16),
            pltpu.VMEM((length, HEAD_DIM), BF16),
            pltpu.VMEM((length, HEAD_DIM), BF16),
            pltpu.VMEM((HEAD_DIM, length), BF16),
            pltpu.VMEM((HEAD_DIM, length), BF16),
            pltpu.VMEM((HEAD_DIM, length), BF16),
            pltpu.VMEM((length, tile), F32),
            pltpu.VMEM((length, 2 * HEAD_DIM), F32),
            pltpu.VMEM((length, 2 * HEAD_DIM), BF16),
        ],
        compiler_params=pltpu.CompilerParams(vmem_limit_bytes=VMEM_BIG),
        name="attention",
    )(order, heads)


def finish_kernel(
    heads_ref, x_ref, cot_ref, gain_ref, wqkv_ref, wout_ref, bias_ref, mlp_a, mlp_b, gn_a, gn_b, tab_ref,
    out_ref, grad_in_ref, att_ref, gproj_ref, small_ref,
):
    tok, width = x_ref.shape
    tables = [tab_ref[i] for i in range(3)]
    low = lax.broadcasted_iota(jnp.int32, (tok, LANES), 1) < HEAD_DIM
    for pair in range(HEADS // 2):
        cols = slice(pair * LANES, (pair + 1) * LANES)
        even, odd = heads_ref[2 * pair].astype(F32), heads_ref[2 * pair + 1].astype(F32)
        att, gq = split_pair(even[:, :LANES], odd[:, :LANES], low)
        gk, gv = split_pair(even[:, LANES:], odd[:, LANES:], low)
        att_ref[:, cols] = att.astype(BF16)
        gproj_ref[:, pair * LANES : (pair + 1) * LANES] = rotate_tile(gq, tables, -1.0).astype(BF16)
        gproj_ref[:, width + pair * LANES : width + (pair + 1) * LANES] = rotate_tile(gk, tables, -1.0).astype(BF16)
        gproj_ref[:, 2 * width + pair * LANES : 2 * width + (pair + 1) * LANES] = gv.astype(BF16)
    rows = x_ref[...].astype(F32)
    cot = cot_ref[...].astype(F32)
    attn = dot_nn(att_ref[...], wout_ref[...])
    branch = mlp_a[...].astype(F32) + mlp_b[...].astype(F32)
    out_ref[...] = (rows + attn + branch + bias_ref[...]).astype(BF16)
    grad_normed = dot_nt(gproj_ref[...], wqkv_ref[...]) + gn_a[...].astype(F32) + gn_b[...].astype(F32)
    centre = jnp.mean(rows, axis=-1, keepdims=True)
    centred = rows - centre
    inv = lax.rsqrt(jnp.mean(centred * centred, axis=-1, keepdims=True) + EPSILON)
    unit = centred * inv
    small_ref[0:1, :] = jnp.sum(grad_normed * unit, axis=0, keepdims=True)
    small_ref[1:2, :] = jnp.sum(grad_normed, axis=0, keepdims=True)
    small_ref[2:3, :] = jnp.sum(cot, axis=0, keepdims=True)
    for part in range(3):
        part_cols = slice(part * width, (part + 1) * width)
        small_ref[3 + part : 4 + part, :] = jnp.sum(gproj_ref[:, part_cols].astype(F32), axis=0, keepdims=True)
    small_ref[6:8, :] = jnp.zeros((2, width), F32)
    grad_unit = grad_normed * gain_ref[...]
    grad_in_ref[...] = cot + inv * (
        grad_unit
        - jnp.mean(grad_unit, axis=-1, keepdims=True)
        - unit * jnp.mean(grad_unit * unit, axis=-1, keepdims=True)
    )


def finish(heads, x, cot, gain, w_qkv, w_out, bias, mlp_parts, gn_parts, tables):
    tok, width = x.shape
    vmem = pl.BlockSpec(memory_space=pltpu.VMEM)
    return pl.pallas_call(
        finish_kernel,
        out_shape=(
            jax.ShapeDtypeStruct((tok, width), BF16),
            jax.ShapeDtypeStruct((tok, width), F32),
            jax.ShapeDtypeStruct((tok, width), BF16),
            jax.ShapeDtypeStruct((tok, 3 * width), BF16),
            jax.ShapeDtypeStruct((8, width), F32),
        ),
        in_specs=[vmem] * 12,
        out_specs=(vmem,) * 5,
        compiler_params=pltpu.CompilerParams(vmem_limit_bytes=VMEM_BIG),
        name="finish",
    )(heads, x, cot, gain, w_qkv, w_out, bias, *mlp_parts, *gn_parts, tables)


CHUNK = 64


def feed_forward_kernel(
    normed_a, normed_b, cot_a, cot_b, wup_ref, bup_ref, wdown_ref,
    mlp_ref, gn_ref, gup_ref, gdown_ref, gbias_ref,
    normed_all, normed_tr, cot_all, mlp_acc, gn_acc,
):
    step = pl.program_id(0)
    tok = normed_a.shape[0]

    @pl.when(step == 0)
    def _():
        for ref, parts in ((normed_all, (normed_a, normed_b)), (cot_all, (cot_a, cot_b))):
            ref[:tok, :] = parts[0][...]
            ref[tok:, :] = parts[1][...]
        normed_tr[...] = normed_all[...].T
        mlp_acc[...] = jnp.zeros_like(mlp_acc)
        gn_acc[...] = jnp.zeros_like(gn_acc)

    w_up, w_down = wup_ref[...], wdown_ref[...]
    up = dot_nn(normed_all[...], w_up) + bup_ref[...]
    half_erf = 0.5 * (1.0 + lax.erf(up * SQRT_HALF))
    activated = (up * half_erf).astype(BF16)
    slope = half_erf + up * jnp.exp(-0.5 * up * up) * INV_ROOT_TWO_PI
    grad_up = (dot_nt(cot_all[...], w_down) * slope).astype(BF16)
    mlp_acc[...] += dot_nn(activated, w_down)
    gn_acc[...] += dot_nt(grad_up, w_up)
    gup_ref[...] = dot_nn(normed_tr[...], grad_up).astype(BF16).reshape(gup_ref.shape)
    gdown_ref[...] = dot_nn(activated.T, cot_all[...]).astype(BF16).reshape(gdown_ref.shape)
    gbias_ref[...] = jnp.sum(grad_up.astype(F32), axis=0, keepdims=True)

    @pl.when(step == pl.num_programs(0) - 1)
    def _():
        mlp_ref[...] = mlp_acc[...].astype(BF16)
        gn_ref[...] = gn_acc[...].astype(BF16)


def feed_forward(normed, normed_peer, cot, cot_peer, w_up, b_up, w_down):
    tok, width = normed.shape
    hidden = w_up.shape[1]
    group = 256
    steps = hidden // group
    per = width // group
    const = lambda shape: pl.BlockSpec(shape, lambda s: (0,) * len(shape))
    chunks = hidden // CHUNK
    return pl.pallas_call(
        feed_forward_kernel,
        grid=(steps,),
        out_shape=(
            jax.ShapeDtypeStruct((2 * tok, width), BF16),
            jax.ShapeDtypeStruct((2 * tok, width), BF16),
            jax.ShapeDtypeStruct((chunks, CHUNK, width), BF16),
            jax.ShapeDtypeStruct((chunks, CHUNK, width), BF16),
            jax.ShapeDtypeStruct((1, hidden), F32),
        ),
        in_specs=[const((tok, width))] * 4
        + [
            pl.BlockSpec((width, group), lambda s: (0, s)),
            pl.BlockSpec((1, group), lambda s: (0, s)),
            pl.BlockSpec((group, width), lambda s: (s, 0)),
        ],
        out_specs=(
            const((2 * tok, width)),
            const((2 * tok, width)),
            pl.BlockSpec((width // CHUNK, CHUNK, group), lambda s: (s // per, 0, s % per)),
            pl.BlockSpec((group // CHUNK, CHUNK, width), lambda s: (s, 0, 0)),
            pl.BlockSpec((1, group), lambda s: (0, s)),
        ),
        scratch_shapes=[
            pltpu.VMEM((2 * tok, width), BF16),
            pltpu.VMEM((width, 2 * tok), BF16),
            pltpu.VMEM((2 * tok, width), BF16),
            pltpu.VMEM((2 * tok, width), F32),
            pltpu.VMEM((2 * tok, width), F32),
        ],
        compiler_params=pltpu.CompilerParams(vmem_limit_bytes=VMEM_BIG),
        name="feed_forward",
    )(normed, normed_peer, cot, cot_peer, w_up, b_up, w_down)


def attention_weights_kernel(
    normed_a, normed_b, cot_a, cot_b, att_a, att_b, gproj_ref, gproj_peer, small_a, small_b, gbias_ref, out_ref,
):
    width = normed_a.shape[1]
    third = gproj_peer.shape[1]
    half = width // 2
    here = lax.axis_index("mlp")
    group = 512
    chunks = width // CHUNK
    normed_tr = jnp.concatenate([normed_a[...], normed_b[...]], axis=0).T
    for start in range(0, third, group):
        cols = pl.ds(pl.multiple_of(here * third + start, LANES), group)
        grads = jnp.concatenate([gproj_ref[:, cols], gproj_peer[:, start : start + group]], axis=0)
        block, at = start // width, start % width
        out_ref[block * chunks : (block + 1) * chunks, :, at : at + group] = (
            dot_nn(normed_tr, grads).astype(BF16).reshape(chunks, CHUNK, group)
        )
    cols = pl.ds(pl.multiple_of(here * half, LANES), half)
    att_tr = jnp.concatenate([att_a[...], att_b[...]], axis=0).T
    cots = jnp.concatenate([cot_a[:, cols], cot_b[:, cols]], axis=0)
    out_ref[chunks : 2 * chunks, :, half:] = dot_nn(att_tr, cots).astype(BF16).reshape(chunks, CHUNK, half)
    rows = small_a[...] + small_b[...]
    out_ref[2 * chunks] = jnp.concatenate(
        [rows[:6], gbias_ref[:, :width], gbias_ref[:, width:], jnp.zeros((CHUNK - 8, width), F32)], axis=0
    ).astype(BF16)
    out_ref[2 * chunks + 1] = jnp.zeros((CHUNK, width), BF16)


def attention_weights(*operands):
    width = operands[0].shape[1]
    vmem = pl.BlockSpec(memory_space=pltpu.VMEM)
    return pl.pallas_call(
        attention_weights_kernel,
        out_shape=jax.ShapeDtypeStruct((2 * (width // CHUNK) + 2, CHUNK, width), BF16),
        in_specs=[vmem] * len(operands),
        out_specs=vmem,
        compiler_params=pltpu.CompilerParams(vmem_limit_bytes=VMEM_BIG),
        name="attention_weights",
    )(*operands)


TREE_PERIOD = 10
TREE_SPINE = 0b0110101011
TREE_ROW = (0, 1, 0, 0, 1, 1, 0, 0, 1, 1)
TREE_ROOT = (1, 2, 0, 2, 3, 1, 2, 1, 2, 1)
TREE_SPAN = 4


def packed_table(values, bits):
    return sum(v << (bits * i) for i, v in enumerate(values))


def tree_roles(i, y, z):
    kind = lax.rem(i, TREE_PERIOD)
    bit = lambda table, bits: lax.bitwise_and(
        lax.shift_right_logical(jnp.int32(table), bits * kind), jnp.int32(2**bits - 1)
    )
    spine = bit(TREE_SPINE, 1) == 1
    row = bit(packed_table(TREE_ROW, 1), 1)
    root = bit(packed_table(TREE_ROOT, 2), 2)
    on_row = y == row
    along = jnp.logical_or(jnp.logical_not(spine), on_row)
    at_root = z == root
    left = jnp.logical_and(along, jnp.logical_and(z <= root, z > 0))
    right = jnp.logical_and(along, jnp.logical_and(z >= root, z < TREE_SPAN - 1))
    side = jnp.logical_and(on_row, jnp.logical_or(spine, at_root))
    to_side = jnp.logical_and(jnp.logical_not(on_row), jnp.logical_or(spine, at_root))
    to_right = jnp.logical_and(along, z < root)
    to_left = jnp.logical_and(along, z > root)
    is_root = jnp.logical_and(on_row, at_root)
    span = jnp.maximum(root, TREE_SPAN - 1 - root)
    base = jnp.where(spine, 1, 0)
    height = jnp.where(
        jnp.logical_and(spine, jnp.logical_not(on_row)), 0,
        base + jnp.where(z < root, z, jnp.where(z > root, TREE_SPAN - 1 - z, span)),
    )
    height = jnp.where(jnp.logical_and(jnp.logical_not(spine), is_root), span + 1, height)
    top = span + 1
    depth = top + jnp.abs(z - root) + jnp.where(on_row, 0, 1)
    return left, right, side, to_left, to_right, to_side, is_root, height, depth


def reduce_kernel(lag, counts, *refs):
    ins, rest = refs[: len(counts)], refs[len(counts) :]
    out = rest[0]
    own, sib, from_left, from_right, from_side, acc = rest[1:7]
    (own_sem, give_sem, sib_recv, up_send, left_recv, right_recv, side_recv, res_recv, pair_recv,
     keep_sem, down_left, down_right, down_side, down_pair) = rest[7:]
    total = own.shape[0]
    me = lax.axis_index("dp")
    core = lax.rem(me, 2)
    y = lax.rem(me // 2, 2)
    z = me // 4
    pair = me + 1 - 2 * core
    flip = me + 2 - 4 * y
    barrier = pltpu.get_barrier_semaphore()
    go = lambda device: pl.semaphore_signal(barrier, inc=1, device_id={"dp": device}, device_id_type=MESH)
    go(pair)
    go(flip)

    @pl.when(z > 0)
    def _():
        go(me - 4)

    @pl.when(z < TREE_SPAN - 1)
    def _():
        go(me + 4)

    pl.semaphore_wait(barrier, 2 + jnp.where(z > 0, 1, 0) + jnp.where(z < TREE_SPAN - 1, 1, 0))

    remote = lambda src, dst, send, recv, device: pltpu.make_async_remote_copy(
        src_ref=src, dst_ref=dst, send_sem=send, recv_sem=recv, device_id={"dp": device}, device_id_type=MESH
    )
    starts = [sum(counts[:n]) for n in range(len(counts))]
    give = lambda n, i: remote(ins[n].at[2 * (i - starts[n]) + 1 - core], sib.at[i], give_sem.at[i], sib_recv.at[i], pair)
    load = lambda n, i: pltpu.make_async_copy(ins[n].at[2 * (i - starts[n]) + core], own.at[i], own_sem.at[i])

    for n, count in enumerate(counts):
        def begin(i, carry, n=n):
            give(n, i).start()
            load(n, i).start()
            return carry

        lax.fori_loop(starts[n], starts[n] + count, begin, 0)

    up = {
        "left": lambda i: remote(own.at[i], from_right.at[i], up_send.at[i], right_recv.at[i], me - 4),
        "right": lambda i: remote(own.at[i], from_left.at[i], up_send.at[i], left_recv.at[i], me + 4),
        "side": lambda i: remote(own.at[i], from_side.at[i], up_send.at[i], side_recv.at[i], flip),
    }
    slot = lambda i: out.at[2 * i + core]
    down = {
        "left": lambda src, i: remote(src, slot(i), down_left.at[i], res_recv.at[i], me - 4),
        "right": lambda src, i: remote(src, slot(i), down_right.at[i], res_recv.at[i], me + 4),
        "side": lambda src, i: remote(src, slot(i), down_side.at[i], res_recv.at[i], flip),
        "pair": lambda src, i: remote(src, slot(i), down_pair.at[i], pair_recv.at[i], pair),
    }
    keep = lambda i: pltpu.make_async_copy(own.at[i], slot(i), keep_sem.at[i])

    def spread(src, i, left, right, side):
        for name, there in (("left", left), ("right", right), ("side", side)):
            @pl.when(there)
            def _(name=name):
                down[name](src, i).start()

        down["pair"](src, i).start()

    def ascend(i, roles):
        left, right, side, to_left, to_right, to_side, is_root, _, _ = roles
        pltpu.make_async_copy(own.at[i], own.at[i], own_sem.at[i]).wait()
        remote(own.at[i], sib.at[i], give_sem.at[i], sib_recv.at[i], pair).wait_recv()
        acc[...] = own[i].astype(F32) + sib[i].astype(F32)
        for there, land, sem in ((left, from_left, left_recv), (right, from_right, right_recv), (side, from_side, side_recv)):
            @pl.when(there)
            def _(land=land, sem=sem):
                remote(own.at[i], land.at[i], give_sem.at[i], sem.at[i], pair).wait_recv()
                acc[...] += land[i].astype(F32)

        own[i] = acc[...].astype(BF16)
        for name, there in (("left", to_left), ("right", to_right), ("side", to_side)):
            @pl.when(there)
            def _(name=name):
                up[name](i).start()

        @pl.when(is_root)
        def _():
            keep(i).start()
            spread(own.at[i], i, left, right, side)

    def descend(i, roles):
        left, right, side = roles[:3]
        remote(own.at[i], slot(i), give_sem.at[i], res_recv.at[i], pair).wait_recv()
        spread(slot(i), i, left, right, side)

    highest, deepest = TREE_SPAN, 2 * TREE_SPAN

    def tick(t, carry):
        for level in range(highest + 1):
            i = t - lag * level
            roles = tree_roles(jnp.maximum(i, 0), y, z)

            @pl.when(jnp.logical_and(jnp.logical_and(i >= 0, i < total), roles[7] == level))
            def _(i=i, roles=roles):
                ascend(i, roles)

        for level in range(2, deepest + 1):
            i = t - lag * level
            roles = tree_roles(jnp.maximum(i, 0), y, z)
            here = jnp.logical_and(roles[8] == level, jnp.logical_not(roles[6]))

            @pl.when(jnp.logical_and(jnp.logical_and(i >= 0, i < total), here))
            def _(i=i, roles=roles):
                descend(i, roles)

        return carry

    lax.fori_loop(0, total + lag * deepest, tick, 0)

    def drain(i, carry):
        left, right, side, to_left, to_right, to_side, is_root, _, _ = tree_roles(i, y, z)
        remote(own.at[i], sib.at[i], give_sem.at[i], sib_recv.at[i], pair).wait_send()

        @pl.when(jnp.logical_not(is_root))
        def _():
            up["side"](i).wait_send()

        @pl.when(is_root)
        def _():
            keep(i).wait()

        for name, there in (("left", left), ("right", right), ("side", side)):
            @pl.when(there)
            def _(name=name):
                down[name](own.at[i], i).wait_send()

        down["pair"](own.at[i], i).wait_send()
        remote(own.at[i], out.at[2 * i + 1 - core], give_sem.at[i], pair_recv.at[i], pair).wait_recv()
        return carry

    lax.fori_loop(0, total, drain, 0)


def reduce_chunks(arrays, collective, lag=4):
    counts = tuple(a.shape[0] // 2 for a in arrays)
    total = sum(counts)
    chunk = arrays[0].shape[1:]
    any_spec = pl.BlockSpec(memory_space=pl.ANY)
    return pl.pallas_call(
        functools.partial(reduce_kernel, lag, counts),
        out_shape=jax.ShapeDtypeStruct((2 * total,) + chunk, BF16),
        in_specs=[any_spec] * len(arrays),
        out_specs=any_spec,
        scratch_shapes=[pltpu.VMEM((total,) + chunk, BF16)] * 5
        + [pltpu.VMEM(chunk, F32)]
        + [pltpu.SemaphoreType.DMA((total,))] * 14,
        compiler_params=pltpu.CompilerParams(
            collective_id=collective, has_side_effects=True, vmem_limit_bytes=VMEM_BIG
        ),
        name="reduce" + str(collective),
    )(*arrays)


def by_heads(
    block_input, span_offset, ln_gain, ln_bias, w_qkv, b_qkv, w_out, b_out, w_up, b_up, w_down, b_down, cotangent
):
    tok, width = block_input.shape[2:]
    spans = span_offset.shape[0]
    span_here = lax.axis_index("dp")
    seq_here = lax.axis_index("mlp")
    offsets = lax.dynamic_index_in_dim(span_offset, seq_here, axis=1, keepdims=False)
    places = jnp.arange(spans, dtype=jnp.int32)
    order = jnp.sum(jnp.where(offsets[None, :] == places[:, None], places[None, :], 0), axis=1)
    offset_here = lax.dynamic_index_in_dim(offsets, span_here, axis=0, keepdims=False)
    tables = rotary_tables(offset_here * tok + jnp.arange(tok, dtype=jnp.int32))
    x, cot = block_input[0, 0], cotangent[0, 0]
    gain, shift = ln_gain[None], ln_bias[None]

    normed, send = project(x, cot, gain, shift, w_qkv, b_qkv[None], w_out, tables)
    heads, (normed_peer, cot_peer) = exchange(send, (normed, cot), 0)
    mlp_part, gn_part, sum_up, sum_down, grad_b_up = feed_forward(
        normed, normed_peer, cot, cot_peer, w_up, b_up[None], w_down
    )
    done = attention(heads, order)
    back, (mlp_other, gn_other) = exchange(done, (mlp_part[tok:], gn_part[tok:]), 1)
    output, grad_input, attended, grad_project, small = finish(
        back, x, cot, gain, w_qkv, w_out, (b_out + b_down)[None],
        (mlp_part[:tok], mlp_other), (gn_part[:tok], gn_other), tables,
    )
    third = 3 * width // 2
    half = width // 2
    give = lax.dynamic_slice_in_dim(grad_project, (1 - seq_here) * third, third, axis=1)
    att_peer, gproj_peer, small_peer = swap((attended, give, small), 2)
    sum_att = attention_weights(
        normed, normed_peer, cot, cot_peer, attended, att_peer, grad_project, gproj_peer, small, small_peer, grad_b_up
    )
    summed = reduce_chunks((sum_up, sum_down, sum_att), 3)
    block = lambda n: summed[n * (width // CHUNK) : (n + 1) * (width // CHUNK)].reshape(width, width).astype(F32)
    vec = summed[6 * (width // CHUNK), :8].astype(F32)
    piece = lambda rows, size: lax.dynamic_slice_in_dim(vec[rows].reshape(-1), seq_here * size, size)
    bias_sum = piece(slice(2, 3), half)
    last = block(5)
    return (
        output.reshape(1, 1, tok, width),
        grad_input.reshape(1, 1, tok, width),
        piece(slice(0, 1), half),
        piece(slice(1, 2), half),
        jnp.concatenate([block(4), last[:, :half]], axis=1),
        piece(slice(3, 6), third),
        last[:, half:],
        bias_sum,
        jnp.concatenate([block(0), block(1)], axis=1),
        vec[6:8].reshape(-1),
        jnp.concatenate([block(2), block(3)], axis=0),
        bias_sum,
    )


def rotate(values, positions, sign_factor):
    half_rot = ROT // 2
    frequency = ROPE_BASE ** (-(jnp.arange(half_rot, dtype=jnp.float32) * 2.0 / ROT))
    angles = positions.astype(jnp.float32)[:, None] * frequency[None, :]
    cosine = jnp.cos(angles)[:, None, :]
    sine_part = sign_factor * jnp.sin(angles)[:, None, :]
    first_half = values[..., :half_rot]
    second_half = values[..., half_rot:ROT]
    return jnp.concatenate(
        [
            first_half * cosine - second_half * sine_part,
            second_half * cosine + first_half * sine_part,
            values[..., ROT:],
        ],
        axis=-1,
    )


def gelu_exact(values):
    return 0.5 * values * (1.0 + lax.erf(values * SQRT_HALF))


def gelu_slope(values):
    return (
        0.5 * (1.0 + lax.erf(values * SQRT_HALF))
        + values * jnp.exp(-0.5 * values * values) * INV_ROOT_TWO_PI
    )


def piece_count(total_rows):
    count_blocks = max(1, total_rows // 1024)
    while total_rows % count_blocks:
        count_blocks += 1
    return count_blocks


def row_positions(offsets, count_rows, tok_count):
    index_all = jnp.arange(count_rows, dtype=jnp.int32)
    span_of = index_all // tok_count
    within = index_all - span_of * tok_count
    matches = span_of[:, None] == jnp.arange(offsets.shape[0], dtype=jnp.int32)[None, :]
    offset_of = jnp.sum(jnp.where(matches, offsets[None, :], 0), axis=1)
    return offset_of * tok_count + within


def contract_rows(left_mat, right_mat):
    return lax.dot_general(
        left_mat, right_mat, (((0,), (0,)), ((), ())), preferred_element_type=jnp.float32
    )


def contract_cols(left_mat, right_mat):
    return lax.dot_general(
        left_mat, right_mat, (((1,), (1,)), ((), ())), preferred_element_type=jnp.float32
    )


def local(
    block_input,
    span_offset,
    ln_gain,
    ln_bias,
    w_qkv,
    b_qkv,
    w_out,
    b_out,
    w_up,
    b_up,
    w_down,
    b_down,
    cotangent,
):
    tok_count = block_input.shape[2]
    model_width = block_input.shape[3]
    scale_dot = 1.0 / math.sqrt(HEAD_DIM)
    span_here = lax.axis_index("dp")
    seq_here = lax.axis_index("mlp")
    offsets = lax.dynamic_index_in_dim(span_offset, seq_here, axis=1, keepdims=False)
    offset_here = lax.dynamic_index_in_dim(offsets, span_here, axis=0, keepdims=False)
    positions = offset_here * tok_count + jnp.arange(tok_count, dtype=jnp.int32)
    row_data = block_input[0, 0].astype(jnp.float32)
    centre = jnp.mean(row_data, axis=-1, keepdims=True)
    centred = row_data - centre
    spread = jnp.mean(centred * centred, axis=-1, keepdims=True)
    inv_scale = lax.rsqrt(spread + EPSILON)
    unit_rows = centred * inv_scale
    normed = (unit_rows * ln_gain + ln_bias).astype(jnp.bfloat16)
    project = jnp.dot(normed, w_qkv, preferred_element_type=jnp.float32) + b_qkv
    queries = rotate(
        project[:, :model_width].reshape(tok_count, HEADS, HEAD_DIM), positions, 1.0
    ).astype(jnp.bfloat16)
    keys_here = rotate(
        project[:, model_width : 2 * model_width].reshape(tok_count, HEADS, HEAD_DIM),
        positions,
        1.0,
    ).astype(jnp.bfloat16)
    values_here = (
        project[:, 2 * model_width :].reshape(tok_count, HEADS, HEAD_DIM).astype(jnp.bfloat16)
    )
    keys_flat = keys_here.reshape(tok_count, model_width)
    values_flat = values_here.reshape(tok_count, model_width)
    start_state = (
        jnp.zeros((tok_count, HEADS, HEAD_DIM), jnp.float32),
        jnp.zeros((HEADS, tok_count), jnp.float32),
    )
    keys_piece = lax.all_gather(keys_flat, "dp", axis=0, tiled=True)
    values_piece = lax.all_gather(values_flat, "dp", axis=0, tiled=True)
    piece_rows = keys_piece.shape[0]
    blocks = piece_count(piece_rows)
    sub_rows = piece_rows // blocks
    key_pos = row_positions(offsets, piece_rows, tok_count)

    def attend_one_block(state_now, packed):
        keys_blk, values_blk, pos_blk = packed
        key_heads = keys_blk.reshape(sub_rows, HEADS, HEAD_DIM)
        value_heads = values_blk.reshape(sub_rows, HEADS, HEAD_DIM)
        scores = (
            jnp.einsum("qhd,khd->hqk", queries, key_heads, preferred_element_type=jnp.float32)
            * scale_dot
        )
        allowed = pos_blk[None, :] <= positions[:, None]
        weights_exp = jnp.where(allowed[None], jnp.exp(scores), 0.0)
        mixed_sum, totals = state_now
        mixed_sum = mixed_sum + jnp.einsum(
            "hqk,khd->qhd",
            weights_exp.astype(jnp.bfloat16),
            value_heads,
            preferred_element_type=jnp.float32,
        )
        return ((mixed_sum, totals + jnp.sum(weights_exp, axis=-1)), None)

    state_now, _unused = lax.scan(
        attend_one_block,
        start_state,
        (
            keys_piece.reshape(blocks, sub_rows, model_width),
            values_piece.reshape(blocks, sub_rows, model_width),
            key_pos.reshape(blocks, sub_rows),
        ),
    )
    mixed_sum, totals = state_now
    attended = mixed_sum / totals.T[:, :, None]
    attended_low = attended.reshape(tok_count, model_width).astype(jnp.bfloat16)
    attn_branch = jnp.dot(attended_low, w_out, preferred_element_type=jnp.float32) + b_out
    normed_all = lax.all_gather(normed, "mlp", axis=0, tiled=True)
    up_proj = jnp.dot(normed_all, w_up, preferred_element_type=jnp.float32) + b_up
    activated = gelu_exact(up_proj).astype(jnp.bfloat16)
    mlp_branch = (
        lax.psum_scatter(
            jnp.dot(activated, w_down, preferred_element_type=jnp.float32).astype(jnp.bfloat16),
            "mlp",
            scatter_dimension=0,
            tiled=True,
        ).astype(jnp.float32)
        + b_down
    )
    output = (row_data + attn_branch + mlp_branch).astype(jnp.bfloat16)
    grad_out = cotangent[0, 0]
    grad_w_out = contract_rows(attended_low, grad_out)
    grad_bias_out = jnp.sum(grad_out.astype(jnp.float32), axis=0)
    grad_all = lax.all_gather(grad_out, "mlp", axis=0, tiled=True)
    grad_w_down = contract_rows(activated, grad_all)
    grad_act = contract_cols(grad_all, w_down)
    grad_up = (grad_act * gelu_slope(up_proj)).astype(jnp.bfloat16)
    grad_w_up = contract_rows(normed_all, grad_up)
    grad_b_up = jnp.sum(grad_up.astype(jnp.float32), axis=0)
    grad_norm_mlp = lax.psum_scatter(
        contract_cols(grad_up, w_up).astype(jnp.bfloat16), "mlp", scatter_dimension=0, tiled=True
    ).astype(jnp.float32)
    grad_att = contract_cols(grad_out, w_out).reshape(tok_count, HEADS, HEAD_DIM)
    grad_mixed = (grad_att / totals.T[:, :, None]).astype(jnp.bfloat16)
    grad_totals = ((-jnp.sum(grad_att * attended, axis=-1)).T / totals).astype(jnp.bfloat16)
    grad_totals_wide = grad_totals.astype(jnp.float32)[:, :, None]
    zero_heads = jnp.zeros((tok_count, HEADS, HEAD_DIM), jnp.float32)
    grad_query_sum = zero_heads
    keys_piece = lax.all_gather(keys_flat, "dp", axis=0, tiled=True)
    values_piece = lax.all_gather(values_flat, "dp", axis=0, tiled=True)
    piece_rows = keys_piece.shape[0]
    blocks = piece_count(piece_rows)
    back_sub_rows = piece_rows // blocks
    key_pos = row_positions(offsets, piece_rows, tok_count)

    def back_one_block(running_sum, packed):
        keys_blk, values_blk, pos_blk = packed
        key_heads = keys_blk.reshape(back_sub_rows, HEADS, HEAD_DIM)
        value_heads = values_blk.reshape(back_sub_rows, HEADS, HEAD_DIM)
        scores = (
            jnp.einsum("qhd,khd->hqk", queries, key_heads, preferred_element_type=jnp.float32)
            * scale_dot
        )
        allowed = pos_blk[None, :] <= positions[:, None]
        weights_exp = jnp.where(allowed[None], jnp.exp(scores), 0.0)
        grad_exp = jnp.einsum(
            "qhd,khd->hqk", grad_mixed, value_heads, preferred_element_type=jnp.float32
        )
        grad_scores = (weights_exp * (grad_exp + grad_totals_wide)).astype(jnp.bfloat16)
        running_sum = running_sum + scale_dot * jnp.einsum(
            "hqk,khd->qhd", grad_scores, key_heads, preferred_element_type=jnp.float32
        )
        grad_key_blk = scale_dot * jnp.einsum(
            "hqk,qhd->khd", grad_scores, queries, preferred_element_type=jnp.float32
        )
        grad_value_blk = jnp.einsum(
            "hqk,qhd->khd",
            weights_exp.astype(jnp.bfloat16),
            grad_mixed,
            preferred_element_type=jnp.float32,
        )
        joined = jnp.concatenate(
            [
                grad_key_blk.reshape(back_sub_rows, model_width),
                grad_value_blk.reshape(back_sub_rows, model_width),
            ],
            axis=1,
        )
        return (running_sum, joined)

    grad_query_sum, stacked = lax.scan(
        back_one_block,
        grad_query_sum,
        (
            keys_piece.reshape(blocks, back_sub_rows, model_width),
            values_piece.reshape(blocks, back_sub_rows, model_width),
            key_pos.reshape(blocks, back_sub_rows),
        ),
    )
    grad_kv_sum = stacked.reshape(piece_rows, 2 * model_width)
    grad_kv = lax.psum_scatter(
        grad_kv_sum.astype(jnp.bfloat16), "dp", scatter_dimension=0, tiled=True
    ).astype(jnp.float32)
    grad_keys = grad_kv[:, :model_width].reshape(tok_count, HEADS, HEAD_DIM)
    grad_values = grad_kv[:, model_width:].reshape(tok_count, HEADS, HEAD_DIM)
    grad_query_pre = rotate(grad_query_sum, positions, -1.0).reshape(tok_count, model_width)
    grad_key_pre = rotate(grad_keys, positions, -1.0).reshape(tok_count, model_width)
    grad_project = jnp.concatenate(
        [grad_query_pre, grad_key_pre, grad_values.reshape(tok_count, model_width)], axis=1
    ).astype(jnp.bfloat16)
    grad_w_qkv = contract_rows(normed, grad_project)
    grad_b_qkv = jnp.sum(grad_project.astype(jnp.float32), axis=0)
    grad_normed = contract_cols(grad_project, w_qkv) + grad_norm_mlp
    grad_ln_gain = jnp.sum(grad_normed * unit_rows, axis=0)
    grad_ln_bias = jnp.sum(grad_normed, axis=0)
    grad_unit = grad_normed * ln_gain
    grad_rows = inv_scale * (
        grad_unit
        - jnp.mean(grad_unit, axis=-1, keepdims=True)
        - unit_rows * jnp.mean(grad_unit * unit_rows, axis=-1, keepdims=True)
    )
    grad_input = (grad_out.astype(jnp.float32) + grad_rows).reshape(1, 1, tok_count, model_width)
    part_qkv, part_out, part_bqkv, part_bias, part_gain, part_shift = (
        lax.psum_scatter(
            grad_w_qkv.astype(jnp.bfloat16), "mlp", scatter_dimension=1, tiled=True
        ).astype(jnp.float32),
        lax.psum_scatter(
            grad_w_out.astype(jnp.bfloat16), "mlp", scatter_dimension=1, tiled=True
        ).astype(jnp.float32),
        lax.psum_scatter(
            grad_b_qkv.astype(jnp.bfloat16), "mlp", scatter_dimension=0, tiled=True
        ).astype(jnp.float32),
        lax.psum_scatter(
            grad_bias_out.astype(jnp.bfloat16), "mlp", scatter_dimension=0, tiled=True
        ).astype(jnp.float32),
        lax.psum_scatter(
            grad_ln_gain.astype(jnp.bfloat16), "mlp", scatter_dimension=0, tiled=True
        ).astype(jnp.float32),
        lax.psum_scatter(
            grad_ln_bias.astype(jnp.bfloat16), "mlp", scatter_dimension=0, tiled=True
        ).astype(jnp.float32),
    )
    summed = (
        lax.psum(part_qkv.astype(jnp.bfloat16), "dp").astype(jnp.float32),
        lax.psum(part_out.astype(jnp.bfloat16), "dp").astype(jnp.float32),
        lax.psum(part_bqkv.astype(jnp.bfloat16), "dp").astype(jnp.float32),
        lax.psum(part_bias.astype(jnp.bfloat16), "dp").astype(jnp.float32),
        lax.psum(part_gain.astype(jnp.bfloat16), "dp").astype(jnp.float32),
        lax.psum(part_shift.astype(jnp.bfloat16), "dp").astype(jnp.float32),
        lax.psum(grad_w_up.astype(jnp.bfloat16), "dp").astype(jnp.float32),
        lax.psum(grad_b_up.astype(jnp.bfloat16), "dp").astype(jnp.float32),
        lax.psum(grad_w_down.astype(jnp.bfloat16), "dp").astype(jnp.float32),
    )
    return (
        output.reshape(1, 1, tok_count, model_width),
        grad_input,
        summed[4],
        summed[5],
        summed[0],
        summed[2],
        summed[1],
        summed[3],
        summed[6],
        summed[7],
        summed[8],
        summed[3],
    )


def solution(mesh):
    fits = mesh.shape["dp"] == HEADS and mesh.shape["mlp"] == 2
    return jax.shard_map(
        by_heads if fits else local,
        mesh=mesh,
        in_specs=(
            P("dp", "mlp", None, None),
            P(),
            P(),
            P(),
            P(),
            P(),
            P(),
            P(),
            P(None, "mlp"),
            P("mlp"),
            P("mlp", None),
            P(),
            P("dp", "mlp", None, None),
        ),
        out_specs=(
            P("dp", "mlp", None, None),
            P("dp", "mlp", None, None),
            P("mlp"),
            P("mlp"),
            P(None, "mlp"),
            P("mlp"),
            P(None, "mlp"),
            P("mlp"),
            P(None, "mlp"),
            P("mlp"),
            P("mlp", None),
            P("mlp"),
        ),
        check_vma=False,
    )
```

```python
import functools
import math

import jax
import jax.numpy as jnp
from jax import lax
from jax.experimental import pallas as pl
from jax.experimental.pallas import tpu as pltpu
from jax.sharding import PartitionSpec as P

HEADS = 16
HEAD_DIM = 64
ROT = 16

EPSILON = 1e-05
ROPE_BASE = 10000.0
SQRT_HALF = 1.0 / math.sqrt(2.0)
INV_ROOT_TWO_PI = 1.0 / math.sqrt(2.0 * math.pi)

MESH = pl.DeviceIdType.MESH
F32 = jnp.float32
BF16 = jnp.bfloat16
LANES = 128
VMEM_BIG = 60 * 1024 * 1024
TREE_LAG = 4
TREE_GAP = 12
TICKS_PER_BLOCK = 2
VMEM_ALL = 66 * 1024 * 1024 - 2**20 // 2


def dot_nn(a, b):
    return lax.dot_general(a, b, (((1,), (0,)), ((), ())), preferred_element_type=F32)


def dot_nt(a, b):
    return lax.dot_general(a, b, (((1,), (1,)), ((), ())), preferred_element_type=F32)


def dot_tn(a, b):
    return lax.dot_general(a, b, (((0,), (0,)), ((), ())), preferred_element_type=F32)


def rotary_tables(positions):
    lane = jnp.arange(LANES, dtype=jnp.int32) % HEAD_DIM
    half = ROT // 2
    frequency = ROPE_BASE ** (-((lane % half).astype(F32) * 2.0 / ROT))
    angles = positions.astype(F32)[:, None] * frequency[None, :]
    cosine = jnp.where(lane < ROT, jnp.cos(angles), 1.0)
    sine = jnp.sin(angles)
    up = jnp.where(lane < half, -sine, 0.0)
    down = jnp.where((lane >= half) & (lane < ROT), sine, 0.0)
    return jnp.stack([cosine, up, down])


def rotate_tile(x, tables, sign):
    half = ROT // 2
    return (
        x * tables[0]
        + pltpu.roll(x, LANES - half, 1) * (tables[1] * sign)
        + pltpu.roll(x, half, 1) * (tables[2] * sign)
    )


def split_pair(first, second, low):
    swap_first = pltpu.roll(first, HEAD_DIM, 1)
    swap_second = pltpu.roll(second, HEAD_DIM, 1)
    return jnp.where(low, first, swap_second), jnp.where(low, swap_first, second)


def project_kernel(
    x_ref, cot_ref, gain_ref, shift_ref, wq_ref, wk_ref, wv_ref, bq_ref, bk_ref, bv_ref, wo_ref, tab_ref,
    normed_ref, send_ref,
):
    @pl.when(pl.program_id(0) == 0)
    def _():
        rows = x_ref[...].astype(F32)
        centre = jnp.mean(rows, axis=-1, keepdims=True)
        centred = rows - centre
        spread = jnp.mean(centred * centred, axis=-1, keepdims=True)
        unit = centred * lax.rsqrt(spread + EPSILON)
        normed_ref[...] = (unit * gain_ref[...] + shift_ref[...]).astype(BF16)

    normed = normed_ref[...]
    q = dot_nn(normed, wq_ref[...]) + bq_ref[...]
    k = dot_nn(normed, wk_ref[...]) + bk_ref[...]
    v = dot_nn(normed, wv_ref[...]) + bv_ref[...]
    grad_att = dot_nt(cot_ref[...], wo_ref[...])
    tables = [tab_ref[i] for i in range(3)]
    low = lax.broadcasted_iota(jnp.int32, (x_ref.shape[0], LANES), 1) < HEAD_DIM
    for tile in range(q.shape[1] // LANES):
        cols = slice(tile * LANES, (tile + 1) * LANES)
        q_tile = rotate_tile(q[:, cols], tables, 1.0)
        k_tile = rotate_tile(k[:, cols], tables, 1.0)
        qk = split_pair(q_tile, k_tile, low)
        vg = split_pair(v[:, cols], grad_att[:, cols], low)
        for side in range(2):
            send_ref[2 * tile + side, :, :LANES] = qk[side].astype(BF16)
            send_ref[2 * tile + side, :, LANES:] = vg[side].astype(BF16)


def project(x, cot, gain, shift, w_qkv, b_qkv, w_out, tables):
    tok, width = x.shape
    group = 256
    steps = width // group
    heads_step = group // HEAD_DIM
    const = lambda shape: pl.BlockSpec(shape, lambda g: (0,) * len(shape))
    w_spec = lambda part: pl.BlockSpec((width, group), lambda g: (0, part * steps + g))
    b_spec = lambda part: pl.BlockSpec((1, group), lambda g: (0, part * steps + g))
    return pl.pallas_call(
        project_kernel,
        grid=(steps,),
        out_shape=(
            jax.ShapeDtypeStruct((tok, width), BF16),
            jax.ShapeDtypeStruct((HEADS, tok, 4 * HEAD_DIM), BF16),
        ),
        in_specs=[
            const((tok, width)), const((tok, width)), const((1, width)), const((1, width)),
            w_spec(0), w_spec(1), w_spec(2), b_spec(0), b_spec(1), b_spec(2),
            pl.BlockSpec((group, width), lambda g: (g, 0)),
            const((3, tok, LANES)),
        ],
        out_specs=(
            const((tok, width)),
            pl.BlockSpec((heads_step, tok, 4 * HEAD_DIM), lambda g: (g, 0, 0)),
        ),
        name="project",
    )(x, cot, gain, shift, w_qkv, w_qkv, w_qkv, b_qkv, b_qkv, b_qkv, w_out, tables)


def exchange_kernel(count, peers, blocks, *refs):
    heads_in, rest = refs[0], refs[1:]
    pairs_in, rest = rest[:count], rest[count:]
    heads_out, rest = rest[0], rest[1:]
    pairs_out, rest = rest[:count], rest[count:]
    head_send, head_recv, pair_send, pair_recv, local_sem = rest
    me = lax.axis_index("dp")
    other = 1 - lax.axis_index("mlp")
    barrier = pltpu.get_barrier_semaphore()
    for step in range(1, peers):
        pl.semaphore_signal(barrier, inc=1, device_id={"dp": lax.rem(me + step, peers)}, device_id_type=MESH)
    if count:
        pl.semaphore_signal(barrier, inc=1, device_id={"mlp": other}, device_id_type=MESH)
    pl.semaphore_wait(barrier, peers - 1 + (1 if count else 0))
    copies = []
    for i in range(count):
        copies.append(
            pltpu.make_async_remote_copy(
                src_ref=pairs_in[i], dst_ref=pairs_out[i], send_sem=pair_send.at[i], recv_sem=pair_recv.at[i],
                device_id={"mlp": other}, device_id_type=MESH,
            )
        )
    for step in range(1, peers):
        target = lax.rem(me + step, peers)
        copies.append(
            pltpu.make_async_remote_copy(
                src_ref=heads_in.at[target], dst_ref=heads_out.at[me],
                send_sem=head_send.at[step], recv_sem=head_recv.at[step],
                device_id={"dp": target}, device_id_type=MESH,
            )
        )
    for copy in copies:
        copy.start()
    own = pltpu.make_async_copy(heads_in.at[me], heads_out.at[me], local_sem)
    own.start()
    own.wait()
    for copy in copies:
        copy.wait()


def exchange(heads, pairs, collective):
    count = len(pairs)
    peers = heads.shape[0]
    any_spec = pl.BlockSpec(memory_space=pl.ANY)
    out = pl.pallas_call(
        functools.partial(exchange_kernel, count, peers, None),
        out_shape=(jax.ShapeDtypeStruct(heads.shape, heads.dtype),)
        + tuple(jax.ShapeDtypeStruct(p.shape, p.dtype) for p in pairs),
        in_specs=[any_spec] * (1 + count),
        out_specs=(any_spec,) * (1 + count),
        scratch_shapes=[
            pltpu.SemaphoreType.DMA((peers,)),
            pltpu.SemaphoreType.DMA((peers,)),
            pltpu.SemaphoreType.DMA((max(count, 1),)),
            pltpu.SemaphoreType.DMA((max(count, 1),)),
            pltpu.SemaphoreType.DMA,
        ],
        compiler_params=pltpu.CompilerParams(collective_id=collective, has_side_effects=True),
        name="exchange" + str(collective),
    )(heads, *pairs)
    return out[0], out[1:]


CHUNK = 64


def feed_forward_kernel(
    normed_a, normed_b, cot_a, cot_b, wup_ref, bup_ref, wdown_ref,
    mlp_ref, mlp_give, gn_ref, gn_give, gup_ref, gdown_ref, gbias_ref,
    normed_all, normed_tr, cot_all, mlp_acc, gn_acc,
):
    step = pl.program_id(0)
    tok = normed_a.shape[0]

    @pl.when(step == 0)
    def _():
        for ref, parts in ((normed_all, (normed_a, normed_b)), (cot_all, (cot_a, cot_b))):
            ref[:tok, :] = parts[0][...]
            ref[tok:, :] = parts[1][...]
        normed_tr[...] = normed_all[...].T
        mlp_acc[...] = jnp.zeros_like(mlp_acc)
        gn_acc[...] = jnp.zeros_like(gn_acc)

    w_up, w_down = wup_ref[...], wdown_ref[...]
    up = dot_nn(normed_all[...], w_up) + bup_ref[...]
    half_erf = 0.5 * (1.0 + lax.erf(up * SQRT_HALF))
    activated = (up * half_erf).astype(BF16)
    slope = half_erf + up * jnp.exp(-0.5 * up * up) * INV_ROOT_TWO_PI
    grad_up = (dot_nt(cot_all[...], w_down) * slope).astype(BF16)
    mlp_acc[...] += dot_nn(activated, w_down)
    gn_acc[...] += dot_nt(grad_up, w_up)
    gup_ref[...] = dot_nn(normed_tr[...], grad_up).astype(BF16).reshape(gup_ref.shape)
    gdown_ref[...] = dot_nn(activated.T, cot_all[...]).astype(BF16).reshape(gdown_ref.shape)
    gbias_ref[...] = jnp.sum(grad_up.astype(F32), axis=0, keepdims=True)

    @pl.when(step == pl.num_programs(0) - 1)
    def _():
        mlp_ref[...] = mlp_acc[:tok, :].astype(BF16)
        mlp_give[...] = mlp_acc[tok:, :].astype(BF16)
        gn_ref[...] = gn_acc[:tok, :].astype(BF16)
        gn_give[...] = gn_acc[tok:, :].astype(BF16)


def feed_forward(normed, normed_peer, cot, cot_peer, w_up, b_up, w_down):
    tok, width = normed.shape
    hidden = w_up.shape[1]
    group = 256
    steps = hidden // group
    per = width // group
    const = lambda shape: pl.BlockSpec(shape, lambda s: (0,) * len(shape))
    chunks = hidden // CHUNK
    return pl.pallas_call(
        feed_forward_kernel,
        grid=(steps,),
        out_shape=(jax.ShapeDtypeStruct((tok, width), BF16),) * 4
        + (
            jax.ShapeDtypeStruct((chunks, CHUNK, width), BF16),
            jax.ShapeDtypeStruct((chunks, CHUNK, width), BF16),
            jax.ShapeDtypeStruct((1, hidden), F32),
        ),
        in_specs=[const((tok, width))] * 4
        + [
            pl.BlockSpec((width, group), lambda s: (0, s)),
            pl.BlockSpec((1, group), lambda s: (0, s)),
            pl.BlockSpec((group, width), lambda s: (s, 0)),
        ],
        out_specs=(const((tok, width)),) * 4
        + (
            pl.BlockSpec((width // CHUNK, CHUNK, group), lambda s: (s // per, 0, s % per)),
            pl.BlockSpec((group // CHUNK, CHUNK, width), lambda s: (s, 0, 0)),
            pl.BlockSpec((1, group), lambda s: (0, s)),
        ),
        scratch_shapes=[
            pltpu.VMEM((2 * tok, width), BF16),
            pltpu.VMEM((width, 2 * tok), BF16),
            pltpu.VMEM((2 * tok, width), BF16),
            pltpu.VMEM((2 * tok, width), F32),
            pltpu.VMEM((2 * tok, width), F32),
        ],
        compiler_params=pltpu.CompilerParams(vmem_limit_bytes=VMEM_BIG),
        name="feed_forward",
    )(normed, normed_peer, cot, cot_peer, w_up, b_up, w_down)


TREE_PERIOD = 10
TREE_SPINE = 0b0110101011
TREE_ROW = (0, 1, 0, 0, 1, 1, 0, 0, 1, 1)
TREE_ROOT = (1, 2, 0, 2, 3, 1, 2, 1, 2, 1)
TREE_SPAN = 4


def packed_table(values, bits):
    return sum(v << (bits * i) for i, v in enumerate(values))


def tree_roles(i, y, z):
    kind = lax.rem(i, TREE_PERIOD)
    bit = lambda table, bits: lax.bitwise_and(
        lax.shift_right_logical(jnp.int32(table), bits * kind), jnp.int32(2**bits - 1)
    )
    spine = bit(TREE_SPINE, 1) == 1
    row = bit(packed_table(TREE_ROW, 1), 1)
    root = bit(packed_table(TREE_ROOT, 2), 2)
    on_row = y == row
    along = jnp.logical_or(jnp.logical_not(spine), on_row)
    at_root = z == root
    left = jnp.logical_and(along, jnp.logical_and(z <= root, z > 0))
    right = jnp.logical_and(along, jnp.logical_and(z >= root, z < TREE_SPAN - 1))
    side = jnp.logical_and(on_row, jnp.logical_or(spine, at_root))
    to_side = jnp.logical_and(jnp.logical_not(on_row), jnp.logical_or(spine, at_root))
    to_right = jnp.logical_and(along, z < root)
    to_left = jnp.logical_and(along, z > root)
    is_root = jnp.logical_and(on_row, at_root)
    span = jnp.maximum(root, TREE_SPAN - 1 - root)
    base = jnp.where(spine, 1, 0)
    height = jnp.where(
        jnp.logical_and(spine, jnp.logical_not(on_row)), 0,
        base + jnp.where(z < root, z, jnp.where(z > root, TREE_SPAN - 1 - z, span)),
    )
    height = jnp.where(jnp.logical_and(jnp.logical_not(spine), is_root), span + 1, height)
    top = span + 1
    depth = top + jnp.abs(z - root) + jnp.where(on_row, 0, 1)
    flags = (left, right, side, to_left, to_right, to_side, is_root)
    packed = sum(jnp.where(flag, 1 << n, 0) for n, flag in enumerate(flags))
    return packed + height * 128 + jnp.where(is_root, 0, depth) * 2048


def has(roles, n):
    return lax.bitwise_and(roles, jnp.int32(1 << n)) != 0


class Reducer:
    def __init__(self, sources, out, buffers, semaphores, lag, early, gap):
        self.sources, self.out, self.lag, self.early, self.gap = sources, out, lag, early, gap
        self.own, self.sib, self.lands, self.acc = buffers[0], buffers[1], buffers[2:5], buffers[5]
        (self.own_sem, self.give_sem, self.sib_recv, self.up_send) = semaphores[:4]
        self.land_recv = semaphores[4:7]
        self.res_recv, self.pair_recv, self.keep_sem = semaphores[7:10]
        self.down_send = semaphores[10:13]
        self.down_pair = semaphores[13]
        self.total = self.own.shape[0]
        self.ticks = self.total + gap + 2 * TREE_SPAN * lag
        me = lax.axis_index("dp")
        self.core = lax.rem(me, 2)
        self.y = lax.rem(me // 2, 2)
        self.z = me // 4
        self.pair = me + 1 - 2 * self.core
        self.near = (me - 4, me + 4, me + 2 - 4 * self.y)

    def remote(self, src, dst, send, recv, device):
        return pltpu.make_async_remote_copy(
            src_ref=src, dst_ref=dst, send_sem=send, recv_sem=recv, device_id={"dp": device}, device_id_type=MESH
        )

    def arrival(self, dst, recv, i):
        return self.remote(self.own.at[i], dst, self.give_sem.at[i], recv.at[i], self.pair)

    def slot(self, i):
        return self.out.at[2 * i + self.core]

    def begin(self, which=None):
        start = 0
        for n, (ref, offset, count) in enumerate(self.sources):
            if which is None or n in which:
                def body(i, carry, ref=ref, offset=offset, start=start):
                    at = 2 * (i - start + offset)
                    self.remote(
                        ref.at[at + 1 - self.core], self.sib.at[i], self.give_sem.at[i], self.sib_recv.at[i], self.pair
                    ).start()
                    pltpu.make_async_copy(ref.at[at + self.core], self.own.at[i], self.own_sem.at[i]).start()
                    return carry

                lax.fori_loop(start, start + count, body, 0)
            start += count

    def up(self, n, i):
        other = (1, 0, 2)[n]
        return self.remote(self.own.at[i], self.lands[other].at[i], self.up_send.at[i], self.land_recv[other].at[i], self.near[n])

    def down(self, n, src, i):
        return self.remote(src, self.slot(i), self.down_send[n].at[i], self.res_recv.at[i], self.near[n])

    def share(self, src, i):
        return self.remote(src, self.slot(i), self.down_pair.at[i], self.pair_recv.at[i], self.pair)

    def keep(self, i):
        return pltpu.make_async_copy(self.own.at[i], self.slot(i), self.keep_sem.at[i])

    def spread(self, src, i, roles):
        for n in range(3):
            @pl.when(has(roles, n))
            def _(n=n):
                self.down(n, src, i).start()

        self.share(src, i).start()

    def ascend(self, i, roles):
        own, sib, acc = self.own, self.sib, self.acc
        pltpu.make_async_copy(own.at[i], own.at[i], self.own_sem.at[i]).wait()
        self.arrival(sib.at[i], self.sib_recv, i).wait_recv()
        leaf = lax.bitwise_and(roles, jnp.int32(7)) == 0

        @pl.when(leaf)
        def _():
            own[i] = (own[i].astype(F32) + sib[i].astype(F32)).astype(BF16)

        @pl.when(jnp.logical_not(leaf))
        def _():
            acc[...] = own[i].astype(F32) + sib[i].astype(F32)
            for n in range(3):
                @pl.when(has(roles, n))
                def _(n=n):
                    self.arrival(self.lands[n].at[i], self.land_recv[n], i).wait_recv()
                    acc[...] += self.lands[n][i].astype(F32)

            own[i] = acc[...].astype(BF16)

        for n in range(3):
            @pl.when(has(roles, 3 + n))
            def _(n=n):
                self.up(n, i).start()

        @pl.when(has(roles, 6))
        def _():
            self.keep(i).start()
            self.spread(own.at[i], i, roles)

    def descend(self, i, roles):
        self.arrival(self.slot(i), self.res_recv, i).wait_recv()
        self.spread(self.slot(i), i, roles)

    def tick(self, t):
        for level in range(2 * TREE_SPAN + 1):
            at = t - self.lag * level
            late = at >= self.early
            i = at - jnp.where(late, self.gap, 0)
            inside = jnp.logical_and(at >= 0, i < self.total)
            inside = jnp.logical_and(inside, jnp.logical_or(jnp.logical_not(late), i >= self.early))
            roles = tree_roles(jnp.clip(i, 0, self.total - 1), self.y, self.z)
            if level <= TREE_SPAN:
                @pl.when(jnp.logical_and(inside, lax.bitwise_and(roles, jnp.int32(15 * 128)) == level * 128))
                def _(i=i, roles=roles):
                    self.ascend(i, roles)

            if level >= 2:
                @pl.when(jnp.logical_and(inside, lax.bitwise_and(roles, jnp.int32(15 * 2048)) == level * 2048))
                def _(i=i, roles=roles):
                    self.descend(i, roles)

    def run(self, first, last):
        def body(t, carry):
            self.tick(t)
            return carry

        lax.fori_loop(first, last, body, 0)

    def drain(self):
        own = self.own

        def body(i, carry):
            roles = tree_roles(i, self.y, self.z)
            self.remote(own.at[i], self.sib.at[i], self.give_sem.at[i], self.sib_recv.at[i], self.pair).wait_send()

            @pl.when(jnp.logical_not(has(roles, 6)))
            def _():
                self.up(2, i).wait_send()

            @pl.when(has(roles, 6))
            def _():
                self.keep(i).wait()

            for n in range(3):
                @pl.when(has(roles, n))
                def _(n=n):
                    self.down(n, own.at[i], i).wait_send()

            self.share(own.at[i], i).wait_send()
            self.arrival(self.out.at[2 * i + 1 - self.core], self.pair_recv, i).wait_recv()
            return carry

        lax.fori_loop(0, self.total, body, 0)


def reducer_scratch(total, chunk):
    return (
        [pltpu.VMEM((total,) + chunk, BF16)] * 5
        + [pltpu.VMEM(chunk, F32)]
        + [pltpu.SemaphoreType.DMA((total,))] * 14
    )


REDUCER_BUFFERS, REDUCER_REFS = 6, 20


def greet(barrier, peers):
    me = lax.axis_index("dp")
    for step in range(1, peers):
        pl.semaphore_signal(barrier, inc=1, device_id={"dp": lax.rem(me + step, peers)}, device_id_type=MESH)
    pl.semaphore_signal(barrier, inc=1, device_id={"mlp": 1 - lax.axis_index("mlp")}, device_id_type=MESH)
    pl.semaphore_wait(barrier, peers)


def to_peer(src, dst, send, recv):
    return pltpu.make_async_remote_copy(
        src_ref=src, dst_ref=dst, send_sem=send, recv_sem=recv,
        device_id={"mlp": 1 - lax.axis_index("mlp")}, device_id_type=MESH,
    )


def attention_kernel(
    tile, order_ref, place_ref, in_ref, angle_ref, stage,
    q_nat, k_nat, v_nat, k_tr, v_tr, g_tr, probs, kv_grad, aq_out,
):
    spans, tok, _ = in_ref.shape
    length = spans * tok
    blocks = length // tile
    scale = 1.0 / math.sqrt(HEAD_DIM)
    zeros = jnp.zeros((tok, HEAD_DIM), BF16)

    def gather(place, carry):
        span = order_ref[place]
        rows = pl.ds(pl.multiple_of(place * tok, tok), tok)
        data = in_ref[span]
        q_nat[rows, :] = jnp.concatenate([data[:, :HEAD_DIM] * jnp.asarray(scale, BF16), zeros], axis=1)
        k_nat[rows, :] = data[:, HEAD_DIM : 2 * HEAD_DIM]
        v_nat[rows, :] = data[:, 2 * HEAD_DIM : 3 * HEAD_DIM]
        aq_out[rows, :HEAD_DIM] = data[:, 3 * HEAD_DIM :]
        return carry

    lax.fori_loop(0, spans, gather, 0)

    def flip(block, carry):
        rows = pl.ds(pl.multiple_of(block * tile, tile), tile)
        k_tr[:, rows] = k_nat[rows, :].T
        v_tr[:, rows] = v_nat[rows, :].T
        g_tr[:, rows] = aq_out[rows, :HEAD_DIM].T
        kv_grad[rows, :] = jnp.zeros((tile, 2 * HEAD_DIM), F32)
        return carry

    lax.fori_loop(0, blocks, flip, 0)

    key_row = lax.broadcasted_iota(jnp.int32, (tile, tile), 0)
    query_col = lax.broadcasted_iota(jnp.int32, (tile, tile), 1)
    causal = key_row <= query_col
    pad = jnp.zeros((tile, HEAD_DIM), BF16)
    half_rot = ROT // 2

    def turn_back(grad, rows):
        cosine, sine = angle_ref[0, :, rows], angle_ref[1, :, rows]
        first, second = grad[:half_rot], grad[half_rot:ROT]
        return jnp.concatenate([first * cosine + second * sine, second * cosine - first * sine, grad[ROT:]], axis=0)

    def query_block(block, carry):
        q_rows = pl.ds(pl.multiple_of(block * tile, tile), tile)
        queries_pad = q_nat[q_rows, :]
        queries = queries_pad[:, :HEAD_DIM]

        def forward(j, state, masked):
            mixed, totals = state
            rows = pl.ds(pl.multiple_of(j * tile, tile), tile)
            prob = jnp.exp(dot_nt(k_nat[rows, :], queries))
            if masked:
                prob = jnp.where(causal, prob, 0.0)
            probs[rows, :] = prob
            mixed = mixed + dot_nn(v_tr[:, rows], prob.astype(BF16))
            totals = totals + jnp.sum(prob.reshape(tile // 8, 8, tile), axis=0)
            return mixed, totals

        state = (jnp.zeros((HEAD_DIM, tile), F32), jnp.zeros((8, tile), F32))
        state = lax.fori_loop(0, block, lambda j, s: forward(j, s, False), state)
        mixed, totals = forward(block, state, True)
        totals = jnp.sum(totals, axis=0, keepdims=True)
        attended = mixed / totals
        grad_att = g_tr[:, q_rows].astype(F32)
        grad_mixed = (grad_att / totals).astype(BF16)
        grad_totals = (-jnp.sum(grad_att * attended, axis=0, keepdims=True) / totals).astype(BF16).astype(F32)
        grad_pad = jnp.concatenate([pad, grad_mixed.T], axis=1)

        def backward(j, grad_q):
            rows = pl.ds(pl.multiple_of(j * tile, tile), tile)
            prob = probs[rows, :]
            grad_scores = (prob * (dot_nn(v_nat[rows, :], grad_mixed) + grad_totals)).astype(BF16)
            kv_grad[rows, :] += dot_nn(grad_scores, queries_pad) + dot_nn(prob.astype(BF16), grad_pad)
            return grad_q + dot_nn(k_tr[:, rows], grad_scores)

        grad_q = lax.fori_loop(0, block + 1, backward, jnp.zeros((HEAD_DIM, tile), F32))
        aq_out[q_rows, :] = jnp.concatenate([attended, turn_back(grad_q * scale, q_rows)], axis=0).T.astype(BF16)
        return carry

    lax.fori_loop(0, blocks, query_block, 0)

    def turn_keys(block, carry):
        rows = pl.ds(pl.multiple_of(block * tile, tile), tile)
        kv_grad[rows, :] = turn_back(kv_grad[rows, :].T, rows).T
        return carry

    lax.fori_loop(0, blocks, turn_keys, 0)

    def fill(span, carry):
        rows = pl.ds(pl.multiple_of(place_ref[span] * tok, tok), tok)
        stage[span, :, : 2 * HEAD_DIM] = aq_out[rows, :]
        stage[span, :, 2 * HEAD_DIM :] = kv_grad[rows, :].astype(BF16)
        return carry

    lax.fori_loop(0, spans, fill, 0)


def attention(heads, order, places):
    spans, tok, width = heads.shape
    length = spans * tok
    tile = 256
    half_rot = ROT // 2
    frequency = ROPE_BASE ** (-(jnp.arange(half_rot, dtype=F32) * 2.0 / ROT))
    angles = frequency[:, None] * jnp.arange(length, dtype=F32)[None, :]
    angle_tables = jnp.stack([jnp.cos(angles), jnp.sin(angles)])
    vmem = pl.BlockSpec(memory_space=pltpu.VMEM)
    smem = pl.BlockSpec(memory_space=pltpu.SMEM)
    return pl.pallas_call(
        functools.partial(attention_kernel, tile),
        out_shape=jax.ShapeDtypeStruct(heads.shape, BF16),
        in_specs=[smem, smem, vmem, vmem],
        out_specs=vmem,
        scratch_shapes=[
            pltpu.VMEM((length, 2 * HEAD_DIM), BF16),
            pltpu.VMEM((length, HEAD_DIM), BF16),
            pltpu.VMEM((length, HEAD_DIM), BF16),
            pltpu.VMEM((HEAD_DIM, length), BF16),
            pltpu.VMEM((HEAD_DIM, length), BF16),
            pltpu.VMEM((HEAD_DIM, length), BF16),
            pltpu.VMEM((length, tile), F32),
            pltpu.VMEM((length, 2 * HEAD_DIM), F32),
            pltpu.VMEM((length, 2 * HEAD_DIM), BF16),
        ],
        compiler_params=pltpu.CompilerParams(vmem_limit_bytes=VMEM_BIG),
        cost_estimate=pl.CostEstimate(flops=40 * 10**9, bytes_accessed=10**7, transcendentals=10**7),
        name="attention",
    )(order, places, heads, angle_tables)


def last_kernel(
    lag, gap, per_block,
    stage, mlp_in, gn_in, up_in, down_in, wqkv_hbm, wout_hbm,
    x_ref, cot_ref, cot_peer, normed_ref, normed_peer, gain_ref, bias_ref, mlp_own, gn_own, gbias_ref,
    out_ref, grad_in_ref, summed, *scratch,
):
    (heads_own, heads_peer, mlp_other, gn_other, wqkv_ref, wout_ref, att_ref, att_peer, gproj_ref, gproj_peer, normed_tr,
     sums_ref, small_ref, landing) = scratch[:14]
    (head_send, head_recv, relay_send, relay_recv, pair_send, pair_recv, local_sem, load_sem, swap_send, swap_recv) = scratch[14:24]
    buffers = scratch[24:]
    spans = stage.shape[0]
    tok, width = x_ref.shape
    chunks = width // CHUNK
    me = lax.axis_index("dp")
    here = lax.axis_index("mlp")
    greet(pltpu.get_barrier_semaphore(), spans)
    pairs = [
        to_peer(src, dst, pair_send.at[n], pair_recv.at[n])
        for n, (src, dst) in enumerate(((mlp_in, mlp_other), (gn_in, gn_other)))
    ]
    loads = [
        pltpu.make_async_copy(src, dst, load_sem.at[n])
        for n, (src, dst) in enumerate(((wqkv_hbm, wqkv_ref), (wout_hbm, wout_ref)))
    ]

    def block_copy(step):
        target = lax.rem(me + step, spans)
        return pltpu.make_async_remote_copy(
            src_ref=stage.at[target], dst_ref=heads_own.at[me], send_sem=head_send.at[step], recv_sem=head_recv.at[step],
            device_id={"dp": target}, device_id_type=MESH,
        )

    def relay(source_ref, step):
        source = lax.rem(me + spans - step, spans)
        return to_peer(source_ref.at[source], heads_peer.at[source], relay_send.at[step], relay_recv.at[step])

    for step in range(1, spans):
        block_copy(step).start()
    relay(stage, 0).start()
    own = pltpu.make_async_copy(stage.at[me], heads_own.at[me], local_sem)
    own.start()
    for copy in loads + pairs:
        copy.start()
    early = up_in.shape[0] // 2 + down_in.shape[0] // 2
    reducer = Reducer(
        ((up_in, 0, up_in.shape[0] // 2), (down_in, 0, down_in.shape[0] // 2), (sums_ref, 0, sums_ref.shape[0] // 2)),
        summed, buffers[:REDUCER_BUFFERS], buffers[REDUCER_BUFFERS:], lag, early, gap,
    )
    reducer.begin((0, 1))

    def hand_on(step, carry):
        block_copy(step).wait_recv()
        relay(heads_own, step).start()
        reducer.run((step - 1) * per_block, step * per_block)
        return carry

    lax.fori_loop(1, spans, hand_on, 0)
    state = [(spans - 1) * per_block]

    def advance(count):
        stop = min(state[0] + count, early + gap)
        reducer.run(state[0], stop)
        state[0] = stop

    own.wait()
    for copy in loads:
        copy.wait()
    low = lax.broadcasted_iota(jnp.int32, (tok, LANES), 1) < HEAD_DIM

    def unpack(source, att_to, gproj_to):
        for pair in range(HEADS // 2):
            at = pair * LANES
            even, odd = source[2 * pair].astype(F32), source[2 * pair + 1].astype(F32)
            att, gq = split_pair(even[:, :LANES], odd[:, :LANES], low)
            gk, gv = split_pair(even[:, LANES:], odd[:, LANES:], low)
            att_to[:, at : at + LANES] = att.astype(BF16)
            for part, grad in enumerate((gq, gk, gv)):
                gproj_to[:, part * width + at : part * width + at + LANES] = grad.astype(BF16)

    unpack(heads_own, att_ref, gproj_ref)
    advance(1)
    normed_tr[:, :tok] = normed_ref[...].T
    normed_tr[:, tok:] = normed_peer[...].T
    for copy in pairs:
        copy.wait()
    advance(1)
    rows = x_ref[...].astype(F32)
    branch = mlp_own[...].astype(F32) + mlp_other[...].astype(F32)
    out_ref[...] = (rows + dot_nn(att_ref[...], wout_ref[...]) + branch + bias_ref[...]).astype(BF16)
    advance(1)
    grad_normed = dot_nt(gproj_ref[...], wqkv_ref[...]) + gn_own[...].astype(F32) + gn_other[...].astype(F32)
    grad_in_ref[...] = grad_normed
    advance(1)
    rows = x_ref[...].astype(F32)
    cot = cot_ref[...].astype(F32)
    grad_normed = grad_in_ref[...]
    centre = jnp.mean(rows, axis=-1, keepdims=True)
    centred = rows - centre
    inv = lax.rsqrt(jnp.mean(centred * centred, axis=-1, keepdims=True) + EPSILON)
    unit = centred * inv
    small_ref[0:1, :] = jnp.sum(grad_normed * unit, axis=0, keepdims=True)
    small_ref[1:2, :] = jnp.sum(grad_normed, axis=0, keepdims=True)
    small_ref[2:3, :] = jnp.sum(cot, axis=0, keepdims=True)
    for part in range(3):
        part_cols = slice(part * width, (part + 1) * width)
        small_ref[3 + part : 4 + part, :] = jnp.sum(gproj_ref[:, part_cols].astype(F32), axis=0, keepdims=True)
    small_ref[6:7, :] = gbias_ref[:, :width]
    small_ref[7:8, :] = gbias_ref[:, width:]
    grad_unit = grad_normed * gain_ref[...]
    grad_in_ref[...] = cot + inv * (
        grad_unit
        - jnp.mean(grad_unit, axis=-1, keepdims=True)
        - unit * jnp.mean(grad_unit * unit, axis=-1, keepdims=True)
    )
    swap = to_peer(small_ref, landing, swap_send, swap_recv)
    swap.start()
    advance(1)
    for step in range(spans):
        relay(heads_own, step).wait()
    unpack(heads_peer, att_peer, gproj_peer)
    advance(1)
    third, half, group = 3 * width // 2, width // 2, 512
    for start in range(0, third, group):
        cols = pl.ds(pl.multiple_of(here * third + start, LANES), group)
        block, at = start // width, start % width
        sums_ref[block * chunks : (block + 1) * chunks, :, at : at + group] = (
            dot_nn(normed_tr[...], jnp.concatenate([gproj_ref[:, cols], gproj_peer[:, cols]], axis=0))
            .astype(BF16).reshape(chunks, CHUNK, group)
        )
        advance(1)
    cols = pl.ds(pl.multiple_of(here * half, LANES), half)
    att_tr = jnp.concatenate([att_ref[...], att_peer[...]], axis=0).T
    cots = jnp.concatenate([cot_ref[:, cols], cot_peer[:, cols]], axis=0)
    sums_ref[chunks : 2 * chunks, :, half:] = dot_nn(att_tr, cots).astype(BF16).reshape(chunks, CHUNK, half)
    swap.wait()
    shared = lax.broadcasted_iota(jnp.int32, (8, width), 0) < 6
    sums_ref[2 * chunks : 2 * chunks + 2] = jnp.zeros((2, CHUNK, width), BF16)
    sums_ref[2 * chunks, 0:16, :] = jnp.concatenate(
        [small_ref[...] + jnp.where(shared, landing[...], 0.0), jnp.zeros((8, width), F32)], axis=0
    ).astype(BF16)
    advance(early + gap)
    reducer.begin((2,))
    reducer.run(early + gap, reducer.ticks)
    reducer.drain()
    for step in range(1, spans):
        block_copy(step).wait_send()


def last(stage, mlp_give, gn_give, sum_up, sum_down, w_qkv, w_out, *operands):
    spans = stage.shape[0]
    tok, width = operands[0].shape
    chunk = sum_up.shape[1:]
    late = 2 * (width // CHUNK) + 2
    total = (sum_up.shape[0] + sum_down.shape[0] + late) // 2
    vmem = pl.BlockSpec(memory_space=pltpu.VMEM)
    any_spec = pl.BlockSpec(memory_space=pl.ANY)
    tokens, wide = pltpu.VMEM((tok, width), BF16), pltpu.VMEM((tok, 3 * width), BF16)
    return pl.pallas_call(
        functools.partial(last_kernel, TREE_LAG, TREE_GAP, TICKS_PER_BLOCK),
        out_shape=(
            jax.ShapeDtypeStruct((tok, width), BF16),
            jax.ShapeDtypeStruct((tok, width), F32),
            jax.ShapeDtypeStruct((2 * total,) + chunk, BF16),
        ),
        in_specs=[any_spec] * 7 + [vmem] * len(operands),
        out_specs=(vmem, vmem, any_spec),
        scratch_shapes=[
            pltpu.VMEM(stage.shape, BF16), pltpu.VMEM(stage.shape, BF16), tokens, tokens,
            pltpu.VMEM(w_qkv.shape, BF16), pltpu.VMEM(w_out.shape, BF16), tokens, tokens, wide, wide,
            pltpu.VMEM((width, 2 * tok), BF16), pltpu.VMEM((late,) + chunk, BF16),
            pltpu.VMEM((8, width), F32), pltpu.VMEM((8, width), F32),
        ]
        + [pltpu.SemaphoreType.DMA((spans,))] * 4
        + [pltpu.SemaphoreType.DMA((2,))] * 2
        + [pltpu.SemaphoreType.DMA, pltpu.SemaphoreType.DMA((2,)), pltpu.SemaphoreType.DMA, pltpu.SemaphoreType.DMA]
        + reducer_scratch(total, chunk),
        compiler_params=pltpu.CompilerParams(
            collective_id=1, has_side_effects=True, vmem_limit_bytes=VMEM_ALL
        ),
        name="last",
    )(stage, mlp_give, gn_give, sum_up, sum_down, w_qkv, w_out, *operands)


def widen_kernel(up_a, up_b, down_a, down_b, first_ref, second_ref, vec_ref, out_in, grad_in,
                 qkv_ref, out_ref, up_ref, down_ref, vec_out, out_out, grad_out):
    width = first_ref.shape[-1]
    half = width // 2
    qkv_ref[:, :width] = first_ref[0].astype(F32)
    qkv_ref[:, width:] = second_ref[0, :, :half].astype(F32)
    out_ref[...] = second_ref[0, :, half:].astype(F32)
    up_ref[:, :width] = up_a[0].astype(F32)
    up_ref[:, width:] = up_b[0].astype(F32)
    down_ref[0] = down_a[0].astype(F32)
    down_ref[1] = down_b[0].astype(F32)

    @pl.when(pl.program_id(0) == 0)
    def _():
        vec_out[...] = vec_ref[0, :16, :].astype(F32)
        out_out[...] = out_in[...]
        grad_out[...] = grad_in[...]


def widen(summed, output, grad_input):
    chunk, width = summed.shape[1:]
    steps = width // chunk
    row = lambda cols: pl.BlockSpec((chunk, cols), lambda s: (s, 0))
    blocks = [pl.BlockSpec((1, chunk, width), lambda s, n=n: (n * steps + s, 0, 0)) for n in range(6)]
    const = lambda shape: pl.BlockSpec(shape, lambda s: (0,) * len(shape))
    qkv, out, up, down, vec, output, grad_input = pl.pallas_call(
        widen_kernel,
        grid=(steps,),
        out_shape=(
            jax.ShapeDtypeStruct((width, 3 * width // 2), F32),
            jax.ShapeDtypeStruct((width, width // 2), F32),
            jax.ShapeDtypeStruct((width, 2 * width), F32),
            jax.ShapeDtypeStruct((2, width, width), F32),
            jax.ShapeDtypeStruct((16, width), F32),
            jax.ShapeDtypeStruct(output.shape, BF16),
            jax.ShapeDtypeStruct(grad_input.shape, F32),
        ),
        in_specs=blocks
        + [
            pl.BlockSpec((1, chunk, width), lambda s: (6 * steps, 0, 0)),
            const(output.shape), const(grad_input.shape),
        ],
        out_specs=(
            row(3 * width // 2), row(width // 2), row(2 * width),
            pl.BlockSpec((2, chunk, width), lambda s: (0, s, 0)),
            const((16, width)), const(output.shape), const(grad_input.shape),
        ),
        name="widen",
    )(*[summed] * 7, output, grad_input)
    return qkv, out, up, down.reshape(2 * width, width), vec, output, grad_input


def by_heads(
    block_input, span_offset, ln_gain, ln_bias, w_qkv, b_qkv, w_out, b_out, w_up, b_up, w_down, b_down, cotangent
):
    tok, width = block_input.shape[2:]
    spans = span_offset.shape[0]
    span_here = lax.axis_index("dp")
    seq_here = lax.axis_index("mlp")
    offsets = lax.dynamic_index_in_dim(span_offset, seq_here, axis=1, keepdims=False)
    places = jnp.arange(spans, dtype=jnp.int32)
    order = jnp.sum(jnp.where(offsets[None, :] == places[:, None], places[None, :], 0), axis=1)
    offset_here = lax.dynamic_index_in_dim(offsets, span_here, axis=0, keepdims=False)
    tables = rotary_tables(offset_here * tok + jnp.arange(tok, dtype=jnp.int32))
    x, cot = block_input[0, 0], cotangent[0, 0]
    gain, shift = ln_gain[None], ln_bias[None]

    normed, send = project(x, cot, gain, shift, w_qkv, b_qkv[None], w_out, tables)
    heads, (normed_peer, cot_peer) = exchange(send, (normed, cot), 0)
    mlp_part, mlp_give, gn_part, gn_give, sum_up, sum_down, grad_b_up = feed_forward(
        normed, normed_peer, cot, cot_peer, w_up, b_up[None], w_down
    )
    stage = attention(heads, order, offsets)
    output, grad_input, summed = last(
        stage, mlp_give, gn_give, sum_up, sum_down, w_qkv, w_out,
        x, cot, cot_peer, normed, normed_peer, gain, (b_out + b_down)[None], mlp_part, gn_part, grad_b_up,
    )
    qkv, out, up, down, vec, output, grad_input = widen(summed, output, grad_input)
    half = width // 2
    piece = lambda start, rows: lax.dynamic_slice_in_dim(
        vec[start : start + rows].reshape(-1), seq_here * (rows * half), rows * half
    )
    bias_sum = piece(2, 1)
    return (
        output.reshape(1, 1, tok, width),
        grad_input.reshape(1, 1, tok, width),
        piece(0, 1),
        piece(1, 1),
        qkv,
        piece(3, 3),
        out,
        bias_sum,
        up,
        vec[6:8].reshape(-1),
        down,
        bias_sum,
    )


def rotate(values, positions, sign_factor):
    half_rot = ROT // 2
    frequency = ROPE_BASE ** (-(jnp.arange(half_rot, dtype=jnp.float32) * 2.0 / ROT))
    angles = positions.astype(jnp.float32)[:, None] * frequency[None, :]
    cosine = jnp.cos(angles)[:, None, :]
    sine_part = sign_factor * jnp.sin(angles)[:, None, :]
    first_half = values[..., :half_rot]
    second_half = values[..., half_rot:ROT]
    return jnp.concatenate(
        [
            first_half * cosine - second_half * sine_part,
            second_half * cosine + first_half * sine_part,
            values[..., ROT:],
        ],
        axis=-1,
    )


def gelu_exact(values):
    return 0.5 * values * (1.0 + lax.erf(values * SQRT_HALF))


def gelu_slope(values):
    return (
        0.5 * (1.0 + lax.erf(values * SQRT_HALF))
        + values * jnp.exp(-0.5 * values * values) * INV_ROOT_TWO_PI
    )


def piece_count(total_rows):
    count_blocks = max(1, total_rows // 1024)
    while total_rows % count_blocks:
        count_blocks += 1
    return count_blocks


def row_positions(offsets, count_rows, tok_count):
    index_all = jnp.arange(count_rows, dtype=jnp.int32)
    span_of = index_all // tok_count
    within = index_all - span_of * tok_count
    matches = span_of[:, None] == jnp.arange(offsets.shape[0], dtype=jnp.int32)[None, :]
    offset_of = jnp.sum(jnp.where(matches, offsets[None, :], 0), axis=1)
    return offset_of * tok_count + within


def contract_rows(left_mat, right_mat):
    return lax.dot_general(
        left_mat, right_mat, (((0,), (0,)), ((), ())), preferred_element_type=jnp.float32
    )


def contract_cols(left_mat, right_mat):
    return lax.dot_general(
        left_mat, right_mat, (((1,), (1,)), ((), ())), preferred_element_type=jnp.float32
    )


def local(
    block_input,
    span_offset,
    ln_gain,
    ln_bias,
    w_qkv,
    b_qkv,
    w_out,
    b_out,
    w_up,
    b_up,
    w_down,
    b_down,
    cotangent,
):
    tok_count = block_input.shape[2]
    model_width = block_input.shape[3]
    scale_dot = 1.0 / math.sqrt(HEAD_DIM)
    span_here = lax.axis_index("dp")
    seq_here = lax.axis_index("mlp")
    offsets = lax.dynamic_index_in_dim(span_offset, seq_here, axis=1, keepdims=False)
    offset_here = lax.dynamic_index_in_dim(offsets, span_here, axis=0, keepdims=False)
    positions = offset_here * tok_count + jnp.arange(tok_count, dtype=jnp.int32)
    row_data = block_input[0, 0].astype(jnp.float32)
    centre = jnp.mean(row_data, axis=-1, keepdims=True)
    centred = row_data - centre
    spread = jnp.mean(centred * centred, axis=-1, keepdims=True)
    inv_scale = lax.rsqrt(spread + EPSILON)
    unit_rows = centred * inv_scale
    normed = (unit_rows * ln_gain + ln_bias).astype(jnp.bfloat16)
    project = jnp.dot(normed, w_qkv, preferred_element_type=jnp.float32) + b_qkv
    queries = rotate(
        project[:, :model_width].reshape(tok_count, HEADS, HEAD_DIM), positions, 1.0
    ).astype(jnp.bfloat16)
    keys_here = rotate(
        project[:, model_width : 2 * model_width].reshape(tok_count, HEADS, HEAD_DIM),
        positions,
        1.0,
    ).astype(jnp.bfloat16)
    values_here = (
        project[:, 2 * model_width :].reshape(tok_count, HEADS, HEAD_DIM).astype(jnp.bfloat16)
    )
    keys_flat = keys_here.reshape(tok_count, model_width)
    values_flat = values_here.reshape(tok_count, model_width)
    start_state = (
        jnp.zeros((tok_count, HEADS, HEAD_DIM), jnp.float32),
        jnp.zeros((HEADS, tok_count), jnp.float32),
    )
    keys_piece = lax.all_gather(keys_flat, "dp", axis=0, tiled=True)
    values_piece = lax.all_gather(values_flat, "dp", axis=0, tiled=True)
    piece_rows = keys_piece.shape[0]
    blocks = piece_count(piece_rows)
    sub_rows = piece_rows // blocks
    key_pos = row_positions(offsets, piece_rows, tok_count)

    def attend_one_block(state_now, packed):
        keys_blk, values_blk, pos_blk = packed
        key_heads = keys_blk.reshape(sub_rows, HEADS, HEAD_DIM)
        value_heads = values_blk.reshape(sub_rows, HEADS, HEAD_DIM)
        scores = (
            jnp.einsum("qhd,khd->hqk", queries, key_heads, preferred_element_type=jnp.float32)
            * scale_dot
        )
        allowed = pos_blk[None, :] <= positions[:, None]
        weights_exp = jnp.where(allowed[None], jnp.exp(scores), 0.0)
        mixed_sum, totals = state_now
        mixed_sum = mixed_sum + jnp.einsum(
            "hqk,khd->qhd",
            weights_exp.astype(jnp.bfloat16),
            value_heads,
            preferred_element_type=jnp.float32,
        )
        return ((mixed_sum, totals + jnp.sum(weights_exp, axis=-1)), None)

    state_now, _unused = lax.scan(
        attend_one_block,
        start_state,
        (
            keys_piece.reshape(blocks, sub_rows, model_width),
            values_piece.reshape(blocks, sub_rows, model_width),
            key_pos.reshape(blocks, sub_rows),
        ),
    )
    mixed_sum, totals = state_now
    attended = mixed_sum / totals.T[:, :, None]
    attended_low = attended.reshape(tok_count, model_width).astype(jnp.bfloat16)
    attn_branch = jnp.dot(attended_low, w_out, preferred_element_type=jnp.float32) + b_out
    normed_all = lax.all_gather(normed, "mlp", axis=0, tiled=True)
    up_proj = jnp.dot(normed_all, w_up, preferred_element_type=jnp.float32) + b_up
    activated = gelu_exact(up_proj).astype(jnp.bfloat16)
    mlp_branch = (
        lax.psum_scatter(
            jnp.dot(activated, w_down, preferred_element_type=jnp.float32).astype(jnp.bfloat16),
            "mlp",
            scatter_dimension=0,
            tiled=True,
        ).astype(jnp.float32)
        + b_down
    )
    output = (row_data + attn_branch + mlp_branch).astype(jnp.bfloat16)
    grad_out = cotangent[0, 0]
    grad_w_out = contract_rows(attended_low, grad_out)
    grad_bias_out = jnp.sum(grad_out.astype(jnp.float32), axis=0)
    grad_all = lax.all_gather(grad_out, "mlp", axis=0, tiled=True)
    grad_w_down = contract_rows(activated, grad_all)
    grad_act = contract_cols(grad_all, w_down)
    grad_up = (grad_act * gelu_slope(up_proj)).astype(jnp.bfloat16)
    grad_w_up = contract_rows(normed_all, grad_up)
    grad_b_up = jnp.sum(grad_up.astype(jnp.float32), axis=0)
    grad_norm_mlp = lax.psum_scatter(
        contract_cols(grad_up, w_up).astype(jnp.bfloat16), "mlp", scatter_dimension=0, tiled=True
    ).astype(jnp.float32)
    grad_att = contract_cols(grad_out, w_out).reshape(tok_count, HEADS, HEAD_DIM)
    grad_mixed = (grad_att / totals.T[:, :, None]).astype(jnp.bfloat16)
    grad_totals = ((-jnp.sum(grad_att * attended, axis=-1)).T / totals).astype(jnp.bfloat16)
    grad_totals_wide = grad_totals.astype(jnp.float32)[:, :, None]
    zero_heads = jnp.zeros((tok_count, HEADS, HEAD_DIM), jnp.float32)
    grad_query_sum = zero_heads
    keys_piece = lax.all_gather(keys_flat, "dp", axis=0, tiled=True)
    values_piece = lax.all_gather(values_flat, "dp", axis=0, tiled=True)
    piece_rows = keys_piece.shape[0]
    blocks = piece_count(piece_rows)
    back_sub_rows = piece_rows // blocks
    key_pos = row_positions(offsets, piece_rows, tok_count)

    def back_one_block(running_sum, packed):
        keys_blk, values_blk, pos_blk = packed
        key_heads = keys_blk.reshape(back_sub_rows, HEADS, HEAD_DIM)
        value_heads = values_blk.reshape(back_sub_rows, HEADS, HEAD_DIM)
        scores = (
            jnp.einsum("qhd,khd->hqk", queries, key_heads, preferred_element_type=jnp.float32)
            * scale_dot
        )
        allowed = pos_blk[None, :] <= positions[:, None]
        weights_exp = jnp.where(allowed[None], jnp.exp(scores), 0.0)
        grad_exp = jnp.einsum(
            "qhd,khd->hqk", grad_mixed, value_heads, preferred_element_type=jnp.float32
        )
        grad_scores = (weights_exp * (grad_exp + grad_totals_wide)).astype(jnp.bfloat16)
        running_sum = running_sum + scale_dot * jnp.einsum(
            "hqk,khd->qhd", grad_scores, key_heads, preferred_element_type=jnp.float32
        )
        grad_key_blk = scale_dot * jnp.einsum(
            "hqk,qhd->khd", grad_scores, queries, preferred_element_type=jnp.float32
        )
        grad_value_blk = jnp.einsum(
            "hqk,qhd->khd",
            weights_exp.astype(jnp.bfloat16),
            grad_mixed,
            preferred_element_type=jnp.float32,
        )
        joined = jnp.concatenate(
            [
                grad_key_blk.reshape(back_sub_rows, model_width),
                grad_value_blk.reshape(back_sub_rows, model_width),
            ],
            axis=1,
        )
        return (running_sum, joined)

    grad_query_sum, stacked = lax.scan(
        back_one_block,
        grad_query_sum,
        (
            keys_piece.reshape(blocks, back_sub_rows, model_width),
            values_piece.reshape(blocks, back_sub_rows, model_width),
            key_pos.reshape(blocks, back_sub_rows),
        ),
    )
    grad_kv_sum = stacked.reshape(piece_rows, 2 * model_width)
    grad_kv = lax.psum_scatter(
        grad_kv_sum.astype(jnp.bfloat16), "dp", scatter_dimension=0, tiled=True
    ).astype(jnp.float32)
    grad_keys = grad_kv[:, :model_width].reshape(tok_count, HEADS, HEAD_DIM)
    grad_values = grad_kv[:, model_width:].reshape(tok_count, HEADS, HEAD_DIM)
    grad_query_pre = rotate(grad_query_sum, positions, -1.0).reshape(tok_count, model_width)
    grad_key_pre = rotate(grad_keys, positions, -1.0).reshape(tok_count, model_width)
    grad_project = jnp.concatenate(
        [grad_query_pre, grad_key_pre, grad_values.reshape(tok_count, model_width)], axis=1
    ).astype(jnp.bfloat16)
    grad_w_qkv = contract_rows(normed, grad_project)
    grad_b_qkv = jnp.sum(grad_project.astype(jnp.float32), axis=0)
    grad_normed = contract_cols(grad_project, w_qkv) + grad_norm_mlp
    grad_ln_gain = jnp.sum(grad_normed * unit_rows, axis=0)
    grad_ln_bias = jnp.sum(grad_normed, axis=0)
    grad_unit = grad_normed * ln_gain
    grad_rows = inv_scale * (
        grad_unit
        - jnp.mean(grad_unit, axis=-1, keepdims=True)
        - unit_rows * jnp.mean(grad_unit * unit_rows, axis=-1, keepdims=True)
    )
    grad_input = (grad_out.astype(jnp.float32) + grad_rows).reshape(1, 1, tok_count, model_width)
    part_qkv, part_out, part_bqkv, part_bias, part_gain, part_shift = (
        lax.psum_scatter(
            grad_w_qkv.astype(jnp.bfloat16), "mlp", scatter_dimension=1, tiled=True
        ).astype(jnp.float32),
        lax.psum_scatter(
            grad_w_out.astype(jnp.bfloat16), "mlp", scatter_dimension=1, tiled=True
        ).astype(jnp.float32),
        lax.psum_scatter(
            grad_b_qkv.astype(jnp.bfloat16), "mlp", scatter_dimension=0, tiled=True
        ).astype(jnp.float32),
        lax.psum_scatter(
            grad_bias_out.astype(jnp.bfloat16), "mlp", scatter_dimension=0, tiled=True
        ).astype(jnp.float32),
        lax.psum_scatter(
            grad_ln_gain.astype(jnp.bfloat16), "mlp", scatter_dimension=0, tiled=True
        ).astype(jnp.float32),
        lax.psum_scatter(
            grad_ln_bias.astype(jnp.bfloat16), "mlp", scatter_dimension=0, tiled=True
        ).astype(jnp.float32),
    )
    summed = (
        lax.psum(part_qkv.astype(jnp.bfloat16), "dp").astype(jnp.float32),
        lax.psum(part_out.astype(jnp.bfloat16), "dp").astype(jnp.float32),
        lax.psum(part_bqkv.astype(jnp.bfloat16), "dp").astype(jnp.float32),
        lax.psum(part_bias.astype(jnp.bfloat16), "dp").astype(jnp.float32),
        lax.psum(part_gain.astype(jnp.bfloat16), "dp").astype(jnp.float32),
        lax.psum(part_shift.astype(jnp.bfloat16), "dp").astype(jnp.float32),
        lax.psum(grad_w_up.astype(jnp.bfloat16), "dp").astype(jnp.float32),
        lax.psum(grad_b_up.astype(jnp.bfloat16), "dp").astype(jnp.float32),
        lax.psum(grad_w_down.astype(jnp.bfloat16), "dp").astype(jnp.float32),
    )
    return (
        output.reshape(1, 1, tok_count, model_width),
        grad_input,
        summed[4],
        summed[5],
        summed[0],
        summed[2],
        summed[1],
        summed[3],
        summed[6],
        summed[7],
        summed[8],
        summed[3],
    )


def solution(mesh):
    fits = mesh.shape["dp"] == HEADS and mesh.shape["mlp"] == 2
    return jax.shard_map(
        by_heads if fits else local,
        mesh=mesh,
        in_specs=(
            P("dp", "mlp", None, None),
            P(),
            P(),
            P(),
            P(),
            P(),
            P(),
            P(),
            P(None, "mlp"),
            P("mlp"),
            P("mlp", None),
            P(),
            P("dp", "mlp", None, None),
        ),
        out_specs=(
            P("dp", "mlp", None, None),
            P("dp", "mlp", None, None),
            P("mlp"),
            P("mlp"),
            P(None, "mlp"),
            P("mlp"),
            P(None, "mlp"),
            P("mlp"),
            P(None, "mlp"),
            P("mlp"),
            P("mlp", None),
            P("mlp"),
        ),
        check_vma=False,
    )
```

```python
import functools
import math

import jax
import jax.numpy as jnp
from jax import lax
from jax.experimental import pallas as pl
from jax.experimental.pallas import tpu as pltpu
from jax.sharding import PartitionSpec as P

HEADS = 16
HEAD_DIM = 64
ROT = 16

EPSILON = 1e-05
ROPE_BASE = 10000.0
SQRT_HALF = 1.0 / math.sqrt(2.0)
INV_ROOT_TWO_PI = 1.0 / math.sqrt(2.0 * math.pi)

MESH = pl.DeviceIdType.MESH
F32 = jnp.float32
BF16 = jnp.bfloat16
LANES = 128
VMEM_BIG = 60 * 1024 * 1024
TREE_LAG = 4
TREE_GAP = 4
TICKS_PER_BLOCK = 2
VMEM_ALL = 66 * 1024 * 1024 - 2**20 // 2


def dot_nn(a, b):
    return lax.dot_general(a, b, (((1,), (0,)), ((), ())), preferred_element_type=F32)


def dot_nt(a, b):
    return lax.dot_general(a, b, (((1,), (1,)), ((), ())), preferred_element_type=F32)


def dot_tn(a, b):
    return lax.dot_general(a, b, (((0,), (0,)), ((), ())), preferred_element_type=F32)


def rotary_tables(positions):
    lane = jnp.arange(LANES, dtype=jnp.int32) % HEAD_DIM
    half = ROT // 2
    frequency = ROPE_BASE ** (-((lane % half).astype(F32) * 2.0 / ROT))
    angles = positions.astype(F32)[:, None] * frequency[None, :]
    cosine = jnp.where(lane < ROT, jnp.cos(angles), 1.0)
    sine = jnp.sin(angles)
    up = jnp.where(lane < half, -sine, 0.0)
    down = jnp.where((lane >= half) & (lane < ROT), sine, 0.0)
    return jnp.stack([cosine, up, down])


def rotate_tile(x, tables, sign):
    half = ROT // 2
    return (
        x * tables[0]
        + pltpu.roll(x, LANES - half, 1) * (tables[1] * sign)
        + pltpu.roll(x, half, 1) * (tables[2] * sign)
    )


def split_pair(first, second, low):
    swap_first = pltpu.roll(first, HEAD_DIM, 1)
    swap_second = pltpu.roll(second, HEAD_DIM, 1)
    return jnp.where(low, first, swap_second), jnp.where(low, swap_first, second)


def project_kernel(
    x_ref, cot_ref, gain_ref, shift_ref, wq_ref, wk_ref, wv_ref, bq_ref, bk_ref, bv_ref, wo_ref, tab_ref,
    normed_ref, send_ref,
):
    @pl.when(pl.program_id(0) == 0)
    def _():
        rows = x_ref[...].astype(F32)
        centre = jnp.mean(rows, axis=-1, keepdims=True)
        centred = rows - centre
        spread = jnp.mean(centred * centred, axis=-1, keepdims=True)
        unit = centred * lax.rsqrt(spread + EPSILON)
        normed_ref[...] = (unit * gain_ref[...] + shift_ref[...]).astype(BF16)

    normed = normed_ref[...]
    q = dot_nn(normed, wq_ref[...]) + bq_ref[...]
    k = dot_nn(normed, wk_ref[...]) + bk_ref[...]
    v = dot_nn(normed, wv_ref[...]) + bv_ref[...]
    grad_att = dot_nt(cot_ref[...], wo_ref[...])
    tables = [tab_ref[i] for i in range(3)]
    low = lax.broadcasted_iota(jnp.int32, (x_ref.shape[0], LANES), 1) < HEAD_DIM
    for tile in range(q.shape[1] // LANES):
        cols = slice(tile * LANES, (tile + 1) * LANES)
        q_tile = rotate_tile(q[:, cols], tables, 1.0)
        k_tile = rotate_tile(k[:, cols], tables, 1.0)
        qk = split_pair(q_tile, k_tile, low)
        vg = split_pair(v[:, cols], grad_att[:, cols], low)
        for side in range(2):
            send_ref[2 * tile + side, :, :LANES] = qk[side].astype(BF16)
            send_ref[2 * tile + side, :, LANES:] = vg[side].astype(BF16)


def project(x, cot, gain, shift, w_qkv, b_qkv, w_out, tables):
    tok, width = x.shape
    group = 256
    steps = width // group
    heads_step = group // HEAD_DIM
    const = lambda shape: pl.BlockSpec(shape, lambda g: (0,) * len(shape))
    w_spec = lambda part: pl.BlockSpec((width, group), lambda g: (0, part * steps + g))
    b_spec = lambda part: pl.BlockSpec((1, group), lambda g: (0, part * steps + g))
    return pl.pallas_call(
        project_kernel,
        grid=(steps,),
        out_shape=(
            jax.ShapeDtypeStruct((tok, width), BF16),
            jax.ShapeDtypeStruct((HEADS, tok, 4 * HEAD_DIM), BF16),
        ),
        in_specs=[
            const((tok, width)), const((tok, width)), const((1, width)), const((1, width)),
            w_spec(0), w_spec(1), w_spec(2), b_spec(0), b_spec(1), b_spec(2),
            pl.BlockSpec((group, width), lambda g: (g, 0)),
            const((3, tok, LANES)),
        ],
        out_specs=(
            const((tok, width)),
            pl.BlockSpec((heads_step, tok, 4 * HEAD_DIM), lambda g: (g, 0, 0)),
        ),
        name="project",
    )(x, cot, gain, shift, w_qkv, w_qkv, w_qkv, b_qkv, b_qkv, b_qkv, w_out, tables)


def greet(barrier, peers):
    me = lax.axis_index("dp")
    for step in range(1, peers):
        pl.semaphore_signal(barrier, inc=1, device_id={"dp": lax.rem(me + step, peers)}, device_id_type=MESH)
    pl.semaphore_signal(barrier, inc=1, device_id={"mlp": 1 - lax.axis_index("mlp")}, device_id_type=MESH)
    pl.semaphore_wait(barrier, peers)


def to_peer(src, dst, send, recv):
    return pltpu.make_async_remote_copy(
        src_ref=src, dst_ref=dst, send_sem=send, recv_sem=recv,
        device_id={"mlp": 1 - lax.axis_index("mlp")}, device_id_type=MESH,
    )


CHUNK = 64


def first_kernel(
    group, heads_in, normed_ref, cot_ref, wup_hbm, wdown_hbm, bup_ref,
    heads_out, normed_peer, cot_peer, mlp_ref, mlp_give, gn_ref, gn_give, up_out, down_out, gbias_ref,
    wup_ref, wdown_ref, normed_all, normed_tr, cot_all, mlp_acc, gn_acc, up_sum, down_sum,
    head_send, head_recv, pair_send, pair_recv, local_sem, load_sem, store_sem,
):
    spans = heads_in.shape[0]
    tok, width = normed_ref.shape
    hidden = wup_ref.shape[1]
    me = lax.axis_index("dp")
    greet(pltpu.get_barrier_semaphore(), spans)
    pairs = [
        to_peer(src, dst, pair_send.at[n], pair_recv.at[n])
        for n, (src, dst) in enumerate(((normed_ref, normed_peer), (cot_ref, cot_peer)))
    ]
    loads = [
        pltpu.make_async_copy(src, dst, load_sem.at[n])
        for n, (src, dst) in enumerate(((wup_hbm, wup_ref), (wdown_hbm, wdown_ref)))
    ]

    def block_copy(step):
        target = lax.rem(me + step, spans)
        return pltpu.make_async_remote_copy(
            src_ref=heads_in.at[target], dst_ref=heads_out.at[me], send_sem=head_send.at[step],
            recv_sem=head_recv.at[step], device_id={"dp": target}, device_id_type=MESH,
        )

    for copy in pairs + loads:
        copy.start()
    for step in range(1, spans):
        block_copy(step).start()
    own = pltpu.make_async_copy(heads_in.at[me], heads_out.at[me], local_sem)
    own.start()
    normed_all[:tok, :] = normed_ref[...]
    normed_tr[:, :tok] = normed_ref[...].T
    cot_all[:tok, :] = cot_ref[...]
    mlp_acc[...] = jnp.zeros_like(mlp_acc)
    gn_acc[...] = jnp.zeros_like(gn_acc)
    for copy in loads + pairs:
        copy.wait()
    normed_all[tok:, :] = normed_peer[...]
    normed_tr[:, tok:] = normed_peer[...].T
    cot_all[tok:, :] = cot_peer[...]
    per = width // group

    def body(step, carry):
        hid = pl.ds(pl.multiple_of(step * group, group), group)
        at = pl.ds(pl.multiple_of(lax.rem(step, per) * group, group), group)
        w_up, w_down = wup_ref[:, hid], wdown_ref[hid, :]
        up = dot_nn(normed_all[...], w_up) + bup_ref[:, hid]
        half_erf = 0.5 * (1.0 + lax.erf(up * SQRT_HALF))
        activated = (up * half_erf).astype(BF16)
        slope = half_erf + up * jnp.exp(-0.5 * up * up) * INV_ROOT_TWO_PI
        grad_up = (dot_nt(cot_all[...], w_down) * slope).astype(BF16)
        mlp_acc[...] += dot_nn(activated, w_down)
        gn_acc[...] += dot_nt(grad_up, w_up)
        up_sum[pl.ds(step // per * (width // CHUNK), width // CHUNK), :, at] = (
            dot_nn(normed_tr[...], grad_up).astype(BF16).reshape(width // CHUNK, CHUNK, group)
        )
        down_sum[pl.ds(step * (group // CHUNK), group // CHUNK)] = (
            dot_nn(activated.T, cot_all[...]).astype(BF16).reshape(group // CHUNK, CHUNK, width)
        )
        gbias_ref[:, hid] = jnp.sum(grad_up.astype(F32), axis=0, keepdims=True)
        return carry

    lax.fori_loop(0, hidden // group, body, 0)
    stores = [
        pltpu.make_async_copy(src, dst, store_sem.at[n])
        for n, (src, dst) in enumerate(((up_sum, up_out), (down_sum, down_out)))
    ]
    for copy in stores:
        copy.start()
    mlp_ref[...] = mlp_acc[:tok, :].astype(BF16)
    mlp_give[...] = mlp_acc[tok:, :].astype(BF16)
    gn_ref[...] = gn_acc[:tok, :].astype(BF16)
    gn_give[...] = gn_acc[tok:, :].astype(BF16)
    own.wait()
    for step in range(1, spans):
        block_copy(step).wait()
    for copy in stores:
        copy.wait()


def first(heads, normed, cot, w_up, w_down, b_up):
    spans = heads.shape[0]
    tok, width = normed.shape
    hidden = w_up.shape[1]
    vmem = pl.BlockSpec(memory_space=pltpu.VMEM)
    any_spec = pl.BlockSpec(memory_space=pl.ANY)
    tokens = jax.ShapeDtypeStruct((tok, width), BF16)
    sums = (hidden // CHUNK, CHUNK, width)
    both = (2 * tok, width)
    return pl.pallas_call(
        functools.partial(first_kernel, 256),
        out_shape=(jax.ShapeDtypeStruct(heads.shape, BF16),) + (tokens,) * 6
        + (jax.ShapeDtypeStruct(sums, BF16),) * 2
        + (jax.ShapeDtypeStruct((1, hidden), F32),),
        in_specs=[any_spec, vmem, vmem, any_spec, any_spec, vmem],
        out_specs=(any_spec,) + (vmem,) * 6 + (any_spec,) * 2 + (vmem,),
        scratch_shapes=[
            pltpu.VMEM(w_up.shape, BF16), pltpu.VMEM(w_down.shape, BF16),
            pltpu.VMEM(both, BF16), pltpu.VMEM((width, 2 * tok), BF16), pltpu.VMEM(both, BF16),
            pltpu.VMEM(both, F32), pltpu.VMEM(both, F32), pltpu.VMEM(sums, BF16), pltpu.VMEM(sums, BF16),
        ]
        + [pltpu.SemaphoreType.DMA((spans,))] * 2
        + [pltpu.SemaphoreType.DMA((2,))] * 2
        + [pltpu.SemaphoreType.DMA]
        + [pltpu.SemaphoreType.DMA((2,))] * 2,
        compiler_params=pltpu.CompilerParams(collective_id=0, has_side_effects=True, vmem_limit_bytes=VMEM_BIG),
        name="first",
    )(heads, normed, cot, w_up, w_down, b_up)


TREE_PERIOD = 10
TREE_SPINE = 0b0110101011
TREE_ROW = (0, 1, 0, 0, 1, 1, 0, 0, 1, 1)
TREE_ROOT = (1, 2, 0, 2, 3, 1, 2, 1, 2, 1)
TREE_SPAN = 4


def packed_table(values, bits):
    return sum(v << (bits * i) for i, v in enumerate(values))


def tree_roles(i, y, z):
    kind = lax.rem(i, TREE_PERIOD)
    bit = lambda table, bits: lax.bitwise_and(
        lax.shift_right_logical(jnp.int32(table), bits * kind), jnp.int32(2**bits - 1)
    )
    spine = bit(TREE_SPINE, 1) == 1
    row = bit(packed_table(TREE_ROW, 1), 1)
    root = bit(packed_table(TREE_ROOT, 2), 2)
    on_row = y == row
    along = jnp.logical_or(jnp.logical_not(spine), on_row)
    at_root = z == root
    left = jnp.logical_and(along, jnp.logical_and(z <= root, z > 0))
    right = jnp.logical_and(along, jnp.logical_and(z >= root, z < TREE_SPAN - 1))
    side = jnp.logical_and(on_row, jnp.logical_or(spine, at_root))
    to_side = jnp.logical_and(jnp.logical_not(on_row), jnp.logical_or(spine, at_root))
    to_right = jnp.logical_and(along, z < root)
    to_left = jnp.logical_and(along, z > root)
    is_root = jnp.logical_and(on_row, at_root)
    span = jnp.maximum(root, TREE_SPAN - 1 - root)
    base = jnp.where(spine, 1, 0)
    height = jnp.where(
        jnp.logical_and(spine, jnp.logical_not(on_row)), 0,
        base + jnp.where(z < root, z, jnp.where(z > root, TREE_SPAN - 1 - z, span)),
    )
    height = jnp.where(jnp.logical_and(jnp.logical_not(spine), is_root), span + 1, height)
    top = span + 1
    depth = top + jnp.abs(z - root) + jnp.where(on_row, 0, 1)
    flags = (left, right, side, to_left, to_right, to_side, is_root)
    packed = sum(jnp.where(flag, 1 << n, 0) for n, flag in enumerate(flags))
    return packed + height * 128 + jnp.where(is_root, 0, depth) * 2048


def has(roles, n):
    return lax.bitwise_and(roles, jnp.int32(1 << n)) != 0


class Reducer:
    def __init__(self, sources, out, buffers, semaphores, lag, early, gap):
        self.sources, self.out, self.lag, self.early, self.gap = sources, out, lag, early, gap
        self.own, self.sib, self.lands, self.acc = buffers[0], buffers[1], buffers[2:5], buffers[5]
        (self.own_sem, self.give_sem, self.sib_recv, self.up_send) = semaphores[:4]
        self.land_recv = semaphores[4:7]
        self.res_recv, self.pair_recv, self.keep_sem = semaphores[7:10]
        self.down_send = semaphores[10:13]
        self.down_pair = semaphores[13]
        self.total = self.own.shape[0]
        self.ticks = self.total + gap + 2 * TREE_SPAN * lag
        me = lax.axis_index("dp")
        self.core = lax.rem(me, 2)
        self.y = lax.rem(me // 2, 2)
        self.z = me // 4
        self.pair = me + 1 - 2 * self.core
        self.near = (me - 4, me + 4, me + 2 - 4 * self.y)

    def remote(self, src, dst, send, recv, device):
        return pltpu.make_async_remote_copy(
            src_ref=src, dst_ref=dst, send_sem=send, recv_sem=recv, device_id={"dp": device}, device_id_type=MESH
        )

    def arrival(self, dst, recv, i):
        return self.remote(self.own.at[i], dst, self.give_sem.at[i], recv.at[i], self.pair)

    def slot(self, i):
        return self.out.at[2 * i + self.core]

    def begin(self, which=None):
        start = 0
        for n, (ref, offset, count) in enumerate(self.sources):
            if which is None or n in which:
                def body(i, carry, ref=ref, offset=offset, start=start):
                    at = 2 * (i - start + offset)
                    self.remote(
                        ref.at[at + 1 - self.core], self.sib.at[i], self.give_sem.at[i], self.sib_recv.at[i], self.pair
                    ).start()
                    pltpu.make_async_copy(ref.at[at + self.core], self.own.at[i], self.own_sem.at[i]).start()
                    return carry

                lax.fori_loop(start, start + count, body, 0)
            start += count

    def up(self, n, i):
        other = (1, 0, 2)[n]
        return self.remote(self.own.at[i], self.lands[other].at[i], self.up_send.at[i], self.land_recv[other].at[i], self.near[n])

    def down(self, n, src, i):
        return self.remote(src, self.slot(i), self.down_send[n].at[i], self.res_recv.at[i], self.near[n])

    def share(self, src, i):
        return self.remote(src, self.slot(i), self.down_pair.at[i], self.pair_recv.at[i], self.pair)

    def keep(self, i):
        return pltpu.make_async_copy(self.own.at[i], self.slot(i), self.keep_sem.at[i])

    def spread(self, src, i, roles):
        for n in range(3):
            @pl.when(has(roles, n))
            def _(n=n):
                self.down(n, src, i).start()

        self.share(src, i).start()

    def ascend(self, i, roles):
        own, sib, acc = self.own, self.sib, self.acc
        pltpu.make_async_copy(own.at[i], own.at[i], self.own_sem.at[i]).wait()
        self.arrival(sib.at[i], self.sib_recv, i).wait_recv()
        leaf = lax.bitwise_and(roles, jnp.int32(7)) == 0

        @pl.when(leaf)
        def _():
            own[i] = (own[i].astype(F32) + sib[i].astype(F32)).astype(BF16)

        @pl.when(jnp.logical_not(leaf))
        def _():
            acc[...] = own[i].astype(F32) + sib[i].astype(F32)
            for n in range(3):
                @pl.when(has(roles, n))
                def _(n=n):
                    self.arrival(self.lands[n].at[i], self.land_recv[n], i).wait_recv()
                    acc[...] += self.lands[n][i].astype(F32)

            own[i] = acc[...].astype(BF16)

        for n in range(3):
            @pl.when(has(roles, 3 + n))
            def _(n=n):
                self.up(n, i).start()

        @pl.when(has(roles, 6))
        def _():
            self.keep(i).start()
            self.spread(own.at[i], i, roles)

    def descend(self, i, roles):
        self.arrival(self.slot(i), self.res_recv, i).wait_recv()
        self.spread(self.slot(i), i, roles)

    def tick(self, t):
        for level in range(2 * TREE_SPAN + 1):
            at = t - self.lag * level
            late = at >= self.early
            i = at - jnp.where(late, self.gap, 0)
            inside = jnp.logical_and(at >= 0, i < self.total)
            inside = jnp.logical_and(inside, jnp.logical_or(jnp.logical_not(late), i >= self.early))
            roles = tree_roles(jnp.clip(i, 0, self.total - 1), self.y, self.z)
            if level <= TREE_SPAN:
                @pl.when(jnp.logical_and(inside, lax.bitwise_and(roles, jnp.int32(15 * 128)) == level * 128))
                def _(i=i, roles=roles):
                    self.ascend(i, roles)

            if level >= 2:
                @pl.when(jnp.logical_and(inside, lax.bitwise_and(roles, jnp.int32(15 * 2048)) == level * 2048))
                def _(i=i, roles=roles):
                    self.descend(i, roles)

    def run(self, first, last):
        def body(t, carry):
            self.tick(t)
            return carry

        lax.fori_loop(first, last, body, 0)

    def drain(self):
        own = self.own

        def body(i, carry):
            roles = tree_roles(i, self.y, self.z)
            self.remote(own.at[i], self.sib.at[i], self.give_sem.at[i], self.sib_recv.at[i], self.pair).wait_send()

            @pl.when(jnp.logical_not(has(roles, 6)))
            def _():
                self.up(2, i).wait_send()

            @pl.when(has(roles, 6))
            def _():
                self.keep(i).wait()

            for n in range(3):
                @pl.when(has(roles, n))
                def _(n=n):
                    self.down(n, own.at[i], i).wait_send()

            self.share(own.at[i], i).wait_send()
            self.arrival(self.out.at[2 * i + 1 - self.core], self.pair_recv, i).wait_recv()
            return carry

        lax.fori_loop(0, self.total, body, 0)


def reducer_scratch(total, chunk):
    return (
        [pltpu.VMEM((total,) + chunk, BF16)] * 5
        + [pltpu.VMEM(chunk, F32)]
        + [pltpu.SemaphoreType.DMA((total,))] * 14
    )


REDUCER_BUFFERS, REDUCER_REFS = 6, 20


def attention_kernel(
    tile, order_ref, place_ref, in_ref, angle_ref, stage,
    q_nat, k_nat, v_nat, k_tr, v_tr, g_tr, probs, kv_grad, aq_out,
):
    spans, tok, _ = in_ref.shape
    length = spans * tok
    blocks = length // tile
    scale = 1.0 / math.sqrt(HEAD_DIM)
    zeros = jnp.zeros((tok, HEAD_DIM), BF16)

    def gather(place, carry):
        span = order_ref[place]
        rows = pl.ds(pl.multiple_of(place * tok, tok), tok)
        data = in_ref[span]
        q_nat[rows, :] = jnp.concatenate([data[:, :HEAD_DIM] * jnp.asarray(scale, BF16), zeros], axis=1)
        k_nat[rows, :] = data[:, HEAD_DIM : 2 * HEAD_DIM]
        v_nat[rows, :] = data[:, 2 * HEAD_DIM : 3 * HEAD_DIM]
        aq_out[rows, :HEAD_DIM] = data[:, 3 * HEAD_DIM :]
        return carry

    lax.fori_loop(0, spans, gather, 0)

    def flip(block, carry):
        rows = pl.ds(pl.multiple_of(block * tile, tile), tile)
        k_tr[:, rows] = k_nat[rows, :].T
        v_tr[:, rows] = v_nat[rows, :].T
        g_tr[:, rows] = aq_out[rows, :HEAD_DIM].T
        kv_grad[rows, :] = jnp.zeros((tile, 2 * HEAD_DIM), F32)
        return carry

    lax.fori_loop(0, blocks, flip, 0)

    tall = 2 * tile
    ahead = lax.broadcasted_iota(jnp.int32, (tall, tile), 0) - lax.broadcasted_iota(jnp.int32, (tall, tile), 1)
    pad = jnp.zeros((tile, HEAD_DIM), BF16)
    half_rot = ROT // 2

    def turn_back(grad, rows):
        cosine, sine = angle_ref[0, :, rows], angle_ref[1, :, rows]
        first, second = grad[:half_rot], grad[half_rot:ROT]
        return jnp.concatenate([first * cosine + second * sine, second * cosine - first * sine, grad[ROT:]], axis=0)

    def query_block(block, carry):
        q_rows = pl.ds(pl.multiple_of(block * tile, tile), tile)
        queries_pad = q_nat[q_rows, :]
        queries = queries_pad[:, :HEAD_DIM]

        final = block // 2

        def forward(j, state, masked):
            mixed, totals = state
            rows = pl.ds(pl.multiple_of(j * tall, tall), tall)
            prob = jnp.exp(dot_nt(k_nat[rows, :], queries))
            if masked:
                prob = jnp.where(ahead <= block * tile - j * tall, prob, 0.0)
            probs[rows, :] = prob
            mixed = mixed + dot_nn(v_tr[:, rows], prob.astype(BF16))
            totals = totals + jnp.sum(prob.reshape(tall // 8, 8, tile), axis=0)
            return mixed, totals

        state = (jnp.zeros((HEAD_DIM, tile), F32), jnp.zeros((8, tile), F32))
        state = lax.fori_loop(0, final, lambda j, s: forward(j, s, False), state)
        mixed, totals = forward(final, state, True)
        totals = jnp.sum(totals, axis=0, keepdims=True)
        attended = mixed / totals
        grad_att = g_tr[:, q_rows].astype(F32)
        grad_mixed = (grad_att / totals).astype(BF16)
        grad_totals = (-jnp.sum(grad_att * attended, axis=0, keepdims=True) / totals).astype(BF16).astype(F32)
        grad_pad = jnp.concatenate([pad, grad_mixed.T], axis=1)

        def backward(j, grad_q):
            rows = pl.ds(pl.multiple_of(j * tall, tall), tall)
            prob = probs[rows, :]
            grad_scores = (prob * (dot_nn(v_nat[rows, :], grad_mixed) + grad_totals)).astype(BF16)
            kv_grad[rows, :] += dot_nn(grad_scores, queries_pad) + dot_nn(prob.astype(BF16), grad_pad)
            return grad_q + dot_nn(k_tr[:, rows], grad_scores)

        grad_q = lax.fori_loop(0, final + 1, backward, jnp.zeros((HEAD_DIM, tile), F32))
        aq_out[q_rows, :] = jnp.concatenate([attended, turn_back(grad_q * scale, q_rows)], axis=0).T.astype(BF16)
        return carry

    lax.fori_loop(0, blocks, query_block, 0)

    def turn_keys(block, carry):
        rows = pl.ds(pl.multiple_of(block * tile, tile), tile)
        kv_grad[rows, :] = turn_back(kv_grad[rows, :].T, rows).T
        return carry

    lax.fori_loop(0, blocks, turn_keys, 0)

    def fill(span, carry):
        rows = pl.ds(pl.multiple_of(place_ref[span] * tok, tok), tok)
        stage[span, :, : 2 * HEAD_DIM] = aq_out[rows, :]
        stage[span, :, 2 * HEAD_DIM :] = kv_grad[rows, :].astype(BF16)
        return carry

    lax.fori_loop(0, spans, fill, 0)


def attention(heads, order, places):
    spans, tok, width = heads.shape
    length = spans * tok
    tile = 256
    half_rot = ROT // 2
    frequency = ROPE_BASE ** (-(jnp.arange(half_rot, dtype=F32) * 2.0 / ROT))
    angles = frequency[:, None] * jnp.arange(length, dtype=F32)[None, :]
    angle_tables = jnp.stack([jnp.cos(angles), jnp.sin(angles)])
    vmem = pl.BlockSpec(memory_space=pltpu.VMEM)
    smem = pl.BlockSpec(memory_space=pltpu.SMEM)
    return pl.pallas_call(
        functools.partial(attention_kernel, tile),
        out_shape=jax.ShapeDtypeStruct(heads.shape, BF16),
        in_specs=[smem, smem, vmem, vmem],
        out_specs=vmem,
        scratch_shapes=[
            pltpu.VMEM((length, 2 * HEAD_DIM), BF16),
            pltpu.VMEM((length, HEAD_DIM), BF16),
            pltpu.VMEM((length, HEAD_DIM), BF16),
            pltpu.VMEM((HEAD_DIM, length), BF16),
            pltpu.VMEM((HEAD_DIM, length), BF16),
            pltpu.VMEM((HEAD_DIM, length), BF16),
            pltpu.VMEM((length, tile), F32),
            pltpu.VMEM((length, 2 * HEAD_DIM), F32),
            pltpu.VMEM((length, 2 * HEAD_DIM), BF16),
        ],
        compiler_params=pltpu.CompilerParams(vmem_limit_bytes=VMEM_BIG),
        cost_estimate=pl.CostEstimate(flops=40 * 10**9, bytes_accessed=10**7, transcendentals=10**7),
        name="attention",
    )(order, places, heads, angle_tables)


def last_kernel(
    lag, gap, per_block,
    stage, mlp_in, gn_in, up_in, down_in, wqkv_hbm, wout_hbm,
    x_ref, cot_ref, cot_peer, normed_ref, normed_peer, gain_ref, bias_ref, mlp_own, gn_own, gbias_ref,
    out_ref, grad_in_ref, summed, *scratch,
):
    (heads_own, heads_peer, mlp_other, gn_other, wqkv_ref, wout_ref, att_ref, att_peer, gproj_ref, gproj_peer, normed_tr,
     sums_ref, small_ref, landing) = scratch[:14]
    (head_send, head_recv, relay_send, relay_recv, pair_send, pair_recv, local_sem, load_sem, swap_send, swap_recv) = scratch[14:24]
    buffers = scratch[24:]
    spans = stage.shape[0]
    tok, width = x_ref.shape
    chunks = width // CHUNK
    me = lax.axis_index("dp")
    here = lax.axis_index("mlp")
    greet(pltpu.get_barrier_semaphore(), spans)
    pairs = [
        to_peer(src, dst, pair_send.at[n], pair_recv.at[n])
        for n, (src, dst) in enumerate(((mlp_in, mlp_other), (gn_in, gn_other)))
    ]
    loads = [
        pltpu.make_async_copy(src, dst, load_sem.at[n])
        for n, (src, dst) in enumerate(((wqkv_hbm, wqkv_ref), (wout_hbm, wout_ref)))
    ]

    def block_copy(step):
        target = lax.rem(me + step, spans)
        return pltpu.make_async_remote_copy(
            src_ref=stage.at[target], dst_ref=heads_own.at[me], send_sem=head_send.at[step], recv_sem=head_recv.at[step],
            device_id={"dp": target}, device_id_type=MESH,
        )

    def relay(source_ref, step):
        source = lax.rem(me + spans - step, spans)
        return to_peer(source_ref.at[source], heads_peer.at[source], relay_send.at[step], relay_recv.at[step])

    for step in range(1, spans):
        block_copy(step).start()
    relay(stage, 0).start()
    own = pltpu.make_async_copy(stage.at[me], heads_own.at[me], local_sem)
    own.start()
    for copy in loads + pairs:
        copy.start()
    early = up_in.shape[0] // 2 + down_in.shape[0] // 2
    reducer = Reducer(
        ((up_in, 0, up_in.shape[0] // 2), (down_in, 0, down_in.shape[0] // 2), (sums_ref, 0, sums_ref.shape[0] // 2)),
        summed, buffers[:REDUCER_BUFFERS], buffers[REDUCER_BUFFERS:], lag, early, gap,
    )
    reducer.begin((0, 1))

    def hand_on(step, carry):
        block_copy(step).wait_recv()
        relay(heads_own, step).start()
        reducer.run((step - 1) * per_block, step * per_block)
        return carry

    lax.fori_loop(1, spans, hand_on, 0)
    state = [(spans - 1) * per_block]

    def advance(count):
        stop = min(state[0] + count, early + gap)
        reducer.run(state[0], stop)
        state[0] = stop

    own.wait()
    for copy in loads:
        copy.wait()
    low = lax.broadcasted_iota(jnp.int32, (tok, LANES), 1) < HEAD_DIM

    def unpack(source, att_to, gproj_to):
        for pair in range(HEADS // 2):
            at = pair * LANES
            even, odd = source[2 * pair].astype(F32), source[2 * pair + 1].astype(F32)
            att, gq = split_pair(even[:, :LANES], odd[:, :LANES], low)
            gk, gv = split_pair(even[:, LANES:], odd[:, LANES:], low)
            att_to[:, at : at + LANES] = att.astype(BF16)
            for part, grad in enumerate((gq, gk, gv)):
                gproj_to[:, part * width + at : part * width + at + LANES] = grad.astype(BF16)

    unpack(heads_own, att_ref, gproj_ref)
    advance(1)
    normed_tr[:, :tok] = normed_ref[...].T
    normed_tr[:, tok:] = normed_peer[...].T
    for copy in pairs:
        copy.wait()
    advance(1)
    rows = x_ref[...].astype(F32)
    branch = mlp_own[...].astype(F32) + mlp_other[...].astype(F32)
    out_ref[...] = (rows + dot_nn(att_ref[...], wout_ref[...]) + branch + bias_ref[...]).astype(BF16)
    advance(1)
    grad_normed = dot_nt(gproj_ref[...], wqkv_ref[...]) + gn_own[...].astype(F32) + gn_other[...].astype(F32)
    grad_in_ref[...] = grad_normed
    advance(1)
    rows = x_ref[...].astype(F32)
    cot = cot_ref[...].astype(F32)
    grad_normed = grad_in_ref[...]
    centre = jnp.mean(rows, axis=-1, keepdims=True)
    centred = rows - centre
    inv = lax.rsqrt(jnp.mean(centred * centred, axis=-1, keepdims=True) + EPSILON)
    unit = centred * inv
    small_ref[0:1, :] = jnp.sum(grad_normed * unit, axis=0, keepdims=True)
    small_ref[1:2, :] = jnp.sum(grad_normed, axis=0, keepdims=True)
    small_ref[2:3, :] = jnp.sum(cot, axis=0, keepdims=True)
    for part in range(3):
        part_cols = slice(part * width, (part + 1) * width)
        small_ref[3 + part : 4 + part, :] = jnp.sum(gproj_ref[:, part_cols].astype(F32), axis=0, keepdims=True)
    small_ref[6:7, :] = gbias_ref[:, :width]
    small_ref[7:8, :] = gbias_ref[:, width:]
    grad_unit = grad_normed * gain_ref[...]
    grad_in_ref[...] = cot + inv * (
        grad_unit
        - jnp.mean(grad_unit, axis=-1, keepdims=True)
        - unit * jnp.mean(grad_unit * unit, axis=-1, keepdims=True)
    )
    swap = to_peer(small_ref, landing, swap_send, swap_recv)
    swap.start()
    advance(1)
    for step in range(spans):
        relay(heads_own, step).wait()
    unpack(heads_peer, att_peer, gproj_peer)
    advance(1)
    third, half, group = 3 * width // 2, width // 2, 512
    for start in range(0, third, group):
        cols = pl.ds(pl.multiple_of(here * third + start, LANES), group)
        block, at = start // width, start % width
        sums_ref[block * chunks : (block + 1) * chunks, :, at : at + group] = (
            dot_nn(normed_tr[...], jnp.concatenate([gproj_ref[:, cols], gproj_peer[:, cols]], axis=0))
            .astype(BF16).reshape(chunks, CHUNK, group)
        )
        advance(1)
    cols = pl.ds(pl.multiple_of(here * half, LANES), half)
    att_tr = jnp.concatenate([att_ref[...], att_peer[...]], axis=0).T
    cots = jnp.concatenate([cot_ref[:, cols], cot_peer[:, cols]], axis=0)
    sums_ref[chunks : 2 * chunks, :, half:] = dot_nn(att_tr, cots).astype(BF16).reshape(chunks, CHUNK, half)
    swap.wait()
    shared = lax.broadcasted_iota(jnp.int32, (8, width), 0) < 6
    sums_ref[2 * chunks : 2 * chunks + 2] = jnp.zeros((2, CHUNK, width), BF16)
    sums_ref[2 * chunks, 0:16, :] = jnp.concatenate(
        [small_ref[...] + jnp.where(shared, landing[...], 0.0), jnp.zeros((8, width), F32)], axis=0
    ).astype(BF16)
    advance(early + gap)
    reducer.begin((2,))
    reducer.run(early + gap, reducer.ticks)
    reducer.drain()
    for step in range(1, spans):
        block_copy(step).wait_send()


def last(stage, mlp_give, gn_give, sum_up, sum_down, w_qkv, w_out, *operands):
    spans = stage.shape[0]
    tok, width = operands[0].shape
    chunk = sum_up.shape[1:]
    late = 2 * (width // CHUNK) + 2
    total = (sum_up.shape[0] + sum_down.shape[0] + late) // 2
    vmem = pl.BlockSpec(memory_space=pltpu.VMEM)
    any_spec = pl.BlockSpec(memory_space=pl.ANY)
    tokens, wide = pltpu.VMEM((tok, width), BF16), pltpu.VMEM((tok, 3 * width), BF16)
    return pl.pallas_call(
        functools.partial(last_kernel, TREE_LAG, TREE_GAP, TICKS_PER_BLOCK),
        out_shape=(
            jax.ShapeDtypeStruct((tok, width), BF16),
            jax.ShapeDtypeStruct((tok, width), F32),
            jax.ShapeDtypeStruct((2 * total,) + chunk, BF16),
        ),
        in_specs=[any_spec] * 7 + [vmem] * len(operands),
        out_specs=(vmem, vmem, any_spec),
        scratch_shapes=[
            pltpu.VMEM(stage.shape, BF16), pltpu.VMEM(stage.shape, BF16), tokens, tokens,
            pltpu.VMEM(w_qkv.shape, BF16), pltpu.VMEM(w_out.shape, BF16), tokens, tokens, wide, wide,
            pltpu.VMEM((width, 2 * tok), BF16), pltpu.VMEM((late,) + chunk, BF16),
            pltpu.VMEM((8, width), F32), pltpu.VMEM((8, width), F32),
        ]
        + [pltpu.SemaphoreType.DMA((spans,))] * 4
        + [pltpu.SemaphoreType.DMA((2,))] * 2
        + [pltpu.SemaphoreType.DMA, pltpu.SemaphoreType.DMA((2,)), pltpu.SemaphoreType.DMA, pltpu.SemaphoreType.DMA]
        + reducer_scratch(total, chunk),
        compiler_params=pltpu.CompilerParams(
            collective_id=1, has_side_effects=True, vmem_limit_bytes=VMEM_ALL
        ),
        name="last",
    )(stage, mlp_give, gn_give, sum_up, sum_down, w_qkv, w_out, *operands)


def widen_kernel(up_a, up_b, down_a, down_b, first_ref, second_ref, vec_ref, out_in, grad_in,
                 qkv_ref, out_ref, up_ref, down_ref, vec_out, out_out, grad_out):
    width = first_ref.shape[-1]
    half = width // 2
    qkv_ref[:, :width] = first_ref[0].astype(F32)
    qkv_ref[:, width:] = second_ref[0, :, :half].astype(F32)
    out_ref[...] = second_ref[0, :, half:].astype(F32)
    up_ref[:, :width] = up_a[0].astype(F32)
    up_ref[:, width:] = up_b[0].astype(F32)
    down_ref[0] = down_a[0].astype(F32)
    down_ref[1] = down_b[0].astype(F32)

    @pl.when(pl.program_id(0) == 0)
    def _():
        vec_out[...] = vec_ref[0, :16, :].astype(F32)
        out_out[...] = out_in[...]
        grad_out[...] = grad_in[...]


def widen(summed, output, grad_input):
    chunk, width = summed.shape[1:]
    steps = width // chunk
    row = lambda cols: pl.BlockSpec((chunk, cols), lambda s: (s, 0))
    blocks = [pl.BlockSpec((1, chunk, width), lambda s, n=n: (n * steps + s, 0, 0)) for n in range(6)]
    const = lambda shape: pl.BlockSpec(shape, lambda s: (0,) * len(shape))
    qkv, out, up, down, vec, output, grad_input = pl.pallas_call(
        widen_kernel,
        grid=(steps,),
        out_shape=(
            jax.ShapeDtypeStruct((width, 3 * width // 2), F32),
            jax.ShapeDtypeStruct((width, width // 2), F32),
            jax.ShapeDtypeStruct((width, 2 * width), F32),
            jax.ShapeDtypeStruct((2, width, width), F32),
            jax.ShapeDtypeStruct((16, width), F32),
            jax.ShapeDtypeStruct(output.shape, BF16),
            jax.ShapeDtypeStruct(grad_input.shape, F32),
        ),
        in_specs=blocks
        + [
            pl.BlockSpec((1, chunk, width), lambda s: (6 * steps, 0, 0)),
            const(output.shape), const(grad_input.shape),
        ],
        out_specs=(
            row(3 * width // 2), row(width // 2), row(2 * width),
            pl.BlockSpec((2, chunk, width), lambda s: (0, s, 0)),
            const((16, width)), const(output.shape), const(grad_input.shape),
        ),
        name="widen",
    )(*[summed] * 7, output, grad_input)
    return qkv, out, up, down.reshape(2 * width, width), vec, output, grad_input


def by_heads(
    block_input, span_offset, ln_gain, ln_bias, w_qkv, b_qkv, w_out, b_out, w_up, b_up, w_down, b_down, cotangent
):
    tok, width = block_input.shape[2:]
    spans = span_offset.shape[0]
    span_here = lax.axis_index("dp")
    seq_here = lax.axis_index("mlp")
    offsets = lax.dynamic_index_in_dim(span_offset, seq_here, axis=1, keepdims=False)
    places = jnp.arange(spans, dtype=jnp.int32)
    order = jnp.sum(jnp.where(offsets[None, :] == places[:, None], places[None, :], 0), axis=1)
    offset_here = lax.dynamic_index_in_dim(offsets, span_here, axis=0, keepdims=False)
    tables = rotary_tables(offset_here * tok + jnp.arange(tok, dtype=jnp.int32))
    x, cot = block_input[0, 0], cotangent[0, 0]
    gain, shift = ln_gain[None], ln_bias[None]

    normed, send = project(x, cot, gain, shift, w_qkv, b_qkv[None], w_out, tables)
    heads, normed_peer, cot_peer, mlp_part, mlp_give, gn_part, gn_give, sum_up, sum_down, grad_b_up = first(
        send, normed, cot, w_up, w_down, b_up[None]
    )
    stage = attention(heads, order, offsets)
    output, grad_input, summed = last(
        stage, mlp_give, gn_give, sum_up, sum_down, w_qkv, w_out,
        x, cot, cot_peer, normed, normed_peer, gain, (b_out + b_down)[None], mlp_part, gn_part, grad_b_up,
    )
    qkv, out, up, down, vec, output, grad_input = widen(summed, output, grad_input)
    half = width // 2
    piece = lambda start, rows: lax.dynamic_slice_in_dim(
        vec[start : start + rows].reshape(-1), seq_here * (rows * half), rows * half
    )
    bias_sum = piece(2, 1)
    return (
        output.reshape(1, 1, tok, width),
        grad_input.reshape(1, 1, tok, width),
        piece(0, 1),
        piece(1, 1),
        qkv,
        piece(3, 3),
        out,
        bias_sum,
        up,
        vec[6:8].reshape(-1),
        down,
        bias_sum,
    )


def rotate(values, positions, sign_factor):
    half_rot = ROT // 2
    frequency = ROPE_BASE ** (-(jnp.arange(half_rot, dtype=jnp.float32) * 2.0 / ROT))
    angles = positions.astype(jnp.float32)[:, None] * frequency[None, :]
    cosine = jnp.cos(angles)[:, None, :]
    sine_part = sign_factor * jnp.sin(angles)[:, None, :]
    first_half = values[..., :half_rot]
    second_half = values[..., half_rot:ROT]
    return jnp.concatenate(
        [
            first_half * cosine - second_half * sine_part,
            second_half * cosine + first_half * sine_part,
            values[..., ROT:],
        ],
        axis=-1,
    )


def gelu_exact(values):
    return 0.5 * values * (1.0 + lax.erf(values * SQRT_HALF))


def gelu_slope(values):
    return (
        0.5 * (1.0 + lax.erf(values * SQRT_HALF))
        + values * jnp.exp(-0.5 * values * values) * INV_ROOT_TWO_PI
    )


def piece_count(total_rows):
    count_blocks = max(1, total_rows // 1024)
    while total_rows % count_blocks:
        count_blocks += 1
    return count_blocks


def row_positions(offsets, count_rows, tok_count):
    index_all = jnp.arange(count_rows, dtype=jnp.int32)
    span_of = index_all // tok_count
    within = index_all - span_of * tok_count
    matches = span_of[:, None] == jnp.arange(offsets.shape[0], dtype=jnp.int32)[None, :]
    offset_of = jnp.sum(jnp.where(matches, offsets[None, :], 0), axis=1)
    return offset_of * tok_count + within


def contract_rows(left_mat, right_mat):
    return lax.dot_general(
        left_mat, right_mat, (((0,), (0,)), ((), ())), preferred_element_type=jnp.float32
    )


def contract_cols(left_mat, right_mat):
    return lax.dot_general(
        left_mat, right_mat, (((1,), (1,)), ((), ())), preferred_element_type=jnp.float32
    )


def local(
    block_input,
    span_offset,
    ln_gain,
    ln_bias,
    w_qkv,
    b_qkv,
    w_out,
    b_out,
    w_up,
    b_up,
    w_down,
    b_down,
    cotangent,
):
    tok_count = block_input.shape[2]
    model_width = block_input.shape[3]
    scale_dot = 1.0 / math.sqrt(HEAD_DIM)
    span_here = lax.axis_index("dp")
    seq_here = lax.axis_index("mlp")
    offsets = lax.dynamic_index_in_dim(span_offset, seq_here, axis=1, keepdims=False)
    offset_here = lax.dynamic_index_in_dim(offsets, span_here, axis=0, keepdims=False)
    positions = offset_here * tok_count + jnp.arange(tok_count, dtype=jnp.int32)
    row_data = block_input[0, 0].astype(jnp.float32)
    centre = jnp.mean(row_data, axis=-1, keepdims=True)
    centred = row_data - centre
    spread = jnp.mean(centred * centred, axis=-1, keepdims=True)
    inv_scale = lax.rsqrt(spread + EPSILON)
    unit_rows = centred * inv_scale
    normed = (unit_rows * ln_gain + ln_bias).astype(jnp.bfloat16)
    project = jnp.dot(normed, w_qkv, preferred_element_type=jnp.float32) + b_qkv
    queries = rotate(
        project[:, :model_width].reshape(tok_count, HEADS, HEAD_DIM), positions, 1.0
    ).astype(jnp.bfloat16)
    keys_here = rotate(
        project[:, model_width : 2 * model_width].reshape(tok_count, HEADS, HEAD_DIM),
        positions,
        1.0,
    ).astype(jnp.bfloat16)
    values_here = (
        project[:, 2 * model_width :].reshape(tok_count, HEADS, HEAD_DIM).astype(jnp.bfloat16)
    )
    keys_flat = keys_here.reshape(tok_count, model_width)
    values_flat = values_here.reshape(tok_count, model_width)
    start_state = (
        jnp.zeros((tok_count, HEADS, HEAD_DIM), jnp.float32),
        jnp.zeros((HEADS, tok_count), jnp.float32),
    )
    keys_piece = lax.all_gather(keys_flat, "dp", axis=0, tiled=True)
    values_piece = lax.all_gather(values_flat, "dp", axis=0, tiled=True)
    piece_rows = keys_piece.shape[0]
    blocks = piece_count(piece_rows)
    sub_rows = piece_rows // blocks
    key_pos = row_positions(offsets, piece_rows, tok_count)

    def attend_one_block(state_now, packed):
        keys_blk, values_blk, pos_blk = packed
        key_heads = keys_blk.reshape(sub_rows, HEADS, HEAD_DIM)
        value_heads = values_blk.reshape(sub_rows, HEADS, HEAD_DIM)
        scores = (
            jnp.einsum("qhd,khd->hqk", queries, key_heads, preferred_element_type=jnp.float32)
            * scale_dot
        )
        allowed = pos_blk[None, :] <= positions[:, None]
        weights_exp = jnp.where(allowed[None], jnp.exp(scores), 0.0)
        mixed_sum, totals = state_now
        mixed_sum = mixed_sum + jnp.einsum(
            "hqk,khd->qhd",
            weights_exp.astype(jnp.bfloat16),
            value_heads,
            preferred_element_type=jnp.float32,
        )
        return ((mixed_sum, totals + jnp.sum(weights_exp, axis=-1)), None)

    state_now, _unused = lax.scan(
        attend_one_block,
        start_state,
        (
            keys_piece.reshape(blocks, sub_rows, model_width),
            values_piece.reshape(blocks, sub_rows, model_width),
            key_pos.reshape(blocks, sub_rows),
        ),
    )
    mixed_sum, totals = state_now
    attended = mixed_sum / totals.T[:, :, None]
    attended_low = attended.reshape(tok_count, model_width).astype(jnp.bfloat16)
    attn_branch = jnp.dot(attended_low, w_out, preferred_element_type=jnp.float32) + b_out
    normed_all = lax.all_gather(normed, "mlp", axis=0, tiled=True)
    up_proj = jnp.dot(normed_all, w_up, preferred_element_type=jnp.float32) + b_up
    activated = gelu_exact(up_proj).astype(jnp.bfloat16)
    mlp_branch = (
        lax.psum_scatter(
            jnp.dot(activated, w_down, preferred_element_type=jnp.float32).astype(jnp.bfloat16),
            "mlp",
            scatter_dimension=0,
            tiled=True,
        ).astype(jnp.float32)
        + b_down
    )
    output = (row_data + attn_branch + mlp_branch).astype(jnp.bfloat16)
    grad_out = cotangent[0, 0]
    grad_w_out = contract_rows(attended_low, grad_out)
    grad_bias_out = jnp.sum(grad_out.astype(jnp.float32), axis=0)
    grad_all = lax.all_gather(grad_out, "mlp", axis=0, tiled=True)
    grad_w_down = contract_rows(activated, grad_all)
    grad_act = contract_cols(grad_all, w_down)
    grad_up = (grad_act * gelu_slope(up_proj)).astype(jnp.bfloat16)
    grad_w_up = contract_rows(normed_all, grad_up)
    grad_b_up = jnp.sum(grad_up.astype(jnp.float32), axis=0)
    grad_norm_mlp = lax.psum_scatter(
        contract_cols(grad_up, w_up).astype(jnp.bfloat16), "mlp", scatter_dimension=0, tiled=True
    ).astype(jnp.float32)
    grad_att = contract_cols(grad_out, w_out).reshape(tok_count, HEADS, HEAD_DIM)
    grad_mixed = (grad_att / totals.T[:, :, None]).astype(jnp.bfloat16)
    grad_totals = ((-jnp.sum(grad_att * attended, axis=-1)).T / totals).astype(jnp.bfloat16)
    grad_totals_wide = grad_totals.astype(jnp.float32)[:, :, None]
    zero_heads = jnp.zeros((tok_count, HEADS, HEAD_DIM), jnp.float32)
    grad_query_sum = zero_heads
    keys_piece = lax.all_gather(keys_flat, "dp", axis=0, tiled=True)
    values_piece = lax.all_gather(values_flat, "dp", axis=0, tiled=True)
    piece_rows = keys_piece.shape[0]
    blocks = piece_count(piece_rows)
    back_sub_rows = piece_rows // blocks
    key_pos = row_positions(offsets, piece_rows, tok_count)

    def back_one_block(running_sum, packed):
        keys_blk, values_blk, pos_blk = packed
        key_heads = keys_blk.reshape(back_sub_rows, HEADS, HEAD_DIM)
        value_heads = values_blk.reshape(back_sub_rows, HEADS, HEAD_DIM)
        scores = (
            jnp.einsum("qhd,khd->hqk", queries, key_heads, preferred_element_type=jnp.float32)
            * scale_dot
        )
        allowed = pos_blk[None, :] <= positions[:, None]
        weights_exp = jnp.where(allowed[None], jnp.exp(scores), 0.0)
        grad_exp = jnp.einsum(
            "qhd,khd->hqk", grad_mixed, value_heads, preferred_element_type=jnp.float32
        )
        grad_scores = (weights_exp * (grad_exp + grad_totals_wide)).astype(jnp.bfloat16)
        running_sum = running_sum + scale_dot * jnp.einsum(
            "hqk,khd->qhd", grad_scores, key_heads, preferred_element_type=jnp.float32
        )
        grad_key_blk = scale_dot * jnp.einsum(
            "hqk,qhd->khd", grad_scores, queries, preferred_element_type=jnp.float32
        )
        grad_value_blk = jnp.einsum(
            "hqk,qhd->khd",
            weights_exp.astype(jnp.bfloat16),
            grad_mixed,
            preferred_element_type=jnp.float32,
        )
        joined = jnp.concatenate(
            [
                grad_key_blk.reshape(back_sub_rows, model_width),
                grad_value_blk.reshape(back_sub_rows, model_width),
            ],
            axis=1,
        )
        return (running_sum, joined)

    grad_query_sum, stacked = lax.scan(
        back_one_block,
        grad_query_sum,
        (
            keys_piece.reshape(blocks, back_sub_rows, model_width),
            values_piece.reshape(blocks, back_sub_rows, model_width),
            key_pos.reshape(blocks, back_sub_rows),
        ),
    )
    grad_kv_sum = stacked.reshape(piece_rows, 2 * model_width)
    grad_kv = lax.psum_scatter(
        grad_kv_sum.astype(jnp.bfloat16), "dp", scatter_dimension=0, tiled=True
    ).astype(jnp.float32)
    grad_keys = grad_kv[:, :model_width].reshape(tok_count, HEADS, HEAD_DIM)
    grad_values = grad_kv[:, model_width:].reshape(tok_count, HEADS, HEAD_DIM)
    grad_query_pre = rotate(grad_query_sum, positions, -1.0).reshape(tok_count, model_width)
    grad_key_pre = rotate(grad_keys, positions, -1.0).reshape(tok_count, model_width)
    grad_project = jnp.concatenate(
        [grad_query_pre, grad_key_pre, grad_values.reshape(tok_count, model_width)], axis=1
    ).astype(jnp.bfloat16)
    grad_w_qkv = contract_rows(normed, grad_project)
    grad_b_qkv = jnp.sum(grad_project.astype(jnp.float32), axis=0)
    grad_normed = contract_cols(grad_project, w_qkv) + grad_norm_mlp
    grad_ln_gain = jnp.sum(grad_normed * unit_rows, axis=0)
    grad_ln_bias = jnp.sum(grad_normed, axis=0)
    grad_unit = grad_normed * ln_gain
    grad_rows = inv_scale * (
        grad_unit
        - jnp.mean(grad_unit, axis=-1, keepdims=True)
        - unit_rows * jnp.mean(grad_unit * unit_rows, axis=-1, keepdims=True)
    )
    grad_input = (grad_out.astype(jnp.float32) + grad_rows).reshape(1, 1, tok_count, model_width)
    part_qkv, part_out, part_bqkv, part_bias, part_gain, part_shift = (
        lax.psum_scatter(
            grad_w_qkv.astype(jnp.bfloat16), "mlp", scatter_dimension=1, tiled=True
        ).astype(jnp.float32),
        lax.psum_scatter(
            grad_w_out.astype(jnp.bfloat16), "mlp", scatter_dimension=1, tiled=True
        ).astype(jnp.float32),
        lax.psum_scatter(
            grad_b_qkv.astype(jnp.bfloat16), "mlp", scatter_dimension=0, tiled=True
        ).astype(jnp.float32),
        lax.psum_scatter(
            grad_bias_out.astype(jnp.bfloat16), "mlp", scatter_dimension=0, tiled=True
        ).astype(jnp.float32),
        lax.psum_scatter(
            grad_ln_gain.astype(jnp.bfloat16), "mlp", scatter_dimension=0, tiled=True
        ).astype(jnp.float32),
        lax.psum_scatter(
            grad_ln_bias.astype(jnp.bfloat16), "mlp", scatter_dimension=0, tiled=True
        ).astype(jnp.float32),
    )
    summed = (
        lax.psum(part_qkv.astype(jnp.bfloat16), "dp").astype(jnp.float32),
        lax.psum(part_out.astype(jnp.bfloat16), "dp").astype(jnp.float32),
        lax.psum(part_bqkv.astype(jnp.bfloat16), "dp").astype(jnp.float32),
        lax.psum(part_bias.astype(jnp.bfloat16), "dp").astype(jnp.float32),
        lax.psum(part_gain.astype(jnp.bfloat16), "dp").astype(jnp.float32),
        lax.psum(part_shift.astype(jnp.bfloat16), "dp").astype(jnp.float32),
        lax.psum(grad_w_up.astype(jnp.bfloat16), "dp").astype(jnp.float32),
        lax.psum(grad_b_up.astype(jnp.bfloat16), "dp").astype(jnp.float32),
        lax.psum(grad_w_down.astype(jnp.bfloat16), "dp").astype(jnp.float32),
    )
    return (
        output.reshape(1, 1, tok_count, model_width),
        grad_input,
        summed[4],
        summed[5],
        summed[0],
        summed[2],
        summed[1],
        summed[3],
        summed[6],
        summed[7],
        summed[8],
        summed[3],
    )


def solution(mesh):
    fits = mesh.shape["dp"] == HEADS and mesh.shape["mlp"] == 2
    return jax.shard_map(
        by_heads if fits else local,
        mesh=mesh,
        in_specs=(
            P("dp", "mlp", None, None),
            P(),
            P(),
            P(),
            P(),
            P(),
            P(),
            P(),
            P(None, "mlp"),
            P("mlp"),
            P("mlp", None),
            P(),
            P("dp", "mlp", None, None),
        ),
        out_specs=(
            P("dp", "mlp", None, None),
            P("dp", "mlp", None, None),
            P("mlp"),
            P("mlp"),
            P(None, "mlp"),
            P("mlp"),
            P(None, "mlp"),
            P("mlp"),
            P(None, "mlp"),
            P("mlp"),
            P("mlp", None),
            P("mlp"),
        ),
        check_vma=False,
    )
```
